256 devices in a mesh: ba: 4 (over z_hi, core), gx: 16 (over x, y), gy: 4 (over z_lo).
Axes of the slice: x: 4, y: 4, z: 8 (z_hi: 2, z_lo: 4; z = z_hi * 4 + z_lo), core: 2. Of those that a mesh axis runs over, the one named last changes fastest.
Arguments:
- pixels: bfloat16 [896, 224, 6], P(('ba', 'gx'), 'gy'), parts along dimension 0, may hold values from -6 to 6
- conv_weight: bfloat16 [54, 704], replicated, may hold values from -0.875 to 0.875
- input_gain: float32 [704], replicated, may hold values from 0.5 to 1.5
- key_weight: bfloat16 [704, 1024], replicated, may hold values from -0.21875 to 0.21875
- value_weight: bfloat16 [704, 1024], replicated, may hold values from -0.21875 to 0.21875
- latents: bfloat16 [512, 1024], replicated, may hold values from -6 to 6
- latent_gain: float32 [1024], replicated, may hold values from 0.5 to 1.5
- query_weight: bfloat16 [1024, 1024], replicated, as said below
- out_weight: bfloat16 [1024, 1024], replicated, may hold values from -0.1875 to 0.1875
Outputs:
- new_latents: bfloat16 [2048, 1024], P(('ba', 'gx', 'gy')), parts along dimension 0
The draws below stay inside these ranges and needn't reach their ends.
There are 4 independent parts, one for each index of `ba`. The reference program is written for one: setup_inputs(seed, part) draws one part's arguments, and reference() takes and returns one part's arrays. A program takes and returns all parts, laid end to end along the dimension named above; an argument that names none is the same for every part. Nothing has to cross between parts.
Inputs may be any that keep to these rules, and one draw needn't show every extreme that they name: `query_weight`: independent entries, mean zero, of order 3 * 1024 ** -0.5, and up to 20 times that in the columns of some heads.
All inputs are finite; a program needn't handle non-finite values.
Results may differ from the reference program's by a relative error of at most 0.025.
Values may be sent and summed in bfloat16 or wider, within the bound.
No kernel may reach another device: no remote copies, remote signals or barrier semaphores. Data moves between devices by JAX's collectives and lax.ppermute only.
A program may use at most 64 MiB of HBM per device.

```python
import math
import jax
import jax.numpy as jnp
from jax import lax

C_IN = 6
FEAT = 704
D = 1024
HEADS = 8
LAT = 512
DH = 128
H = 224
W = 224


def draw_query_weight(key, part):
    base = jax.random.truncated_normal(key, -5.0, 5.0, (D, D), jnp.float32) * (3.0 / math.sqrt(D))
    strong = jax.random.randint(jax.random.fold_in(key, 11), (), 0, HEADS)
    head_scale = jnp.where(jnp.arange(HEADS) == strong, 16.0, 1.0).astype(jnp.float32)
    base = base * jnp.repeat(head_scale, D // HEADS)[None, :]
    return base.astype(jnp.bfloat16)


def block_scale(stream_key, dims, pieces, smallest, largest):
    def one(position, blocks):
        steps = jax.random.uniform(jax.random.fold_in(jax.random.fold_in(stream_key, 6), position), (blocks,), jnp.float32, smallest / len(pieces), largest / len(pieces))
        return jnp.repeat(jnp.exp(steps), dims[position] // blocks).reshape((-1,) + (1,) * (len(dims) - position - 1))

    level = one(*pieces[0])
    for cut in pieces[1:]:
        level = level * one(*cut)
    return level


def gaussian(stream_key, extent, scale, reach, cuts=(), kind=jnp.bfloat16):
    values = jax.random.normal(stream_key, extent, jnp.float32) * scale
    if len(cuts) > 0:
        values = block_scale(stream_key, extent, cuts, -0.22, 0.18) * values
    return jnp.clip(values, min=-reach, max=reach).astype(kind)


def setup_inputs(seed: int = 0, part: int = 0) -> dict:
    seeds = jax.random.split(jax.random.key(seed), 10)
    part_keys = jax.random.split(jax.random.fold_in(seeds[9], part), 10)
    return {
        "pixels": gaussian(part_keys[0], (H, W, C_IN), 1.0, 6.0, ((0, 16), (1, 4))),
        "conv_weight": gaussian(seeds[1], (9 * C_IN, FEAT), (9 * C_IN) ** -0.5, 0.875),
        "input_gain": jnp.clip(1.0 + 0.1 * jax.random.normal(seeds[2], (FEAT,), jnp.float32), 0.5, 1.5),
        "key_weight": gaussian(seeds[3], (FEAT, D), FEAT ** -0.5, 0.21875),
        "value_weight": gaussian(seeds[4], (FEAT, D), FEAT ** -0.5, 0.21875),
        "latents": gaussian(seeds[5], (LAT, D), 1.0, 6.0),
        "latent_gain": jnp.clip(1.0 + 0.1 * jax.random.normal(seeds[6], (D,), jnp.float32), 0.5, 1.5),
        "query_weight": draw_query_weight(jax.random.fold_in(seeds[9], 71), part),
        "out_weight": gaussian(seeds[8], (D, D), D ** -0.5, 0.1875),
    }


def layer_norm(values, gain):
    mean = lax.optimization_barrier(jnp.mean(values, axis=-1, keepdims=True))
    centred = values - mean
    variance = lax.optimization_barrier(jnp.mean(centred * centred, axis=-1, keepdims=True))
    return centred * lax.rsqrt(variance + 1e-05) * gain

def reference(pixels, conv_weight, input_gain, key_weight, value_weight, latents, latent_gain, query_weight, out_weight):
    height, width = (pixels.shape[0], pixels.shape[1])
    padded = jnp.pad(pixels, ((1, 1), (1, 1), (0, 0)))
    patches = jnp.concatenate([padded[row_off:row_off + height, col_off:col_off + width, :] for row_off in range(3) for col_off in range(3)], axis=-1)
    patches = patches.reshape(height * width, -1)
    features = jnp.dot(patches, conv_weight, preferred_element_type=jnp.float32).astype(jnp.bfloat16)
    normed = layer_norm(features.astype(jnp.float32), input_gain.astype(jnp.float32)).astype(jnp.bfloat16)
    key_rows = jnp.dot(normed, key_weight, preferred_element_type=jnp.float32).astype(jnp.bfloat16)
    value_rows = jnp.dot(normed, value_weight, preferred_element_type=jnp.float32).astype(jnp.bfloat16)
    lat_normed = layer_norm(latents.astype(jnp.float32), latent_gain.astype(jnp.float32)).astype(jnp.bfloat16)
    queries = jnp.dot(lat_normed, query_weight, preferred_element_type=jnp.float32).astype(jnp.bfloat16)
    scale = 1.0 / DH ** 0.5

    def one_head(head):
        start = (head * DH).astype(jnp.int32)
        query_head = lax.dynamic_slice_in_dim(queries, start, DH, 1)
        key_head = lax.dynamic_slice_in_dim(key_rows, start, DH, 1)
        value_head = lax.dynamic_slice_in_dim(value_rows, start, DH, 1)
        scores = jnp.dot(query_head, key_head.T, preferred_element_type=jnp.float32) * scale
        expo = jnp.exp(scores - lax.optimization_barrier(jnp.max(scores, axis=-1, keepdims=True)))
        total = lax.optimization_barrier(jnp.sum(expo, axis=-1))
        summed = jnp.dot(expo.astype(jnp.bfloat16), value_head, preferred_element_type=jnp.float32)
        return summed / total[:, None]
    per_head = lax.map(one_head, jnp.arange(HEADS, dtype=jnp.int32))
    attended = jnp.transpose(per_head, (1, 0, 2)).reshape(LAT, D).astype(jnp.bfloat16)
    result = latents.astype(jnp.float32) + jnp.dot(attended, out_weight, preferred_element_type=jnp.float32)
    return result.astype(jnp.bfloat16)
```

```python
import jax
import jax.numpy as jnp
from jax import lax
from jax.experimental import pallas as pl
from jax.experimental.pallas import tpu as pltpu
from jax.sharding import PartitionSpec as P

HEADS = 8
DH = 128
LANES = 128
SLOT = 64
ONE = 54
MASK = 56
TOP = 57
BIG = 1e30
QUAD = 4
LOG2E = 1.4426950408889634
GROUP = ("gx", "gy")
F32 = jnp.float32
BF16 = jnp.bfloat16


def extended(cells, sides, width):
    for axis, dim in sides:
        count = lax.axis_size(axis)
        ends = count - 1
        head = lax.slice_in_dim(cells, 0, width, axis=dim)
        tail = lax.slice_in_dim(cells, cells.shape[dim] - width, cells.shape[dim], axis=dim)
        cells = jnp.concatenate(
            [
                lax.ppermute(tail, axis, [(i, (i + 1) % count) for i in range(ends)]),
                cells,
                lax.ppermute(head, axis, [((i + 1) % count, i) for i in range(ends)]),
            ],
            axis=dim,
        )
    return cells


def nn(a, b):
    return lax.dot_general(a, b, (((1,), (0,)), ((), ())), preferred_element_type=F32)


def nt(a, b):
    return lax.dot_general(a, b, (((1,), (1,)), ((), ())), preferred_element_type=F32)


def lanes_of(shape):
    return lax.broadcasted_iota(jnp.int32, shape, len(shape) - 1)


def centred_weight(conv_ref):
    weight = conv_ref[...].astype(F32)
    return weight - jnp.mean(weight, axis=-1, keepdims=True)


def split_up(values):
    high = values.astype(BF16)
    return high, (values - high.astype(F32)).astype(BF16)


def through(conv_ref, gain_ref, weight_ref):
    high, low = split_up(centred_weight(conv_ref) * gain_ref[...])
    both = nn(jnp.concatenate([high, low], axis=0), weight_ref[...])
    return both[:SLOT] + both[SLOT:]


def query_kernel(lat_ref, lat_gain_ref, query_ref, conv_ref, gain_ref, key_ref, rows_ref, wide_ref):
    high, low = split_up(centred_weight(conv_ref))
    wide_ref[...] = jnp.concatenate([high, low], axis=0)
    keys = through(conv_ref, gain_ref, key_ref) * (LOG2E / DH**0.5)
    key_high, key_low = split_up(keys)
    values = lat_ref[...].astype(F32)
    centred = values - jnp.mean(values, axis=-1, keepdims=True)
    variance = jnp.mean(centred * centred, axis=-1, keepdims=True)
    normed = (centred * lax.rsqrt(variance + 1e-05) * lat_gain_ref[...]).astype(BF16)
    queries = nn(normed, query_ref[...]).astype(BF16)
    count = values.shape[0]
    lane = lanes_of((count, LANES))
    for head in range(HEADS):
        cut = slice(head * DH, (head + 1) * DH)
        query = jnp.concatenate([queries[:, cut], queries[:, cut]], axis=1)
        key = jnp.concatenate([key_high[:, cut], key_low[:, cut]], axis=1)
        rows = nt(query, jnp.concatenate([key, key], axis=0))
        rows = jnp.where(lane == MASK, -1.0, rows)
        top, rest = split_up(rows)
        rows_ref[head, :, :LANES] = jnp.where(lane < SLOT, top, rest)
        rows_ref[head, :, LANES:] = jnp.where(lane < SLOT, top, jnp.zeros_like(top))


def output_kernel(conv_ref, gain_ref, value_ref, out_ref, both_ref):
    values = through(conv_ref, gain_ref, value_ref)
    for head in range(HEADS):
        cut = slice(head * DH, (head + 1) * DH)
        high, low = split_up(values[:, cut])
        both = nn(jnp.concatenate([high, low], axis=1), jnp.concatenate([out_ref[cut], out_ref[cut]], axis=0))
        both_ref[head * SLOT : (head + 1) * SLOT, :] = both.astype(BF16)


def attend_kernel(block, patch_ref, wide_ref, rows_ref, sums_ref, left_ref, right_ref, expo_ref):
    pixels = patch_ref.shape[0]
    padded = left_ref.shape[0]
    taps = patch_ref.shape[1]
    row = lax.broadcasted_iota(jnp.int32, (taps, LANES), 0)
    lane = lanes_of((taps, LANES))
    copies = jnp.where((lane == row) | (lane == row + SLOT), 1.0, 0.0).astype(BF16)
    patches = nn(patch_ref[...], copies)
    features = nn(patches.astype(BF16), wide_ref[...])
    variance = jnp.mean(features * features, axis=-1, keepdims=True)
    scaled = patches * lax.rsqrt(variance + 1e-05)
    lane = lanes_of((pixels, LANES))
    column = lane % SLOT
    scaled = jnp.where((column == ONE) | (column == ONE + 1), 1.0, scaled)
    high, low = split_up(scaled)
    left_ref[:pixels, :LANES] = high
    left_ref[:pixels, LANES:] = low
    nothing = jnp.zeros((padded - pixels, LANES), F32)
    edge = jnp.where(lanes_of(nothing.shape) == MASK, BIG, nothing).astype(BF16)
    nothing = nothing.astype(BF16)
    left_ref[pixels:, :LANES] = edge
    left_ref[pixels:, LANES:] = nothing
    for part in range(QUAD):
        at = part * padded
        side = part // 2 * LANES
        keep = (lane < SLOT) if part % 2 == 0 else (lane >= SLOT)
        right_ref[at : at + pixels, side : side + LANES] = jnp.where(keep, high, jnp.zeros_like(high))
        right_ref[at : at + pixels, LANES - side : 2 * LANES - side] = jnp.zeros_like(high)
        right_ref[at + pixels : at + padded, :LANES] = nothing
        right_ref[at + pixels : at + padded, LANES:] = nothing

    width = QUAD * SLOT
    wide_lane = lanes_of((block, width))
    wide_column = wide_lane % SLOT

    def step(index, carry):
        at = pl.multiple_of(index * block, block)
        for quad in range(HEADS // QUAD):
            tops = []
            for part in range(QUAD):
                scores = nt(rows_ref[quad * QUAD + part, pl.ds(at, block), :], left_ref[...])
                top = jnp.max(scores, axis=-1, keepdims=True)
                expo = jnp.exp2(scores - top).astype(BF16)
                expo_ref[:, part * padded : (part + 1) * padded] = expo
                tops.append(top)
            sums = nn(expo_ref[...], right_ref[...])
            top = tops[QUAD - 1]
            for part in range(QUAD - 1):
                top = jnp.where(wide_lane < (part + 1) * SLOT, tops[part], top) if part == 0 else jnp.where(
                    (wide_lane >= part * SLOT) & (wide_lane < (part + 1) * SLOT), tops[part], top
                )
            one = top.astype(BF16).astype(F32)
            two = (top - one).astype(BF16).astype(F32)
            three = top - one - two
            sums = jnp.where(wide_column == ONE + 1, sums - sums.astype(BF16).astype(F32), sums)
            sums = jnp.where(wide_column == TOP, one, sums)
            sums = jnp.where(wide_column == TOP + 1, two, sums)
            sums = jnp.where(wide_column == TOP + 2, three, sums)
            sums_ref[pl.ds(at, block), quad * width : (quad + 1) * width] = sums.astype(BF16)
        return carry

    lax.fori_loop(0, sums_ref.shape[0] // block, step, 0)


def combine_kernel(share, parts_ref, both_ref, own_ref, result_ref):
    count = parts_ref.shape[0] // share
    row = lax.broadcasted_iota(jnp.int32, (LANES, LANES), 0)
    lane = lanes_of((LANES, LANES))
    same = row // SLOT == lane // SLOT
    column = row % SLOT
    pick_top = jnp.where(same & (column >= TOP) & (column < TOP + 3), 1.0, 0.0).astype(BF16)
    pick_one = jnp.where(same & (column >= ONE) & (column < ONE + 2), 1.0, 0.0).astype(BF16)
    highs, lows = [], []
    for at in range(0, parts_ref.shape[1], LANES):
        parts = parts_ref[:, at : at + LANES]
        tops = nn(parts, pick_top).reshape(count, share, LANES)
        ones = nn(parts, pick_one).reshape(count, share, LANES)
        factor = jnp.exp2(tops - jnp.max(tops, axis=0, keepdims=True))
        sums = jnp.sum(factor * parts.astype(F32).reshape(count, share, LANES), axis=0)
        total = jnp.sum(factor * ones, axis=0)
        high, low = split_up(sums / total)
        highs.append(high)
        lows.append(low)
    mean = jnp.concatenate([jnp.concatenate(highs, axis=1), jnp.concatenate(lows, axis=1)], axis=0)
    result = nn(mean, both_ref[...])
    result = own_ref[...].astype(F32) + (result[:share] + result[share:])
    result_ref[...] = result.astype(BF16)


def vmem(count):
    return [pl.BlockSpec(memory_space=pltpu.VMEM)] * count


def on_device(
    pixels,
    conv_weight,
    input_gain,
    key_weight,
    value_weight,
    latents,
    latent_gain,
    query_weight,
    out_weight,
):
    tile_rows, tile_cols = (pixels.shape[0], pixels.shape[1])
    count = tile_rows * tile_cols
    padded_count = -(-count // LANES) * LANES
    feat = conv_weight.shape[1]
    lat, width = latents.shape
    conv = jnp.pad(conv_weight, ((0, SLOT - conv_weight.shape[0]), (0, 0)))
    gain = input_gain.reshape(1, feat)

    rows, wide = pl.pallas_call(
        query_kernel,
        out_shape=(
            jax.ShapeDtypeStruct((HEADS, lat, 2 * LANES), BF16),
            jax.ShapeDtypeStruct((2 * SLOT, feat), BF16),
        ),
        in_specs=vmem(6),
        out_specs=tuple(vmem(2)),
        cost_estimate=pl.CostEstimate(flops=2 * lat * width * width * 2, bytes_accessed=4 * width * width, transcendentals=0),
        name="query_rows",
    )(latents, latent_gain.reshape(1, width), query_weight, conv, gain, key_weight)

    padded = extended(pixels, (("gx", 0), ("gy", 1)), 1)
    patches = jnp.concatenate(
        [
            padded[row_off : row_off + tile_rows, col_off : col_off + tile_cols, :]
            for row_off in range(3)
            for col_off in range(3)
        ],
        axis=-1,
    ).reshape(count, -1)

    block = 128
    sums = pl.pallas_call(
        lambda *refs: attend_kernel(block, *refs),
        out_shape=jax.ShapeDtypeStruct((lat, HEADS * SLOT), BF16),
        in_specs=vmem(3),
        out_specs=vmem(1)[0],
        scratch_shapes=[
            pltpu.VMEM((padded_count, 2 * LANES), BF16),
            pltpu.VMEM((QUAD * padded_count, QUAD * SLOT), BF16),
            pltpu.VMEM((block, QUAD * padded_count), BF16),
        ],
        cost_estimate=pl.CostEstimate(flops=4 * lat * HEADS * padded_count * 256, bytes_accessed=4 * width * width, transcendentals=0),
        name="attend",
    )(patches, wide, rows)

    devices = lax.axis_size(GROUP)
    share = lat // devices
    parts = lax.all_to_all(sums.reshape(devices, share, -1), GROUP, 0, 0, tiled=True)
    both = pl.pallas_call(
        output_kernel,
        out_shape=jax.ShapeDtypeStruct((HEADS * SLOT, width), BF16),
        in_specs=vmem(4),
        out_specs=vmem(1)[0],
        cost_estimate=pl.CostEstimate(flops=2 * HEADS * SLOT * width * width, bytes_accessed=4 * width * width, transcendentals=0),
        name="value_output",
    )(conv, gain, value_weight, out_weight)
    own = lax.dynamic_slice_in_dim(latents, lax.axis_index(GROUP) * share, share, 0)
    return pl.pallas_call(
        lambda *refs: combine_kernel(share, *refs),
        out_shape=jax.ShapeDtypeStruct((share, width), BF16),
        in_specs=vmem(3),
        out_specs=vmem(1)[0],
        cost_estimate=pl.CostEstimate(flops=2 * share * width * width, bytes_accessed=2 * width * width, transcendentals=0),
        name="combine",
    )(parts.reshape(lat, -1), both, own)


def solution(mesh):
    return jax.shard_map(
        on_device,
        mesh=mesh,
        in_specs=(P(("ba", "gx"), "gy", None), P(), P(), P(), P(), P(), P(), P(), P()),
        out_specs=P(("ba", "gx", "gy"), None),
        check_vma=False,
    )
```

```python
import functools

import jax
import jax.numpy as jnp
from jax import lax
from jax.experimental import pallas as pl
from jax.experimental.pallas import tpu as pltpu
from jax.sharding import PartitionSpec as P

HEADS = 8
DH = 128
LANES = 128
SUB = 8
TAPS = 9
CELL = 64
LINE = 256
SPAN = 80
ONE, MASK, ONE_TOO = 72, 73, 74
SLOT = 64
TOTAL, TOP = 54, 57
BIG = 1e30
EPS = 1e-05
LOG2E = 1.4426950408889634
GROUP = ("gx", "gy")
F32 = jnp.float32
BF16 = jnp.bfloat16


def product(a, b, left, right):
    return lax.dot_general(a, b, (((left,), (right,)), ((), ())), preferred_element_type=F32)


def nn(a, b):
    return product(a, b, 1, 0)


def nt(a, b):
    return product(a, b, 1, 1)


def tn(a, b):
    return product(a, b, 0, 0)


def iota(shape, dim):
    return lax.broadcasted_iota(jnp.int32, shape, dim)


def split_up(values):
    high = values.astype(BF16)
    return high, (values - high.astype(F32)).astype(BF16)


def thrice(values):
    one = values.astype(BF16)
    rest = values - one.astype(F32)
    two, three = split_up(rest)
    return one, two, three


def pack_kernel(pixel_ref, copies_ref):
    rows, columns, channels = pixel_ref.shape
    values = pixel_ref[...].astype(F32)
    values = jnp.concatenate([values, jnp.zeros((rows, CELL - columns, channels), F32)], axis=1)
    values = values.reshape(rows * CELL, channels).astype(BF16)
    pick = jnp.where(iota((SUB, channels), 0) == iota((SUB, channels), 1), 1.0, 0.0).astype(BF16)
    packed = nt(pick, values).astype(BF16)
    for copy in range(copies_ref.shape[0]):
        copies_ref[copy] = packed


def join_kernel(columns, tiles_ref, strip_ref, first_ref, last_ref):
    tiles, _, width = tiles_ref.shape
    pairs = width // LANES
    lane = iota((pairs * SUB, LANES), 1)
    stacked = [
        jnp.concatenate([tiles_ref[tile, :, pair * LANES : (pair + 1) * LANES].astype(F32) for pair in range(pairs)], axis=0)
        for tile in range(tiles)
    ]
    for parity in range(2):
        halves = []
        for half in range(LINE // LANES):
            line = jnp.zeros((pairs * SUB, LANES), F32)
            for tile in range(tiles):
                start, end = tile * columns - half * LANES, (tile + 1) * columns - half * LANES
                if end <= 0 or start >= LANES:
                    continue
                moved = pltpu.roll(stacked[tile], (start - parity * CELL) % LANES, 1)
                line = jnp.where((lane >= start) & (lane < end), moved, line)
            halves.append(line)
        for pair in range(pairs):
            row = 2 * pair + parity
            for half, line in enumerate(halves):
                at = row * LINE + half * LANES
                strip_ref[:, at : at + LANES] = line[pair * SUB : (pair + 1) * SUB]
    first_ref[...] = strip_ref[:, :LINE].astype(BF16)
    last_ref[...] = strip_ref[:, 2 * pairs * LINE - LINE :].astype(BF16)


def spread_weight(conv_ref, copies):
    channels = conv_ref.shape[0] // TAPS
    shape = (copies, conv_ref.shape[0])
    row, tap = iota(shape, 0), iota(shape, 1)
    place = row % SPAN
    hit = (place // SUB == tap // channels) & (place % SUB == tap % channels) & (row < 3 * SPAN)
    spread = nn(jnp.where(hit, 1.0, 0.0).astype(BF16), conv_ref[...])
    return spread - jnp.mean(spread, axis=-1, keepdims=True)


def query_kernel(
    lat_ref, lat_gain_ref, conv_ref, gain_ref, query_hbm, key_hbm, rows_ref, gram_ref, wide_ref, diag_ref, query_ref, key_ref, sems
):
    width = query_ref.shape[1]
    at = pl.multiple_of(lax.axis_index("gy") * width, width)
    query_copy = pltpu.make_async_copy(query_hbm.at[:, pl.ds(at, width)], query_ref, sems.at[0])
    key_copy = pltpu.make_async_copy(key_hbm.at[:, pl.ds(at, width)], key_ref, sems.at[1])
    query_copy.start()
    key_copy.start()

    weight = spread_weight(conv_ref, LINE)
    feat = weight.shape[1]
    high, low = split_up(weight[:SPAN])
    wide_ref[...] = jnp.concatenate([high, low], axis=0)
    both = jnp.concatenate([high, low], axis=0)
    padding = jnp.zeros((LANES - SPAN, feat), BF16)
    gram = nt(both, jnp.concatenate([high, padding], axis=0)) + nt(both, jnp.concatenate([low, padding], axis=0))
    gram = (gram[:SPAN] + gram[SPAN:]) * (1.0 / feat)
    gram_ref[...] = jnp.concatenate(thrice(gram), axis=0)
    shape = (SPAN, LANES)
    diag = jnp.sum(jnp.where(iota(shape, 0) == iota(shape, 1), gram, 0.0), axis=-1, keepdims=True)
    diag_ref[...] = jnp.broadcast_to(diag, shape)

    values = lat_ref[...].astype(F32)
    centred = values - jnp.mean(values, axis=-1, keepdims=True)
    variance = jnp.mean(centred * centred, axis=-1, keepdims=True)
    gain = lat_gain_ref[...].reshape(1, -1)
    normed = (centred * lax.rsqrt(variance + EPS) * gain).astype(BF16)
    query_copy.wait()
    queries = nn(normed, query_ref[...]).astype(BF16)

    key_copy.wait()
    high, low = split_up(weight * gain_ref[...].reshape(1, -1))
    keys = (nn(high, key_ref[...]) + nn(low, key_ref[...])) * (LOG2E / DH**0.5)
    high, low = split_up(keys)
    count = values.shape[0]
    lane = iota((count, LINE), 1)
    for head in range(width // DH):
        cut = slice(head * DH, (head + 1) * DH)
        query = jnp.concatenate([queries[:, cut], queries[:, cut]], axis=1)
        rows = nt(query, jnp.concatenate([high[:, cut], low[:, cut]], axis=1))
        rows = jnp.where(lane == MASK, -1.0, rows)
        top, rest = split_up(rows)
        rows_ref[head * count : (head + 1) * count, :] = jnp.where((lane >= SPAN) & (lane < 2 * SPAN), rest, top)


def scaled_patches(patches, explicit, gram_ref, wide_ref, diag_ref):
    exact = patches.astype(BF16)
    if explicit:
        high, low = wide_ref[:SPAN], wide_ref[SPAN:]
        features = tn(high, exact) + tn(low, exact)
        variance = jnp.mean(features * features, axis=0, keepdims=True)
        lost = None
    else:
        form = nn(gram_ref[:, :SPAN], exact)
        form = form[:SPAN] + form[SPAN : 2 * SPAN] + form[2 * SPAN :]
        variance = jnp.maximum(jnp.sum(form * patches, axis=0, keepdims=True), 0.0)
        scale = jnp.sum(patches * patches * diag_ref[:, :1], axis=0, keepdims=True)
        lost = jnp.where((variance + EPS) * 128.0 < scale, 1.0, 0.0)
    return patches * lax.rsqrt(variance + EPS), lost


def pixel_block(cells, real):
    del real
    return jnp.concatenate(cells + [jnp.zeros_like(cells[0])], axis=0)


def fill_block(patches, columns, explicit, gram_ref, wide_ref, diag_ref, pixel_ref, at):
    width = patches.shape[1]
    scaled, lost = scaled_patches(patches, explicit, gram_ref, wide_ref, diag_ref)
    row, lane = iota((SPAN, width), 0), iota((SPAN, width), 1)
    real = lane % LINE < columns
    scaled = jnp.where((row == ONE) | (row == ONE_TOO), jnp.where(real, 1.0, 0.0), scaled)
    scaled = jnp.where(row == MASK, jnp.where(real, 0.0, BIG), scaled)
    high, low = split_up(scaled)
    cut = slice(at, at + width)
    pixel_ref[:SPAN, cut] = high
    pixel_ref[SPAN : 2 * SPAN, cut] = high
    pixel_ref[2 * SPAN : 3 * SPAN, cut] = low
    pixel_ref[3 * SPAN :, cut] = jnp.zeros((LINE - 3 * SPAN, width), BF16)
    return lost


def attend(blocks, rows_ref, pixel_ref, score_ref, expo_ref):
    tops, sums = {}, {}
    count = len(blocks)
    for turn in range(count + 2):
        if turn < count:
            cut = slice(blocks[turn][0], blocks[turn][1])
            score_ref[turn % 2, :, : cut.stop - cut.start] = nn(rows_ref[...], pixel_ref[:, cut])
        if 0 <= turn - 1 < count:
            block = turn - 1
            size = blocks[block][1] - blocks[block][0]
            top = jnp.max(score_ref[block % 2, :, :size], axis=-1, keepdims=True)
            expo_ref[block % 2, :, :size] = jnp.exp2(score_ref[block % 2, :, :size] - top).astype(BF16)
            tops[block] = top
        if 0 <= turn - 2 < count:
            block = turn - 2
            cut = slice(blocks[block][0], blocks[block][1])
            sums[block] = nt(expo_ref[block % 2, :, : cut.stop - cut.start], pixel_ref[:LANES, cut])
    return tops, sums


def merged(tops, sums):
    top = functools.reduce(jnp.maximum, tops)
    total = sum(jnp.exp2(t - top) * s for t, s in zip(tops, sums))
    return top, total


def inner_kernel(
    columns, size, strip_ref, rows_ref, gram_ref, wide_ref, diag_ref, sums_ref, tops_ref, pixel_ref, score_ref, expo_ref
):
    width = strip_ref.shape[1]
    inner = width - 2 * LINE
    strip = strip_ref[...]
    shifted = [pltpu.roll(strip, 1, 1), strip, pltpu.roll(strip, width - 1, 1)]
    blocks = [(at, at + size) for at in range(0, inner, size)]

    def run(explicit):
        flags = []
        for at, end in blocks:
            cells = [shifted[tap % 3][:, tap // 3 * LINE + at : tap // 3 * LINE + end] for tap in range(TAPS)]
            patches = jnp.concatenate(cells + [jnp.zeros_like(cells[0])], axis=0)
            flags.append(fill_block(patches, columns, explicit, gram_ref, wide_ref, diag_ref, pixel_ref, at))
        tops, sums = attend(blocks, rows_ref, pixel_ref, score_ref, expo_ref)
        top, total = merged(list(tops.values()), list(sums.values()))
        sums_ref[...] = total
        tops_ref[...] = jnp.broadcast_to(top, tops_ref.shape)
        return flags

    lost = jnp.max(functools.reduce(jnp.maximum, run(False)))

    @pl.when(lost > 0.5)
    def _():
        run(True)


def border_kernel(
    columns,
    strip_ref,
    before_ref,
    after_ref,
    rows_ref,
    gram_ref,
    wide_ref,
    diag_ref,
    inner_sums_ref,
    inner_tops_ref,
    sent_ref,
    pixel_ref,
    score_ref,
    expo_ref,
):
    width = strip_ref.shape[1]
    lines = jnp.concatenate(
        [
            before_ref[...].astype(F32),
            strip_ref[:, : 2 * LINE],
            strip_ref[:, width - 2 * LINE :],
            after_ref[...].astype(F32),
        ],
        axis=1,
    )
    shifted = [pltpu.roll(lines, 1, 1), lines, pltpu.roll(lines, lines.shape[1] - 1, 1)]
    cells = []
    for tap in range(TAPS):
        at = tap // 3 * LINE
        source = shifted[tap % 3]
        cells.append(jnp.concatenate([source[:, at : at + LINE], source[:, at + 3 * LINE : at + 4 * LINE]], axis=1))
    patches = jnp.concatenate(cells + [jnp.zeros_like(cells[0])], axis=0)
    count = sent_ref.shape[0]
    shape = (2 * LANES, LANES)
    row, lane = iota(shape, 0), iota(shape, 1)
    tap = row % LANES
    target = jnp.where((tap < ONE) & (tap % SUB < 6), tap // SUB * 6 + tap % SUB, -1)
    target = jnp.where(tap == ONE, TOTAL, jnp.where(tap == ONE_TOO, TOTAL + 1, target))
    place = jnp.where((target >= 0) & (lane == target + row // LANES * SLOT), 1.0, 0.0).astype(BF16)

    def run(explicit):
        lost = fill_block(patches, columns, explicit, gram_ref, wide_ref, diag_ref, pixel_ref, 0)
        tops, sums = attend([(0, patches.shape[1])], rows_ref, pixel_ref, score_ref, expo_ref)
        top, total = merged([inner_tops_ref[...], tops[0]], [inner_sums_ref[...], sums[0]])
        high = total.astype(BF16)
        low = (total - high.astype(F32)).astype(BF16)
        high = jnp.where(iota(total.shape, 1) == ONE_TOO, low, high)
        placed = nn(jnp.concatenate([high[:count], high[count:]], axis=1), place)
        lane = iota((count, LANES), 1)
        column = lane % SLOT
        one, two, three = thrice(jnp.where(lane < SLOT, top[:count], top[count:]))
        placed = jnp.where(column == TOP, one.astype(F32), placed)
        placed = jnp.where(column == TOP + 1, two.astype(F32), placed)
        placed = jnp.where(column == TOP + 2, three.astype(F32), placed)
        sent_ref[...] = placed.astype(BF16)
        return lost

    lost = jnp.max(run(False))

    @pl.when(lost > 0.5)
    def _():
        run(True)


def output_kernel(conv_ref, gain_ref, value_ref, out_ref, both_ref):
    weight = conv_ref[...].astype(F32)
    weight = (weight - jnp.mean(weight, axis=-1, keepdims=True)) * gain_ref[...].reshape(1, -1)
    weight = jnp.concatenate([weight, jnp.zeros((SLOT - weight.shape[0], weight.shape[1]), F32)], axis=0)
    both = nn(jnp.concatenate(split_up(weight), axis=0), value_ref[...])
    high, low = split_up(both[:SLOT] + both[SLOT:])
    for head in range(HEADS):
        cut = slice(head * DH, (head + 1) * DH)
        both = nn(jnp.concatenate([high[:, cut], low[:, cut]], axis=0), out_ref[cut])
        both_ref[head * SLOT : (head + 1) * SLOT, :] = (both[:SLOT] + both[SLOT:]).astype(BF16)


def combine_kernel(share, parts_ref, both_ref, own_ref, result_ref):
    count = parts_ref.shape[0]
    pairs = both_ref.shape[0] // LANES
    row, lane = iota((LANES, LANES), 0), iota((LANES, LANES), 1)
    same = row // SLOT == lane // SLOT
    column = row % SLOT
    pick_top = jnp.where(same & (column >= TOP) & (column < TOP + 3), 1.0, 0.0).astype(BF16)
    pick_one = jnp.where(same & (column >= TOTAL) & (column < TOTAL + 2), 1.0, 0.0).astype(BF16)
    parts = parts_ref[...]
    shape = (count // (pairs * share), pairs * share, LANES)
    tops = nn(parts, pick_top).reshape(shape)
    ones = nn(parts, pick_one).reshape(shape)
    factor = jnp.exp2(tops - jnp.max(tops, axis=0, keepdims=True))
    sums = jnp.sum(factor * parts.astype(F32).reshape(shape), axis=0)
    total = jnp.sum(factor * ones, axis=0)
    mean = sums / total
    mean = jnp.concatenate([mean[pair * share : (pair + 1) * share] for pair in range(pairs)], axis=1)
    high = mean.astype(BF16).astype(F32)
    result = nn(jnp.concatenate([high, mean - high], axis=0).astype(BF16), both_ref[...])
    result = own_ref[...].astype(F32) + (result[:share] + result[share:])
    result_ref[...] = result.astype(BF16)


def vmem(count):
    return [pl.BlockSpec(memory_space=pltpu.VMEM)] * count


def kernel(body, name, outs, scratch=(), others=0, count=0, cycles=1000):
    single = not isinstance(outs, (list, tuple))
    return pl.pallas_call(
        body,
        out_shape=outs,
        in_specs=vmem(count) + [pl.BlockSpec(memory_space=pl.ANY)] * others,
        out_specs=vmem(1)[0] if single else tuple(vmem(len(outs))),
        scratch_shapes=list(scratch),
        cost_estimate=pl.CostEstimate(flops=cycles * 4096, bytes_accessed=1 << 20, transcendentals=0),
        name=name,
    )


def on_device(
    pixels,
    conv_weight,
    input_gain,
    key_weight,
    value_weight,
    latents,
    latent_gain,
    query_weight,
    out_weight,
):
    tile_rows, tile_cols, _ = pixels.shape
    across, down = lax.axis_size("gy"), lax.axis_size("gx")
    columns = tile_cols * across
    feat = conv_weight.shape[1]
    lat, width = latents.shape
    heads = HEADS // across
    share = lat // (across * down)

    def shape(dims, dtype=BF16):
        return jax.ShapeDtypeStruct(dims, dtype)

    copies = kernel(pack_kernel, "pack", shape((across, SUB, tile_rows * CELL)), count=1)(pixels)
    tiles = lax.all_to_all(copies, "gy", 0, 0, tiled=True)
    rows, gram, wide, diag = kernel(
        query_kernel,
        "query_rows",
        [
            shape((heads * lat, LINE)),
            shape((3 * SPAN, LANES)),
            shape((2 * SPAN, feat)),
            shape((SPAN, LANES), F32),
        ],
        [
            pltpu.VMEM((width, heads * DH), BF16),
            pltpu.VMEM((feat, heads * DH), BF16),
            pltpu.SemaphoreType.DMA((2,)),
        ],
        others=2,
        count=4,
        cycles=6000,
    )(latents, latent_gain, conv_weight, input_gain, query_weight, key_weight)
    both = kernel(
        output_kernel, "value_output", shape((HEADS * SLOT, width)), count=4, cycles=6000
    )(conv_weight, input_gain, value_weight, out_weight)

    strip, first, last = kernel(
        functools.partial(join_kernel, tile_cols),
        "join",
        [shape((SUB, tile_rows * LINE), F32), shape((SUB, LINE)), shape((SUB, LINE))],
        count=1,
    )(tiles)
    before = lax.ppermute(last, "gx", [(i, i + 1) for i in range(down - 1)])
    after = lax.ppermute(first, "gx", [(i + 1, i) for i in range(down - 1)])
    inner = (tile_rows - 2) * LINE
    size = inner // 3
    sums, tops = kernel(
        functools.partial(inner_kernel, columns, size),
        "inner",
        [shape((heads * lat, LANES), F32), shape((heads * lat, LANES), F32)],
        [
            pltpu.VMEM((LINE, inner), BF16),
            pltpu.VMEM((2, heads * lat, size), F32),
            pltpu.VMEM((2, heads * lat, size), BF16),
        ],
        count=5,
        cycles=10000,
    )(strip, rows, gram, wide, diag)
    sent = kernel(
        functools.partial(border_kernel, columns),
        "border",
        shape((lat, heads * SLOT)),
        [
            pltpu.VMEM((LINE, 2 * LINE), BF16),
            pltpu.VMEM((2, heads * lat, 2 * LINE), F32),
            pltpu.VMEM((2, heads * lat, 2 * LINE), BF16),
        ],
        count=9,
        cycles=3000,
    )(strip, before, after, rows, gram, wide, diag, sums, tops)
    devices = across * down
    parts = lax.all_to_all(sent.reshape(devices, share, -1), GROUP, 0, 0, tiled=True)
    own = lax.dynamic_slice_in_dim(latents, lax.axis_index(GROUP) * share, share, 0)
    return kernel(
        functools.partial(combine_kernel, share), "combine", shape((share, width)), count=3
    )(parts.reshape(devices * share, -1), both, own)


def solution(mesh):
    return jax.shard_map(
        on_device,
        mesh=mesh,
        in_specs=(P(("ba", "gx"), "gy", None), P(), P(), P(), P(), P(), P(), P(), P()),
        out_specs=P(("ba", "gx", "gy"), None),
        check_vma=False,
    )
```

```python
import functools

import jax
import jax.numpy as jnp
from jax import lax
from jax.experimental import pallas as pl
from jax.experimental.pallas import tpu as pltpu
from jax.sharding import PartitionSpec as P

HEADS = 8
DH = 128
LANES = 128
SUB = 8
TAPS = 9
CELL = 64
LINE = 256
SPAN = 80
ONE, MASK, ONE_TOO = 72, 73, 74
SLOT = 64
TOTAL, TOP = 54, 57
BIG = 1e30
EPS = 1e-05
LOG2E = 1.4426950408889634
GROUP = ("gx", "gy")
F32 = jnp.float32
BF16 = jnp.bfloat16


def product(a, b, left, right):
    return lax.dot_general(a, b, (((left,), (right,)), ((), ())), preferred_element_type=F32)


def nn(a, b):
    return product(a, b, 1, 0)


def nt(a, b):
    return product(a, b, 1, 1)


def tn(a, b):
    return product(a, b, 0, 0)


def iota(shape, dim):
    return lax.broadcasted_iota(jnp.int32, shape, dim)


def split_up(values):
    high = values.astype(BF16)
    return high, (values - high.astype(F32)).astype(BF16)


def thrice(values):
    one = values.astype(BF16)
    rest = values - one.astype(F32)
    two, three = split_up(rest)
    return one, two, three


def pack_kernel(pixel_ref, copies_ref):
    rows, columns, channels = pixel_ref.shape
    values = pixel_ref[...].astype(F32)
    values = jnp.concatenate([values, jnp.zeros((rows, CELL - columns, channels), F32)], axis=1)
    values = values.reshape(rows * CELL, channels).astype(BF16)
    pick = jnp.where(iota((SUB, channels), 0) == iota((SUB, channels), 1), 1.0, 0.0).astype(BF16)
    packed = nt(pick, values).astype(BF16)
    for copy in range(copies_ref.shape[0]):
        copies_ref[copy] = packed


def join_kernel(columns, tiles_ref, strip_ref, first_ref, last_ref):
    tiles, _, width = tiles_ref.shape
    pairs = width // LANES
    lane = iota((pairs * SUB, LANES), 1)
    stacked = [
        jnp.concatenate([tiles_ref[tile, :, pair * LANES : (pair + 1) * LANES].astype(F32) for pair in range(pairs)], axis=0)
        for tile in range(tiles)
    ]
    for parity in range(2):
        halves = []
        for half in range(LINE // LANES):
            line = jnp.zeros((pairs * SUB, LANES), F32)
            for tile in range(tiles):
                start, end = tile * columns - half * LANES, (tile + 1) * columns - half * LANES
                if end <= 0 or start >= LANES:
                    continue
                moved = pltpu.roll(stacked[tile], (start - parity * CELL) % LANES, 1)
                line = jnp.where((lane >= start) & (lane < end), moved, line)
            halves.append(line)
        for pair in range(pairs):
            row = 2 * pair + parity
            for half, line in enumerate(halves):
                at = row * LINE + half * LANES
                strip_ref[:, at : at + LANES] = line[pair * SUB : (pair + 1) * SUB]
    first_ref[...] = strip_ref[:, :LINE].astype(BF16)
    last_ref[...] = strip_ref[:, 2 * pairs * LINE - LINE :].astype(BF16)


def spread_weight(conv_ref, copies):
    channels = conv_ref.shape[0] // TAPS
    shape = (copies, conv_ref.shape[0])
    row, tap = iota(shape, 0), iota(shape, 1)
    place = row % SPAN
    hit = (place // SUB == tap // channels) & (place % SUB == tap % channels) & (row < 3 * SPAN)
    spread = nn(jnp.where(hit, 1.0, 0.0).astype(BF16), conv_ref[...])
    return spread - jnp.mean(spread, axis=-1, keepdims=True)


def query_kernel(
    lat_ref, lat_gain_ref, conv_ref, gain_ref, query_hbm, key_hbm, rows_ref, gram_ref, wide_ref, diag_ref, query_ref, key_ref, sems
):
    width = query_ref.shape[1]
    at = pl.multiple_of(lax.axis_index("gy") * width, width)
    query_copy = pltpu.make_async_copy(query_hbm.at[:, pl.ds(at, width)], query_ref, sems.at[0])
    key_copy = pltpu.make_async_copy(key_hbm.at[:, pl.ds(at, width)], key_ref, sems.at[1])
    query_copy.start()
    key_copy.start()

    weight = spread_weight(conv_ref, LINE)
    feat = weight.shape[1]
    high, low = split_up(weight[:SPAN])
    wide_ref[...] = jnp.concatenate([high, low], axis=0)
    both = jnp.concatenate([high, low], axis=0)
    padding = jnp.zeros((LANES - SPAN, feat), BF16)
    gram = nt(both, jnp.concatenate([high, padding], axis=0)) + nt(both, jnp.concatenate([low, padding], axis=0))
    gram = (gram[:SPAN] + gram[SPAN:]) * (1.0 / feat)
    gram_ref[...] = jnp.concatenate(thrice(gram), axis=0)
    shape = (SPAN, LANES)
    diag = jnp.sum(jnp.where(iota(shape, 0) == iota(shape, 1), gram, 0.0), axis=-1, keepdims=True)
    diag_ref[...] = jnp.broadcast_to(diag, shape)

    values = lat_ref[...].astype(F32)
    centred = values - jnp.mean(values, axis=-1, keepdims=True)
    variance = jnp.mean(centred * centred, axis=-1, keepdims=True)
    gain = lat_gain_ref[...].reshape(1, -1)
    normed = (centred * lax.rsqrt(variance + EPS) * gain).astype(BF16)
    query_copy.wait()
    queries = nn(normed, query_ref[...]).astype(BF16)

    key_copy.wait()
    high, low = split_up(weight * gain_ref[...].reshape(1, -1))
    keys = (nn(high, key_ref[...]) + nn(low, key_ref[...])) * (LOG2E / DH**0.5)
    high, low = split_up(keys)
    count = values.shape[0]
    lane = iota((count, LINE), 1)
    for head in range(width // DH):
        cut = slice(head * DH, (head + 1) * DH)
        query = jnp.concatenate([queries[:, cut], queries[:, cut]], axis=1)
        rows = nt(query, jnp.concatenate([high[:, cut], low[:, cut]], axis=1))
        rows = jnp.where(lane == MASK, -1.0, rows)
        top, rest = split_up(rows)
        rows_ref[head * count : (head + 1) * count, :] = jnp.where((lane >= SPAN) & (lane < 2 * SPAN), rest, top)


def scaled_patches(patches, explicit, gram_ref, wide_ref, diag_ref):
    exact = patches.astype(BF16)
    if explicit:
        high, low = wide_ref[:SPAN], wide_ref[SPAN:]
        features = tn(high, exact) + tn(low, exact)
        variance = jnp.mean(features * features, axis=0, keepdims=True)
        lost = None
    else:
        form = nn(gram_ref[:, :SPAN], exact)
        form = form[:SPAN] + form[SPAN : 2 * SPAN] + form[2 * SPAN :]
        variance = jnp.maximum(jnp.sum(form * patches, axis=0, keepdims=True), 0.0)
        scale = jnp.sum(patches * patches * diag_ref[:, :1], axis=0, keepdims=True)
        lost = jnp.where((variance + EPS) * 128.0 < scale, 1.0, 0.0)
    return patches * lax.rsqrt(variance + EPS), lost


def pixel_block(cells, real):
    del real
    return jnp.concatenate(cells + [jnp.zeros_like(cells[0])], axis=0)


def fill_block(patches, columns, explicit, gram_ref, wide_ref, diag_ref, pixel_ref, at):
    width = patches.shape[1]
    scaled, lost = scaled_patches(patches, explicit, gram_ref, wide_ref, diag_ref)
    row, lane = iota((SPAN, width), 0), iota((SPAN, width), 1)
    real = lane % LINE < columns
    scaled = jnp.where((row == ONE) | (row == ONE_TOO), jnp.where(real, 1.0, 0.0), scaled)
    scaled = jnp.where(row == MASK, jnp.where(real, 0.0, BIG), scaled)
    high, low = split_up(scaled)
    cut = slice(at, at + width)
    pixel_ref[:SPAN, cut] = high
    pixel_ref[SPAN : 2 * SPAN, cut] = high
    pixel_ref[2 * SPAN : 3 * SPAN, cut] = low
    pixel_ref[3 * SPAN :, cut] = jnp.zeros((LINE - 3 * SPAN, width), BF16)
    return lost


def attend(blocks, rows_ref, pixel_ref, score_ref, expo_ref):
    tops, sums = {}, {}
    count = len(blocks)
    for turn in range(count + 2):
        if turn < count:
            cut = slice(blocks[turn][0], blocks[turn][1])
            score_ref[turn % 2, :, : cut.stop - cut.start] = nn(rows_ref[...], pixel_ref[:, cut])
        if 0 <= turn - 1 < count:
            block = turn - 1
            size = blocks[block][1] - blocks[block][0]
            top = jnp.max(score_ref[block % 2, :, :size], axis=-1, keepdims=True)
            expo_ref[block % 2, :, :size] = jnp.exp2(score_ref[block % 2, :, :size] - top).astype(BF16)
            tops[block] = top
        if 0 <= turn - 2 < count:
            block = turn - 2
            cut = slice(blocks[block][0], blocks[block][1])
            sums[block] = nt(expo_ref[block % 2, :, : cut.stop - cut.start], pixel_ref[:LANES, cut])
    return tops, sums


def merged(tops, sums):
    top = functools.reduce(jnp.maximum, tops)
    total = sum(jnp.exp2(t - top) * s for t, s in zip(tops, sums))
    return top, total


def inner_kernel(
    columns, size, strip_ref, rows_ref, gram_ref, wide_ref, diag_ref, sums_ref, tops_ref, pixel_ref, score_ref, expo_ref
):
    width = strip_ref.shape[1]
    inner = width - 2 * LINE
    strip = strip_ref[...]
    shifted = [pltpu.roll(strip, 1, 1), strip, pltpu.roll(strip, width - 1, 1)]
    blocks = [(at, at + size) for at in range(0, inner, size)]

    def run(explicit):
        flags = []
        for at, end in blocks:
            cells = [shifted[tap % 3][:, tap // 3 * LINE + at : tap // 3 * LINE + end] for tap in range(TAPS)]
            patches = jnp.concatenate(cells + [jnp.zeros_like(cells[0])], axis=0)
            flags.append(fill_block(patches, columns, explicit, gram_ref, wide_ref, diag_ref, pixel_ref, at))
        tops, sums = attend(blocks, rows_ref, pixel_ref, score_ref, expo_ref)
        top, total = merged(list(tops.values()), list(sums.values()))
        sums_ref[...] = total
        tops_ref[...] = jnp.broadcast_to(top, tops_ref.shape)
        return flags

    lost = jnp.max(functools.reduce(jnp.maximum, run(False)))

    @pl.when(lost > 0.5)
    def _():
        run(True)


def border_kernel(
    columns,
    strip_ref,
    before_ref,
    after_ref,
    rows_ref,
    gram_ref,
    wide_ref,
    diag_ref,
    inner_sums_ref,
    inner_tops_ref,
    sent_ref,
    pixel_ref,
    score_ref,
    expo_ref,
):
    width = strip_ref.shape[1]
    lines = jnp.concatenate(
        [
            before_ref[...].astype(F32),
            strip_ref[:, : 2 * LINE],
            strip_ref[:, width - 2 * LINE :],
            after_ref[...].astype(F32),
        ],
        axis=1,
    )
    shifted = [pltpu.roll(lines, 1, 1), lines, pltpu.roll(lines, lines.shape[1] - 1, 1)]
    cells = []
    for tap in range(TAPS):
        at = tap // 3 * LINE
        source = shifted[tap % 3]
        cells.append(jnp.concatenate([source[:, at : at + LINE], source[:, at + 3 * LINE : at + 4 * LINE]], axis=1))
    patches = jnp.concatenate(cells + [jnp.zeros_like(cells[0])], axis=0)
    count = sent_ref.shape[0]
    shape = (2 * LANES, LANES)
    row, lane = iota(shape, 0), iota(shape, 1)
    tap = row % LANES
    target = jnp.where((tap < ONE) & (tap % SUB < 6), tap // SUB * 6 + tap % SUB, -1)
    target = jnp.where(tap == ONE, TOTAL, jnp.where(tap == ONE_TOO, TOTAL + 1, target))
    place = jnp.where((target >= 0) & (lane == target + row // LANES * SLOT), 1.0, 0.0).astype(BF16)

    def run(explicit):
        lost = fill_block(patches, columns, explicit, gram_ref, wide_ref, diag_ref, pixel_ref, 0)
        tops, sums = attend([(0, patches.shape[1])], rows_ref, pixel_ref, score_ref, expo_ref)
        top, total = merged([inner_tops_ref[...], tops[0]], [inner_sums_ref[...], sums[0]])
        high = total.astype(BF16)
        low = (total - high.astype(F32)).astype(BF16)
        high = jnp.where(iota(total.shape, 1) == ONE_TOO, low, high)
        placed = nn(jnp.concatenate([high[:count], high[count:]], axis=1), place)
        lane = iota((count, LANES), 1)
        column = lane % SLOT
        one, two, three = thrice(jnp.where(lane < SLOT, top[:count], top[count:]))
        placed = jnp.where(column == TOP, one.astype(F32), placed)
        placed = jnp.where(column == TOP + 1, two.astype(F32), placed)
        placed = jnp.where(column == TOP + 2, three.astype(F32), placed)
        sent_ref[...] = placed.astype(BF16)
        return lost

    lost = jnp.max(run(False))

    @pl.when(lost > 0.5)
    def _():
        run(True)


def output_kernel(conv_ref, gain_ref, value_ref, out_ref, both_ref):
    weight = conv_ref[...].astype(F32)
    weight = (weight - jnp.mean(weight, axis=-1, keepdims=True)) * gain_ref[...].reshape(1, -1)
    weight = jnp.concatenate([weight, jnp.zeros((SLOT - weight.shape[0], weight.shape[1]), F32)], axis=0)
    both = nn(jnp.concatenate(split_up(weight), axis=0), value_ref[...])
    high, low = split_up(both[:SLOT] + both[SLOT:])
    for head in range(HEADS):
        cut = slice(head * DH, (head + 1) * DH)
        both = nn(jnp.concatenate([high[:, cut], low[:, cut]], axis=0), out_ref[cut])
        both_ref[head * SLOT : (head + 1) * SLOT, :] = (both[:SLOT] + both[SLOT:]).astype(BF16)


def combine_kernel(share, parts_ref, both_ref, own_ref, result_ref):
    count = parts_ref.shape[0]
    pairs = both_ref.shape[0] // LANES
    row, lane = iota((LANES, LANES), 0), iota((LANES, LANES), 1)
    same = row // SLOT == lane // SLOT
    column = row % SLOT
    pick_top = jnp.where(same & (column >= TOP) & (column < TOP + 3), 1.0, 0.0).astype(BF16)
    pick_one = jnp.where(same & (column >= TOTAL) & (column < TOTAL + 2), 1.0, 0.0).astype(BF16)
    parts = parts_ref[...]
    shape = (count // (pairs * share), pairs * share, LANES)
    tops = nn(parts, pick_top).reshape(shape)
    ones = nn(parts, pick_one).reshape(shape)
    factor = jnp.exp2(tops - jnp.max(tops, axis=0, keepdims=True))
    sums = jnp.sum(factor * parts.astype(F32).reshape(shape), axis=0)
    total = jnp.sum(factor * ones, axis=0)
    mean = sums / total
    mean = jnp.concatenate([mean[pair * share : (pair + 1) * share] for pair in range(pairs)], axis=1)
    high = mean.astype(BF16).astype(F32)
    result = nn(jnp.concatenate([high, mean - high], axis=0).astype(BF16), both_ref[...])
    result = own_ref[...].astype(F32) + (result[:share] + result[share:])
    result_ref[...] = result.astype(BF16)


def vmem(count):
    return [pl.BlockSpec(memory_space=pltpu.VMEM)] * count


def kernel(body, name, outs, scratch=(), others=0, count=0, cycles=1000, room=4):
    single = not isinstance(outs, (list, tuple))
    return pl.pallas_call(
        body,
        out_shape=outs,
        in_specs=vmem(count) + [pl.BlockSpec(memory_space=pltpu.HBM)] * others,
        out_specs=vmem(1)[0] if single else tuple(vmem(len(outs))),
        scratch_shapes=list(scratch),
        cost_estimate=pl.CostEstimate(flops=cycles * 4096, bytes_accessed=1 << 20, transcendentals=0),
        compiler_params=pltpu.CompilerParams(vmem_limit_bytes=room << 20),
        name=name,
    )


def on_device(
    pixels,
    conv_weight,
    input_gain,
    key_weight,
    value_weight,
    latents,
    latent_gain,
    query_weight,
    out_weight,
):
    tile_rows, tile_cols, _ = pixels.shape
    across, down = lax.axis_size("gy"), lax.axis_size("gx")
    columns = tile_cols * across
    feat = conv_weight.shape[1]
    lat, width = latents.shape
    heads = HEADS // across
    share = lat // (across * down)

    def shape(dims, dtype=BF16):
        return jax.ShapeDtypeStruct(dims, dtype)

    copies = kernel(pack_kernel, "pack", shape((across, SUB, tile_rows * CELL)), count=1)(pixels)
    tiles = lax.all_to_all(copies, "gy", 0, 0, tiled=True)
    rows, gram, wide, diag = kernel(
        query_kernel,
        "query_rows",
        [
            shape((heads * lat, LINE)),
            shape((3 * SPAN, LANES)),
            shape((2 * SPAN, feat)),
            shape((SPAN, LANES), F32),
        ],
        [
            pltpu.VMEM((width, heads * DH), BF16),
            pltpu.VMEM((feat, heads * DH), BF16),
            pltpu.SemaphoreType.DMA((2,)),
        ],
        others=2,
        count=4,
        cycles=6000,
        room=14,
    )(latents, latent_gain, conv_weight, input_gain, query_weight, key_weight)
    both = kernel(
        output_kernel, "value_output", shape((HEADS * SLOT, width)), count=4, cycles=6000, room=10
    )(conv_weight, input_gain, value_weight, out_weight)

    strip, first, last = kernel(
        functools.partial(join_kernel, tile_cols),
        "join",
        [shape((SUB, tile_rows * LINE), F32), shape((SUB, LINE)), shape((SUB, LINE))],
        count=1,
    )(tiles)
    before = lax.ppermute(last, "gx", [(i, i + 1) for i in range(down - 1)])
    after = lax.ppermute(first, "gx", [(i + 1, i) for i in range(down - 1)])
    inner = (tile_rows - 2) * LINE
    size = inner // 3
    sums, tops = kernel(
        functools.partial(inner_kernel, columns, size),
        "inner",
        [shape((heads * lat, LANES), F32), shape((heads * lat, LANES), F32)],
        [
            pltpu.VMEM((LINE, inner), BF16),
            pltpu.VMEM((2, heads * lat, size), F32),
            pltpu.VMEM((2, heads * lat, size), BF16),
        ],
        count=5,
        cycles=10000,
        room=34,
    )(strip, rows, gram, wide, diag)
    sent = kernel(
        functools.partial(border_kernel, columns),
        "border",
        shape((lat, heads * SLOT)),
        [
            pltpu.VMEM((LINE, 2 * LINE), BF16),
            pltpu.VMEM((2, heads * lat, 2 * LINE), F32),
            pltpu.VMEM((2, heads * lat, 2 * LINE), BF16),
        ],
        count=9,
        cycles=3000,
        room=16,
    )(strip, before, after, rows, gram, wide, diag, sums, tops)
    devices = across * down
    parts = lax.all_to_all(sent.reshape(devices, share, -1), GROUP, 0, 0, tiled=True)
    own = lax.dynamic_slice_in_dim(latents, lax.axis_index(GROUP) * share, share, 0)
    return kernel(
        functools.partial(combine_kernel, share), "combine", shape((share, width)), count=3, room=6
    )(parts.reshape(devices * share, -1), both, own)


def solution(mesh):
    return jax.shard_map(
        on_device,
        mesh=mesh,
        in_specs=(P(("ba", "gx"), "gy", None), P(), P(), P(), P(), P(), P(), P(), P()),
        out_specs=P(("ba", "gx", "gy"), None),
        check_vma=False,
    )
```

```python
import functools

import jax
import jax.numpy as jnp
from jax import lax
from jax.experimental import pallas as pl
from jax.experimental.pallas import tpu as pltpu
from jax.sharding import PartitionSpec as P

HEADS = 8
DH = 128
LANES = 128
SUB = 8
TAPS = 9
CELL = 64
LINE = 256
SPAN = 80
ONE, MASK, ONE_TOO = 72, 73, 74
SLOT = 64
TOTAL, TOP = 54, 57
BIG = 1e30
EPS = 1e-05
LOG2E = 1.4426950408889634
GROUP = ("gx", "gy")
F32 = jnp.float32
BF16 = jnp.bfloat16


def product(a, b, left, right):
    return lax.dot_general(a, b, (((left,), (right,)), ((), ())), preferred_element_type=F32)


def nn(a, b):
    return product(a, b, 1, 0)


def nt(a, b):
    return product(a, b, 1, 1)


def tn(a, b):
    return product(a, b, 0, 0)


def iota(shape, dim):
    return lax.broadcasted_iota(jnp.int32, shape, dim)


def split_up(values):
    high = values.astype(BF16)
    return high, (values - high.astype(F32)).astype(BF16)


def thrice(values):
    one = values.astype(BF16)
    rest = values - one.astype(F32)
    two, three = split_up(rest)
    return one, two, three


def pack_kernel(pixel_ref, copies_ref, plane_ref):
    channels, rows, columns = pixel_ref.shape
    pitch = plane_ref.shape[0] // SUB
    plane_ref[...] = jnp.zeros(plane_ref.shape, F32)
    for channel in range(channels):
        plane_ref[channel * pitch : channel * pitch + rows, :columns] = pixel_ref[channel].astype(F32)
    for pair in range(rows // 2):
        even = plane_ref[pl.ds(2 * pair, SUB, stride=pitch), :]
        odd = plane_ref[pl.ds(2 * pair + 1, SUB, stride=pitch), :]
        packed = (even + pltpu.roll(odd, CELL, 1)).astype(BF16)
        for copy in range(copies_ref.shape[0]):
            copies_ref[copy, :, pair * LANES : (pair + 1) * LANES] = packed


def join_kernel(columns, tiles_ref, strip_ref, first_ref, last_ref):
    tiles, _, width = tiles_ref.shape
    pairs = width // LANES
    lane = iota((pairs * SUB, LANES), 1)
    stacked = [
        jnp.concatenate([tiles_ref[tile, :, pair * LANES : (pair + 1) * LANES].astype(F32) for pair in range(pairs)], axis=0)
        for tile in range(tiles)
    ]
    for parity in range(2):
        halves = []
        for half in range(LINE // LANES):
            line = jnp.zeros((pairs * SUB, LANES), F32)
            for tile in range(tiles):
                start, end = tile * columns - half * LANES, (tile + 1) * columns - half * LANES
                if end <= 0 or start >= LANES:
                    continue
                moved = pltpu.roll(stacked[tile], (start - parity * CELL) % LANES, 1)
                line = jnp.where((lane >= start) & (lane < end), moved, line)
            halves.append(line)
        for pair in range(pairs):
            row = 2 * pair + parity
            for half, line in enumerate(halves):
                at = row * LINE + half * LANES
                strip_ref[:, at : at + LANES] = line[pair * SUB : (pair + 1) * SUB]
    first_ref[...] = strip_ref[:, :LINE].astype(BF16)
    last_ref[...] = strip_ref[:, 2 * pairs * LINE - LINE :].astype(BF16)


def spread_weight(conv_ref, copies):
    channels = conv_ref.shape[0] // TAPS
    shape = (copies, conv_ref.shape[0])
    row, tap = iota(shape, 0), iota(shape, 1)
    place = row % SPAN
    hit = (place // SUB == tap // channels) & (place % SUB == tap % channels) & (row < 3 * SPAN)
    spread = nn(jnp.where(hit, 1.0, 0.0).astype(BF16), conv_ref[...])
    return spread - jnp.mean(spread, axis=-1, keepdims=True)


def query_kernel(
    conv_ref, gain_ref, lat_gain_ref, lat_hbm, query_hbm, key_hbm, rows_ref, lat_ref, query_ref, key_ref, sems
):
    lat_copy = pltpu.make_async_copy(lat_hbm.at[:, lax.axis_index("gy")], lat_ref, sems.at[0])
    query_copy = pltpu.make_async_copy(query_hbm, query_ref, sems.at[1])
    key_copy = pltpu.make_async_copy(key_hbm, key_ref, sems.at[2])
    lat_copy.start()
    query_copy.start()
    key_copy.start()

    weight = spread_weight(conv_ref, SPAN)
    feat = weight.shape[1]
    high, low = split_up(weight)
    both = jnp.concatenate([high, low], axis=0)
    held = HEADS * lat_ref.shape[0] * lat_ref.shape[1]
    for part, at in enumerate(range(0, feat, LINE)):
        end = min(at + LINE, feat)
        first = held + LINE + part * 2 * SPAN
        rows_ref[first : first + 2 * SPAN, : end - at] = both[:, at:end]
    padding = jnp.zeros((LANES - SPAN, feat), BF16)
    gram = nt(both, jnp.concatenate([high, padding], axis=0)) + nt(both, jnp.concatenate([low, padding], axis=0))
    gram = (gram[:SPAN] + gram[SPAN:]) * (1.0 / feat)
    rows_ref[held : held + 3 * SPAN, :LANES] = jnp.concatenate(thrice(gram), axis=0)

    lat_copy.wait()
    values = lat_ref[...].astype(F32)
    values = values.reshape(values.shape[0] * values.shape[1], values.shape[2])
    centred = values - jnp.mean(values, axis=-1, keepdims=True)
    variance = jnp.mean(centred * centred, axis=-1, keepdims=True)
    gain = lat_gain_ref[...].reshape(1, -1)
    normed = (centred * lax.rsqrt(variance + EPS) * gain).astype(BF16)
    query_copy.wait()
    queries = nn(normed, query_ref[...]).astype(BF16)

    key_copy.wait()
    keys = nn(jnp.concatenate(split_up(weight * gain_ref[...].reshape(1, -1)), axis=0), key_ref[...])
    high, low = split_up((keys[:SPAN] + keys[SPAN:]) * (LOG2E / DH**0.5))
    count = values.shape[0]
    lane = iota((count, LINE), 1)
    padding = jnp.zeros((LINE - 3 * SPAN, 2 * DH), BF16)
    for head in range(HEADS):
        cut = slice(head * DH, (head + 1) * DH)
        query = jnp.concatenate([queries[:, cut], queries[:, cut]], axis=1)
        key = jnp.concatenate([high[:, cut], low[:, cut]], axis=1)
        rows = nt(query, jnp.concatenate([key, key, key, padding], axis=0))
        rows = jnp.where(lane == MASK, -1.0, rows)
        top, rest = split_up(rows)
        rows_ref[head * count : (head + 1) * count, :] = jnp.where((lane >= SPAN) & (lane < 2 * SPAN), rest, top)


def table_rows(feat):
    return LINE + -(-feat // LINE) * 2 * SPAN


def scaled_patches(patches, explicit, feat, rows_ref):
    exact = patches.astype(BF16)
    held = rows_ref.shape[0] - table_rows(feat)
    if explicit:
        total = 0.0
        for part, at in enumerate(range(0, feat, LINE)):
            end = min(at + LINE, feat)
            first = held + LINE + part * 2 * SPAN
            wide = rows_ref[first : first + 2 * SPAN, : end - at]
            features = tn(wide[:SPAN], exact) + tn(wide[SPAN:], exact)
            total = total + jnp.sum(features * features, axis=0, keepdims=True)
        variance = total * (1.0 / feat)
        lost = None
    else:
        gram = rows_ref[held : held + 3 * SPAN, :LANES]
        form = nn(gram[:, :SPAN], exact)
        form = form[:SPAN] + form[SPAN : 2 * SPAN] + form[2 * SPAN :]
        variance = jnp.maximum(jnp.sum(form * patches, axis=0, keepdims=True), 0.0)
        shape = (SPAN, LANES)
        diag = jnp.where(iota(shape, 0) == iota(shape, 1), gram[:SPAN].astype(F32), 0.0)
        diag = jnp.sum(diag, axis=-1, keepdims=True)
        scale = jnp.sum(patches * patches * diag, axis=0, keepdims=True)
        lost = jnp.where((variance + EPS) * 128.0 < scale, 1.0, 0.0)
    return patches * lax.rsqrt(variance + EPS), lost


def fill_block(patches, columns, explicit, feat, rows_ref, pixel_ref, at):
    width = patches.shape[1]
    scaled, lost = scaled_patches(patches, explicit, feat, rows_ref)
    row, lane = iota((SPAN, width), 0), iota((SPAN, width), 1)
    real = lane % LINE < columns
    scaled = jnp.where((row == ONE) | (row == ONE_TOO), jnp.where(real, 1.0, 0.0), scaled)
    scaled = jnp.where(row == MASK, jnp.where(real, 0.0, BIG), scaled)
    high, low = split_up(scaled)
    cut = slice(at, at + width)
    pixel_ref[:SPAN, cut] = high
    pixel_ref[SPAN : 2 * SPAN, cut] = high
    pixel_ref[2 * SPAN : 3 * SPAN, cut] = low
    pixel_ref[3 * SPAN :, cut] = jnp.zeros((LINE - 3 * SPAN, width), BF16)
    return lost


def attend(blocks, rows_ref, pixel_ref, score_ref, expo_ref):
    tops, sums = {}, {}
    count = len(blocks)
    for turn in range(count + 2):
        if turn < count:
            cut = slice(blocks[turn][0], blocks[turn][1])
            score_ref[turn % 2, :, : cut.stop - cut.start] = nn(rows_ref[: score_ref.shape[1]], pixel_ref[:, cut])
        if 0 <= turn - 1 < count:
            block = turn - 1
            size = blocks[block][1] - blocks[block][0]
            top = jnp.max(score_ref[block % 2, :, :size], axis=-1, keepdims=True)
            expo_ref[block % 2, :, :size] = jnp.exp2(score_ref[block % 2, :, :size] - top).astype(BF16)
            tops[block] = top
        if 0 <= turn - 2 < count:
            block = turn - 2
            cut = slice(blocks[block][0], blocks[block][1])
            sums[block] = nt(expo_ref[block % 2, :, : cut.stop - cut.start], pixel_ref[:LANES, cut])
    return tops, sums


def merged(tops, sums):
    top = functools.reduce(jnp.maximum, tops)
    total = sum(jnp.exp2(t - top) * s for t, s in zip(tops, sums))
    return top, total


def inner_kernel(
    columns, size, feat, strip_ref, rows_ref, sums_ref, tops_ref, pixel_ref, score_ref, expo_ref
):
    width = strip_ref.shape[1]
    inner = width - 2 * LINE
    strip = strip_ref[...]
    shifted = [pltpu.roll(strip, 1, 1), strip, pltpu.roll(strip, width - 1, 1)]
    blocks = [(at, at + size) for at in range(0, inner, size)]

    def run(explicit):
        flags = []
        for at, end in blocks:
            cells = [shifted[tap % 3][:, tap // 3 * LINE + at : tap // 3 * LINE + end] for tap in range(TAPS)]
            patches = jnp.concatenate(cells + [jnp.zeros_like(cells[0])], axis=0)
            flags.append(fill_block(patches, columns, explicit, feat, rows_ref, pixel_ref, at))
        tops, sums = attend(blocks, rows_ref, pixel_ref, score_ref, expo_ref)
        top, total = merged(list(tops.values()), list(sums.values()))
        sums_ref[...] = total
        tops_ref[...] = jnp.broadcast_to(top, tops_ref.shape)
        return flags

    lost = jnp.max(functools.reduce(jnp.maximum, run(False)))

    @pl.when(lost > 0.5)
    def _():
        run(True)


def border_kernel(
    columns,
    feat,
    strip_ref,
    before_ref,
    after_ref,
    rows_ref,
    inner_sums_ref,
    inner_tops_ref,
    sent_ref,
    pixel_ref,
    score_ref,
    expo_ref,
):
    width = strip_ref.shape[1]
    lines = jnp.concatenate(
        [
            before_ref[...].astype(F32),
            strip_ref[:, : 2 * LINE],
            strip_ref[:, width - 2 * LINE :],
            after_ref[...].astype(F32),
        ],
        axis=1,
    )
    shifted = [pltpu.roll(lines, 1, 1), lines, pltpu.roll(lines, lines.shape[1] - 1, 1)]
    cells = []
    for tap in range(TAPS):
        at = tap // 3 * LINE
        source = shifted[tap % 3]
        cells.append(jnp.concatenate([source[:, at : at + LINE], source[:, at + 3 * LINE : at + 4 * LINE]], axis=1))
    patches = jnp.concatenate(cells + [jnp.zeros_like(cells[0])], axis=0)
    count = sent_ref.shape[0]
    shape = (2 * LANES, LANES)
    row, lane = iota(shape, 0), iota(shape, 1)
    tap = row % LANES
    target = jnp.where((tap < ONE) & (tap % SUB < 6), tap // SUB * 6 + tap % SUB, -1)
    target = jnp.where(tap == ONE, TOTAL, jnp.where(tap == ONE_TOO, TOTAL + 1, target))
    place = jnp.where((target >= 0) & (lane == target + row // LANES * SLOT), 1.0, 0.0).astype(BF16)

    def run(explicit):
        lost = fill_block(patches, columns, explicit, feat, rows_ref, pixel_ref, 0)
        tops, sums = attend([(0, patches.shape[1])], rows_ref, pixel_ref, score_ref, expo_ref)
        top, total = merged([inner_tops_ref[...], tops[0]], [inner_sums_ref[...], sums[0]])
        high = total.astype(BF16)
        low = (total - high.astype(F32)).astype(BF16)
        high = jnp.where(iota(total.shape, 1) == ONE_TOO, low, high)

        def side(values, odd):
            heads = range(odd, HEADS, 2)
            return jnp.concatenate([values[head * count : (head + 1) * count] for head in heads], axis=0)

        placed = nn(jnp.concatenate([side(high, 0), side(high, 1)], axis=1), place)
        lane = iota(placed.shape, 1)
        column = lane % SLOT
        one, two, three = thrice(jnp.where(lane < SLOT, side(top, 0), side(top, 1)))
        placed = jnp.where(column == TOP, one.astype(F32), placed)
        placed = jnp.where(column == TOP + 1, two.astype(F32), placed)
        placed = jnp.where(column == TOP + 2, three.astype(F32), placed).astype(BF16)
        for pair in range(HEADS // 2):
            sent_ref[:, pair * LANES : (pair + 1) * LANES] = placed[pair * count : (pair + 1) * count]
        return lost

    lost = jnp.max(run(False))

    @pl.when(lost > 0.5)
    def _():
        run(True)


def output_kernel(conv_ref, gain_ref, value_ref, out_ref, both_ref):
    weight = conv_ref[...].astype(F32)
    weight = (weight - jnp.mean(weight, axis=-1, keepdims=True)) * gain_ref[...].reshape(1, -1)
    weight = jnp.concatenate([weight, jnp.zeros((SLOT - weight.shape[0], weight.shape[1]), F32)], axis=0)
    both = nn(jnp.concatenate(split_up(weight), axis=0), value_ref[...])
    high, low = split_up(both[:SLOT] + both[SLOT:])
    for head in range(HEADS):
        cut = slice(head * DH, (head + 1) * DH)
        both = nn(jnp.concatenate([high[:, cut], low[:, cut]], axis=0), out_ref[cut])
        both_ref[head * SLOT : (head + 1) * SLOT, :] = (both[:SLOT] + both[SLOT:]).astype(BF16)


def combine_kernel(parts_ref, both_ref, own_ref, result_ref):
    count, share, width = parts_ref.shape
    row, lane = iota((LANES, LANES), 0), iota((LANES, LANES), 1)
    same = row // SLOT == lane // SLOT
    column = row % SLOT
    pick_top = jnp.where(same & (column >= TOP) & (column < TOP + 3), 1.0, 0.0).astype(BF16)
    pick_one = jnp.where(same & (column >= TOTAL) & (column < TOTAL + 2), 1.0, 0.0).astype(BF16)
    means = []
    for at in range(0, width, LANES):
        values = parts_ref[:, :, at : at + LANES].astype(F32)
        parts = values.reshape(count * share, LANES).astype(BF16)
        tops = nn(parts, pick_top).reshape(values.shape)
        ones = nn(parts, pick_one).reshape(values.shape)
        factor = jnp.exp2(tops - jnp.max(tops, axis=0, keepdims=True))
        means.append(jnp.sum(factor * values, axis=0) / jnp.sum(factor * ones, axis=0))
    mean = jnp.concatenate(means, axis=1)
    high = mean.astype(BF16).astype(F32)
    result = nn(jnp.concatenate([high, mean - high], axis=0).astype(BF16), both_ref[...])
    result = own_ref[...].astype(F32) + (result[:share] + result[share:])
    result_ref[...] = result.astype(BF16)


def vmem(count):
    return [pl.BlockSpec(memory_space=pltpu.VMEM)] * count


def kernel(body, name, outs, scratch=(), others=0, count=0, cycles=1000, room=4):
    single = not isinstance(outs, (list, tuple))
    return pl.pallas_call(
        body,
        out_shape=outs,
        in_specs=vmem(count) + [pl.BlockSpec(memory_space=pltpu.HBM)] * others,
        out_specs=vmem(1)[0] if single else tuple(vmem(len(outs))),
        scratch_shapes=list(scratch),
        cost_estimate=pl.CostEstimate(flops=cycles * 4096, bytes_accessed=1 << 20, transcendentals=0),
        compiler_params=pltpu.CompilerParams(vmem_limit_bytes=room << 20),
        name=name,
    )


def on_device(
    pixels,
    conv_weight,
    input_gain,
    key_weight,
    value_weight,
    latents,
    latent_gain,
    query_weight,
    out_weight,
):
    tile_rows, tile_cols, _ = pixels.shape
    across, down = lax.axis_size("gy"), lax.axis_size("gx")
    columns = tile_cols * across
    feat = conv_weight.shape[1]
    lat, width = latents.shape
    share = lat // (across * down)
    held = lat // across

    def shape(dims, dtype=BF16):
        return jax.ShapeDtypeStruct(dims, dtype)

    copies = kernel(
        pack_kernel,
        "pack",
        shape((across, SUB, tile_rows * CELL)),
        [pltpu.VMEM((SUB * 16, LANES), F32)],
        count=1,
    )(pixels.transpose(2, 0, 1))
    tiles = lax.all_to_all(copies, "gy", 0, 0, tiled=True)
    rows = kernel(
        query_kernel,
        "query_rows",
        shape((HEADS * held + table_rows(feat), LINE)),
        [
            pltpu.VMEM((down, share, width), BF16),
            pltpu.VMEM(query_weight.shape, BF16),
            pltpu.VMEM(key_weight.shape, BF16),
            pltpu.SemaphoreType.DMA((3,)),
        ],
        others=3,
        count=3,
        cycles=6000,
        room=60,
    )(conv_weight, input_gain, latent_gain, latents.reshape(down, across, share, width), query_weight, key_weight)
    both = kernel(
        output_kernel, "value_output", shape((HEADS * SLOT, width)), count=4, cycles=6000, room=10
    )(conv_weight, input_gain, value_weight, out_weight)

    tiles, rows = lax.optimization_barrier((tiles, rows))
    strip, first, last = kernel(
        functools.partial(join_kernel, tile_cols),
        "join",
        [shape((SUB, tile_rows * LINE), F32), shape((SUB, LINE)), shape((SUB, LINE))],
        count=1,
        cycles=200000,
    )(tiles)
    before = lax.ppermute(last, "gx", [(i, i + 1) for i in range(down - 1)])
    after = lax.ppermute(first, "gx", [(i + 1, i) for i in range(down - 1)])
    inner = (tile_rows - 2) * LINE
    size = inner // 3
    sums, tops = kernel(
        functools.partial(inner_kernel, columns, size, feat),
        "inner",
        [shape((HEADS * held, LANES), F32), shape((HEADS * held, LANES), F32)],
        [
            pltpu.VMEM((LINE, inner), BF16),
            pltpu.VMEM((2, HEADS * held, size), F32),
            pltpu.VMEM((2, HEADS * held, size), BF16),
        ],
        count=2,
        cycles=10000,
        room=34,
    )(strip, rows)
    sent = kernel(
        functools.partial(border_kernel, columns, feat),
        "border",
        shape((held, HEADS * SLOT)),
        [
            pltpu.VMEM((LINE, 2 * LINE), BF16),
            pltpu.VMEM((2, HEADS * held, 2 * LINE), F32),
            pltpu.VMEM((2, HEADS * held, 2 * LINE), BF16),
        ],
        count=6,
        cycles=3000,
        room=16,
    )(strip, before, after, rows, sums, tops)
    parts = lax.all_to_all(sent.reshape(down, share, -1), "gx", 0, 0, tiled=True)
    own = lax.dynamic_slice_in_dim(latents, lax.axis_index(GROUP) * share, share, 0)
    return kernel(combine_kernel, "combine", shape((share, width)), count=3, room=6)(parts, both, own)


def solution(mesh):
    return jax.shard_map(
        on_device,
        mesh=mesh,
        in_specs=(P(("ba", "gx"), "gy", None), P(), P(), P(), P(), P(), P(), P(), P()),
        out_specs=P(("ba", "gx", "gy"), None),
        check_vma=False,
    )
```

```python
import functools

import jax
import jax.numpy as jnp
from jax import lax
from jax.experimental import pallas as pl
from jax.experimental.pallas import tpu as pltpu
from jax.sharding import PartitionSpec as P

HEADS = 8
DH = 128
LANES = 128
SUB = 8
TAPS = 9
CELL = 64
LINE = 256
SPAN = 80
ONE, MASK, ONE_TOO = 72, 73, 74
SLOT = 64
TOTAL, TOP = 54, 57
BIG = 1e30
EPS = 1e-05
LOG2E = 1.4426950408889634
GROUP = ("gx", "gy")
F32 = jnp.float32
BF16 = jnp.bfloat16


def product(a, b, left, right):
    return lax.dot_general(a, b, (((left,), (right,)), ((), ())), preferred_element_type=F32)


def nn(a, b):
    return product(a, b, 1, 0)


def nt(a, b):
    return product(a, b, 1, 1)


def tn(a, b):
    return product(a, b, 0, 0)


def iota(shape, dim):
    return lax.broadcasted_iota(jnp.int32, shape, dim)


def split_up(values):
    high = values.astype(BF16)
    return high, (values - high.astype(F32)).astype(BF16)


def thrice(values):
    one = values.astype(BF16)
    rest = values - one.astype(F32)
    two, three = split_up(rest)
    return one, two, three


def pack_kernel(pixel_ref, copies_ref, plane_ref):
    channels, rows, columns = pixel_ref.shape
    pitch = plane_ref.shape[0] // SUB
    plane_ref[...] = jnp.zeros(plane_ref.shape, F32)
    for channel in range(channels):
        plane_ref[channel * pitch : channel * pitch + rows, :columns] = pixel_ref[channel].astype(F32)
    for pair in range(rows // 2):
        even = plane_ref[pl.ds(2 * pair, SUB, stride=pitch), :]
        odd = plane_ref[pl.ds(2 * pair + 1, SUB, stride=pitch), :]
        packed = (even + pltpu.roll(odd, CELL, 1)).astype(BF16)
        for copy in range(copies_ref.shape[0]):
            copies_ref[copy, :, pair * LANES : (pair + 1) * LANES] = packed


def join_kernel(columns, tiles_ref, strip_ref, last_ref):
    tiles, _, width = tiles_ref.shape
    pairs = width // LANES
    lane = iota((pairs * SUB, LANES), 1)
    stacked = [
        jnp.concatenate([tiles_ref[tile, :, pair * LANES : (pair + 1) * LANES].astype(F32) for pair in range(pairs)], axis=0)
        for tile in range(tiles)
    ]
    for parity in range(2):
        halves = []
        for half in range(LINE // LANES):
            line = jnp.zeros((pairs * SUB, LANES), F32)
            for tile in range(tiles):
                start, end = tile * columns - half * LANES, (tile + 1) * columns - half * LANES
                if end <= 0 or start >= LANES:
                    continue
                moved = pltpu.roll(stacked[tile], (start - parity * CELL) % LANES, 1)
                line = jnp.where((lane >= start) & (lane < end), moved, line)
            halves.append(line)
        for pair in range(pairs):
            row = 2 * pair + parity
            for half, line in enumerate(halves):
                at = row * LINE + half * LANES
                strip_ref[:, at : at + LANES] = line[pair * SUB : (pair + 1) * SUB]
    last_ref[...] = strip_ref[:, 2 * pairs * LINE - 2 * LINE :].astype(BF16)


def spread_weight(conv_ref, copies):
    channels = conv_ref.shape[0] // TAPS
    shape = (copies, conv_ref.shape[0])
    row, tap = iota(shape, 0), iota(shape, 1)
    place = row % SPAN
    hit = (place // SUB == tap // channels) & (place % SUB == tap % channels) & (row < 3 * SPAN)
    spread = nn(jnp.where(hit, 1.0, 0.0).astype(BF16), conv_ref[...])
    return spread - jnp.mean(spread, axis=-1, keepdims=True)


def query_kernel(
    conv_ref, gain_ref, lat_gain_ref, lat_hbm, query_hbm, key_hbm, rows_ref, lat_ref, query_ref, key_ref, sems
):
    lat_copy = pltpu.make_async_copy(lat_hbm.at[:, lax.axis_index("gy")], lat_ref, sems.at[0])
    query_copy = pltpu.make_async_copy(query_hbm, query_ref, sems.at[1])
    key_copy = pltpu.make_async_copy(key_hbm, key_ref, sems.at[2])
    lat_copy.start()
    query_copy.start()
    key_copy.start()

    weight = spread_weight(conv_ref, SPAN)
    feat = weight.shape[1]
    high, low = split_up(weight)
    both = jnp.concatenate([high, low], axis=0)
    held = HEADS * lat_ref.shape[0] * lat_ref.shape[1]
    for part, at in enumerate(range(0, feat, LINE)):
        end = min(at + LINE, feat)
        first = held + LINE + part * 2 * SPAN
        rows_ref[first : first + 2 * SPAN, : end - at] = both[:, at:end]
    padding = jnp.zeros((LANES - SPAN, feat), BF16)
    gram = nt(both, jnp.concatenate([high, padding], axis=0)) + nt(both, jnp.concatenate([low, padding], axis=0))
    gram = (gram[:SPAN] + gram[SPAN:]) * (1.0 / feat)
    rows_ref[held : held + 3 * SPAN, :LANES] = jnp.concatenate(thrice(gram), axis=0)

    lat_copy.wait()
    values = lat_ref[...].astype(F32)
    values = values.reshape(values.shape[0] * values.shape[1], values.shape[2])
    centred = values - jnp.mean(values, axis=-1, keepdims=True)
    variance = jnp.mean(centred * centred, axis=-1, keepdims=True)
    gain = lat_gain_ref[...].reshape(1, -1)
    normed = (centred * lax.rsqrt(variance + EPS) * gain).astype(BF16)
    query_copy.wait()
    queries = nn(normed, query_ref[...]).astype(BF16)

    key_copy.wait()
    keys = nn(jnp.concatenate(split_up(weight * gain_ref[...].reshape(1, -1)), axis=0), key_ref[...])
    high, low = split_up((keys[:SPAN] + keys[SPAN:]) * (LOG2E / DH**0.5))
    count = values.shape[0]
    lane = iota((count, LINE), 1)
    padding = jnp.zeros((LINE - 3 * SPAN, 2 * DH), BF16)
    for head in range(HEADS):
        cut = slice(head * DH, (head + 1) * DH)
        query = jnp.concatenate([queries[:, cut], queries[:, cut]], axis=1)
        key = jnp.concatenate([high[:, cut], low[:, cut]], axis=1)
        rows = nt(query, jnp.concatenate([key, key, key, padding], axis=0))
        rows = jnp.where(lane == MASK, -1.0, rows)
        top, rest = split_up(rows)
        rows_ref[head * count : (head + 1) * count, :] = jnp.where((lane >= SPAN) & (lane < 2 * SPAN), rest, top)


def table_rows(feat):
    return LINE + -(-feat // LINE) * 2 * SPAN


def scaled_patches(patches, explicit, feat, rows_ref):
    exact = patches.astype(BF16)
    held = rows_ref.shape[0] - table_rows(feat)
    if explicit:
        total = 0.0
        for part, at in enumerate(range(0, feat, LINE)):
            end = min(at + LINE, feat)
            first = held + LINE + part * 2 * SPAN
            wide = rows_ref[first : first + 2 * SPAN, : end - at]
            features = tn(wide[:SPAN], exact) + tn(wide[SPAN:], exact)
            total = total + jnp.sum(features * features, axis=0, keepdims=True)
        variance = total * (1.0 / feat)
        lost = None
    else:
        gram = rows_ref[held : held + 3 * SPAN, :LANES]
        form = nn(gram[:, :SPAN], exact)
        form = form[:SPAN] + form[SPAN : 2 * SPAN] + form[2 * SPAN :]
        variance = jnp.maximum(jnp.sum(form * patches, axis=0, keepdims=True), 0.0)
        shape = (SPAN, LANES)
        diag = jnp.where(iota(shape, 0) == iota(shape, 1), gram[:SPAN].astype(F32), 0.0)
        diag = jnp.sum(diag, axis=-1, keepdims=True)
        scale = jnp.sum(patches * patches * diag, axis=0, keepdims=True)
        lost = jnp.where((variance + EPS) * 128.0 < scale, 1.0, 0.0)
    return patches * lax.rsqrt(variance + EPS), lost


def fill_block(patches, real, explicit, feat, rows_ref, pixel_ref, at):
    width = patches.shape[1]
    scaled, lost = scaled_patches(patches, explicit, feat, rows_ref)
    row = iota((SPAN, width), 0)
    scaled = jnp.where((row == ONE) | (row == ONE_TOO), jnp.where(real, 1.0, 0.0), scaled)
    scaled = jnp.where(row == MASK, jnp.where(real, 0.0, BIG), scaled)
    high, low = split_up(scaled)
    cut = slice(at, at + width)
    pixel_ref[:SPAN, cut] = high
    pixel_ref[SPAN : 2 * SPAN, cut] = high
    pixel_ref[2 * SPAN : 3 * SPAN, cut] = low
    pixel_ref[3 * SPAN :, cut] = jnp.zeros((LINE - 3 * SPAN, width), BF16)
    return lost


def attend(blocks, rows_ref, pixel_ref, score_ref, expo_ref):
    tops, sums = [], []
    count = len(blocks)
    for turn in range(count + 2):
        if turn < count:
            rows, cut = blocks[turn]
            score_ref[turn % 2, rows, : cut.stop - cut.start] = nn(rows_ref[rows], pixel_ref[:, cut])
        if 0 <= turn - 1 < count:
            rows, cut = blocks[turn - 1]
            at = ((turn - 1) % 2, rows, slice(0, cut.stop - cut.start))
            top = jnp.max(score_ref[at], axis=-1, keepdims=True)
            expo_ref[at] = jnp.exp2(score_ref[at] - top).astype(BF16)
            tops.append(top)
        if 0 <= turn - 2 < count:
            rows, cut = blocks[turn - 2]
            at = ((turn - 2) % 2, rows, slice(0, cut.stop - cut.start))
            sums.append(nt(expo_ref[at], pixel_ref[:LANES, cut]))
    return tops, sums


def merged(tops, sums):
    top = functools.reduce(jnp.maximum, tops)
    total = sum(jnp.exp2(t - top) * s for t, s in zip(tops, sums))
    return top, total


def inner_kernel(
    columns, size, feat, strip_ref, rows_ref, sums_ref, tops_ref, pixel_ref, score_ref, expo_ref
):
    width = strip_ref.shape[1]
    inner = width - 2 * LINE
    strip = strip_ref[...]
    shifted = [pltpu.roll(strip, 1, 1), strip, pltpu.roll(strip, width - 1, 1)]
    count = sums_ref.shape[0]
    blocks = [(slice(0, count), slice(at, at + size)) for at in range(0, inner, size)]

    def run(explicit):
        flags = []
        for at in range(0, inner, size):
            end = at + size
            cells = [shifted[tap % 3][:, tap // 3 * LINE + at : tap // 3 * LINE + end] for tap in range(TAPS)]
            patches = jnp.concatenate(cells + [jnp.zeros_like(cells[0])], axis=0)
            real = iota(patches.shape, 1) % LINE < columns
            flags.append(fill_block(patches, real, explicit, feat, rows_ref, pixel_ref, at))
        tops, sums = attend(blocks, rows_ref, pixel_ref, score_ref, expo_ref)
        top, total = merged(tops, sums)
        sums_ref[...] = total
        tops_ref[...] = jnp.broadcast_to(top, tops_ref.shape)
        return flags

    lost = jnp.max(functools.reduce(jnp.maximum, run(False)))

    @pl.when(lost > 0.5)
    def _():
        run(True)


def border_kernel(
    columns,
    feat,
    strip_ref,
    before_ref,
    rows_ref,
    inner_sums_ref,
    inner_tops_ref,
    sent_ref,
    pixel_ref,
    score_ref,
    expo_ref,
):
    width = strip_ref.shape[1]
    lines = jnp.concatenate(
        [
            before_ref[...].astype(F32),
            strip_ref[:, : 2 * LINE],
            strip_ref[:, width - 2 * LINE :],
            jnp.zeros((SUB, LINE), F32),
        ],
        axis=1,
    )
    shifted = [pltpu.roll(lines, 1, 1), lines, pltpu.roll(lines, lines.shape[1] - 1, 1)]
    cells = []
    for tap in range(TAPS):
        at = tap // 3 * LINE
        source = shifted[tap % 3]
        cells.append(jnp.concatenate([source[:, at : at + 2 * LINE], source[:, at + 4 * LINE : at + 5 * LINE]], axis=1))
    patches = jnp.concatenate(cells + [jnp.zeros_like(cells[0])], axis=0)
    lane = iota(patches.shape, 1)
    place = lax.axis_index("gx")
    above = (place > 0).astype(jnp.int32)
    final = (place == lax.axis_size("gx") - 1).astype(jnp.int32)
    shown = jnp.where(lane < LINE, above, jnp.where(lane < 2 * LINE, 1, final))
    real = (lane % LINE < columns) & (shown > 0)
    count = sent_ref.shape[0]
    half = score_ref.shape[1] // 2
    blocks = [(slice(at, at + half), slice(0, patches.shape[1])) for at in (0, half)]
    shape = (2 * LANES, LANES)
    row, lane = iota(shape, 0), iota(shape, 1)
    tap = row % LANES
    target = jnp.where((tap < ONE) & (tap % SUB < 6), tap // SUB * 6 + tap % SUB, -1)
    target = jnp.where(tap == ONE, TOTAL, jnp.where(tap == ONE_TOO, TOTAL + 1, target))
    place = jnp.where((target >= 0) & (lane == target + row // LANES * SLOT), 1.0, 0.0).astype(BF16)

    def run(explicit):
        lost = fill_block(patches, real, explicit, feat, rows_ref, pixel_ref, 0)
        tops, sums = attend(blocks, rows_ref, pixel_ref, score_ref, expo_ref)
        tops, sums = jnp.concatenate(tops, axis=0), jnp.concatenate(sums, axis=0)
        top, total = merged([inner_tops_ref[...], tops], [inner_sums_ref[...], sums])
        high = total.astype(BF16)
        low = (total - high.astype(F32)).astype(BF16)
        high = jnp.where(iota(total.shape, 1) == ONE_TOO, low, high)

        def side(values, odd):
            heads = range(odd, HEADS, 2)
            return jnp.concatenate([values[head * count : (head + 1) * count] for head in heads], axis=0)

        placed = nn(jnp.concatenate([side(high, 0), side(high, 1)], axis=1), place)
        lane = iota(placed.shape, 1)
        column = lane % SLOT
        one, two, three = thrice(jnp.where(lane < SLOT, side(top, 0), side(top, 1)))
        placed = jnp.where(column == TOP, one.astype(F32), placed)
        placed = jnp.where(column == TOP + 1, two.astype(F32), placed)
        placed = jnp.where(column == TOP + 2, three.astype(F32), placed).astype(BF16)
        for pair in range(HEADS // 2):
            sent_ref[:, pair * LANES : (pair + 1) * LANES] = placed[pair * count : (pair + 1) * count]
        return lost

    lost = jnp.max(run(False))

    @pl.when(lost > 0.5)
    def _():
        run(True)


def output_kernel(conv_ref, gain_ref, value_ref, out_ref, both_ref):
    weight = conv_ref[...].astype(F32)
    weight = (weight - jnp.mean(weight, axis=-1, keepdims=True)) * gain_ref[...].reshape(1, -1)
    weight = jnp.concatenate([weight, jnp.zeros((SLOT - weight.shape[0], weight.shape[1]), F32)], axis=0)
    both = nn(jnp.concatenate(split_up(weight), axis=0), value_ref[...])
    high, low = split_up(both[:SLOT] + both[SLOT:])
    for head in range(HEADS):
        cut = slice(head * DH, (head + 1) * DH)
        both = nn(jnp.concatenate([high[:, cut], low[:, cut]], axis=0), out_ref[cut])
        both_ref[head * SLOT : (head + 1) * SLOT, :] = (both[:SLOT] + both[SLOT:]).astype(BF16)


def combine_kernel(parts_ref, both_ref, own_ref, result_ref):
    count, share, width = parts_ref.shape
    row, lane = iota((LANES, LANES), 0), iota((LANES, LANES), 1)
    same = row // SLOT == lane // SLOT
    column = row % SLOT
    pick_top = jnp.where(same & (column >= TOP) & (column < TOP + 3), 1.0, 0.0).astype(BF16)
    pick_one = jnp.where(same & (column >= TOTAL) & (column < TOTAL + 2), 1.0, 0.0).astype(BF16)
    means = []
    for at in range(0, width, LANES):
        values = parts_ref[:, :, at : at + LANES].astype(F32)
        parts = values.reshape(count * share, LANES).astype(BF16)
        tops = nn(parts, pick_top).reshape(values.shape)
        ones = nn(parts, pick_one).reshape(values.shape)
        factor = jnp.exp2(tops - jnp.max(tops, axis=0, keepdims=True))
        means.append(jnp.sum(factor * values, axis=0) / jnp.sum(factor * ones, axis=0))
    mean = jnp.concatenate(means, axis=1)
    high = mean.astype(BF16).astype(F32)
    result = nn(jnp.concatenate([high, mean - high], axis=0).astype(BF16), both_ref[...])
    result = own_ref[...].astype(F32) + (result[:share] + result[share:])
    result_ref[...] = result.astype(BF16)


def vmem(count):
    return [pl.BlockSpec(memory_space=pltpu.VMEM)] * count


def kernel(body, name, outs, scratch=(), others=0, count=0, cycles=1000, room=4):
    single = not isinstance(outs, (list, tuple))
    return pl.pallas_call(
        body,
        out_shape=outs,
        in_specs=vmem(count) + [pl.BlockSpec(memory_space=pltpu.HBM)] * others,
        out_specs=vmem(1)[0] if single else tuple(vmem(len(outs))),
        scratch_shapes=list(scratch),
        cost_estimate=pl.CostEstimate(flops=cycles * 4096, bytes_accessed=1 << 20, transcendentals=0),
        compiler_params=pltpu.CompilerParams(vmem_limit_bytes=room << 20),
        name=name,
    )


def on_device(
    pixels,
    conv_weight,
    input_gain,
    key_weight,
    value_weight,
    latents,
    latent_gain,
    query_weight,
    out_weight,
):
    tile_rows, tile_cols, _ = pixels.shape
    across, down = lax.axis_size("gy"), lax.axis_size("gx")
    columns = tile_cols * across
    feat = conv_weight.shape[1]
    lat, width = latents.shape
    share = lat // (across * down)
    held = lat // across

    def shape(dims, dtype=BF16):
        return jax.ShapeDtypeStruct(dims, dtype)

    copies = kernel(
        pack_kernel,
        "pack",
        shape((across, SUB, tile_rows * CELL)),
        [pltpu.VMEM((SUB * 16, LANES), F32)],
        count=1,
    )(pixels.transpose(2, 0, 1))
    tiles = lax.all_to_all(copies, "gy", 0, 0, tiled=True)
    rows = kernel(
        query_kernel,
        "query_rows",
        shape((HEADS * held + table_rows(feat), LINE)),
        [
            pltpu.VMEM((down, share, width), BF16),
            pltpu.VMEM(query_weight.shape, BF16),
            pltpu.VMEM(key_weight.shape, BF16),
            pltpu.SemaphoreType.DMA((3,)),
        ],
        others=3,
        count=3,
        cycles=6000,
        room=60,
    )(conv_weight, input_gain, latent_gain, latents.reshape(down, across, share, width), query_weight, key_weight)
    both = kernel(
        output_kernel, "value_output", shape((HEADS * SLOT, width)), count=4, cycles=6000, room=10
    )(conv_weight, input_gain, value_weight, out_weight)

    tiles, rows = lax.optimization_barrier((tiles, rows))
    strip, last = kernel(
        functools.partial(join_kernel, tile_cols),
        "join",
        [shape((SUB, tile_rows * LINE), F32), shape((SUB, 2 * LINE))],
        count=1,
        cycles=200000,
    )(tiles)
    before = lax.ppermute(last, "gx", [(i, i + 1) for i in range(down - 1)])
    inner = (tile_rows - 2) * LINE
    size = inner // 3
    sums, tops = kernel(
        functools.partial(inner_kernel, columns, size, feat),
        "inner",
        [shape((HEADS * held, LANES), F32), shape((HEADS * held, LANES), F32)],
        [
            pltpu.VMEM((LINE, inner), BF16),
            pltpu.VMEM((2, HEADS * held, size), F32),
            pltpu.VMEM((2, HEADS * held, size), BF16),
        ],
        count=2,
        cycles=10000,
        room=34,
    )(strip, rows)
    sent = kernel(
        functools.partial(border_kernel, columns, feat),
        "border",
        shape((held, HEADS * SLOT)),
        [
            pltpu.VMEM((LINE, 3 * LINE), BF16),
            pltpu.VMEM((2, HEADS * held, 3 * LINE), F32),
            pltpu.VMEM((2, HEADS * held, 3 * LINE), BF16),
        ],
        count=5,
        cycles=3000,
        room=24,
    )(strip, before, rows, sums, tops)
    parts = lax.all_to_all(sent.reshape(down, share, -1), "gx", 0, 0, tiled=True)
    own = lax.dynamic_slice_in_dim(latents, lax.axis_index(GROUP) * share, share, 0)
    return kernel(combine_kernel, "combine", shape((share, width)), count=3, room=6)(parts, both, own)


def solution(mesh):
    return jax.shard_map(
        on_device,
        mesh=mesh,
        in_specs=(P(("ba", "gx"), "gy", None), P(), P(), P(), P(), P(), P(), P(), P()),
        out_specs=P(("ba", "gx", "gy"), None),
        check_vma=False,
    )
```

```python
import functools

import jax
import jax.numpy as jnp
from jax import lax
from jax.experimental import pallas as pl
from jax.experimental.pallas import tpu as pltpu
from jax.sharding import PartitionSpec as P

HEADS = 8
DH = 128
LANES = 128
SUB = 8
TAPS = 9
CELL = 64
LINE = 256
SPAN = 80
ONE, MASK, ONE_TOO = 72, 73, 74
SLOT = 64
TOTAL, TOP = 54, 57
BIG = 1e30
EPS = 1e-05
LOG2E = 1.4426950408889634
GROUP = ("gx", "gy")
F32 = jnp.float32
BF16 = jnp.bfloat16


def product(a, b, left, right):
    return lax.dot_general(a, b, (((left,), (right,)), ((), ())), preferred_element_type=F32)


def nn(a, b):
    return product(a, b, 1, 0)


def nt(a, b):
    return product(a, b, 1, 1)


def tn(a, b):
    return product(a, b, 0, 0)


def iota(shape, dim):
    return lax.broadcasted_iota(jnp.int32, shape, dim)


def split_up(values):
    high = values.astype(BF16)
    return high, (values - high.astype(F32)).astype(BF16)


def thrice(values):
    one = values.astype(BF16)
    rest = values - one.astype(F32)
    two, three = split_up(rest)
    return one, two, three


def pack_kernel(pixel_ref, copies_ref, plane_ref):
    channels, rows, columns = pixel_ref.shape
    pitch = plane_ref.shape[0] // SUB
    plane_ref[...] = jnp.zeros(plane_ref.shape, F32)
    for channel in range(channels):
        plane_ref[channel * pitch : channel * pitch + rows, :columns] = pixel_ref[channel].astype(F32)
    for pair in range(rows // 2):
        even = plane_ref[pl.ds(2 * pair, SUB, stride=pitch), :]
        odd = plane_ref[pl.ds(2 * pair + 1, SUB, stride=pitch), :]
        packed = (even + pltpu.roll(odd, CELL, 1)).astype(BF16)
        for copy in range(copies_ref.shape[0]):
            copies_ref[copy, :, pair * LANES : (pair + 1) * LANES] = packed


def join_kernel(columns, tiles_ref, strip_ref, last_ref):
    tiles, _, width = tiles_ref.shape
    pairs = width // LANES
    lane = iota((pairs * SUB, LANES), 1)
    stacked = [
        jnp.concatenate([tiles_ref[tile, :, pair * LANES : (pair + 1) * LANES].astype(F32) for pair in range(pairs)], axis=0)
        for tile in range(tiles)
    ]
    for parity in range(2):
        halves = []
        for half in range(LINE // LANES):
            line = jnp.zeros((pairs * SUB, LANES), F32)
            for tile in range(tiles):
                start, end = tile * columns - half * LANES, (tile + 1) * columns - half * LANES
                if end <= 0 or start >= LANES:
                    continue
                moved = pltpu.roll(stacked[tile], (start - parity * CELL) % LANES, 1)
                line = jnp.where((lane >= start) & (lane < end), moved, line)
            halves.append(line)
        for pair in range(pairs):
            row = 2 * pair + parity
            for half, line in enumerate(halves):
                at = row * LINE + half * LANES
                strip_ref[:, at : at + LANES] = line[pair * SUB : (pair + 1) * SUB]
    last_ref[...] = strip_ref[:, 2 * pairs * LINE - 2 * LINE :].astype(BF16)


def spread_weight(conv_ref, copies):
    channels = conv_ref.shape[0] // TAPS
    shape = (copies, conv_ref.shape[0])
    row, tap = iota(shape, 0), iota(shape, 1)
    place = row % SPAN
    hit = (place // SUB == tap // channels) & (place % SUB == tap % channels) & (row < 3 * SPAN)
    spread = nn(jnp.where(hit, 1.0, 0.0).astype(BF16), conv_ref[...])
    return spread - jnp.mean(spread, axis=-1, keepdims=True)


def query_kernel(
    conv_ref, gain_ref, lat_gain_ref, lat_hbm, query_hbm, key_hbm, rows_ref, lat_ref, query_ref, key_ref, sems
):
    lat_copy = pltpu.make_async_copy(lat_hbm.at[:, lax.axis_index("gy")], lat_ref, sems.at[0])
    query_copy = pltpu.make_async_copy(query_hbm, query_ref, sems.at[1])
    key_copy = pltpu.make_async_copy(key_hbm, key_ref, sems.at[2])
    key_copy.start()
    lat_copy.start()
    query_copy.start()

    weight = spread_weight(conv_ref, SPAN)
    feat = weight.shape[1]
    high, low = split_up(weight)
    both = jnp.concatenate([high, low], axis=0)
    held = HEADS * lat_ref.shape[0] * lat_ref.shape[1]
    for part, at in enumerate(range(0, feat, LINE)):
        end = min(at + LINE, feat)
        first = held + LINE + part * 2 * SPAN
        rows_ref[first : first + 2 * SPAN, : end - at] = both[:, at:end]
    padding = jnp.zeros((LANES - SPAN, feat), BF16)
    gram = nt(both, jnp.concatenate([high, padding], axis=0)) + nt(both, jnp.concatenate([low, padding], axis=0))
    gram = (gram[:SPAN] + gram[SPAN:]) * (1.0 / feat)
    for part, piece in enumerate(thrice(gram)):
        rows_ref[held : held + SPAN, part * SPAN : (part + 1) * SPAN] = piece[:, :SPAN]

    key_copy.wait()
    keys = nn(jnp.concatenate(split_up(weight * gain_ref[...].reshape(1, -1)), axis=0), key_ref[...])
    high, low = split_up((keys[:SPAN] + keys[SPAN:]) * (LOG2E / DH**0.5))

    lat_copy.wait()
    values = lat_ref[...].astype(F32)
    values = values.reshape(values.shape[0] * values.shape[1], values.shape[2])
    centred = values - jnp.mean(values, axis=-1, keepdims=True)
    variance = jnp.mean(centred * centred, axis=-1, keepdims=True)
    gain = lat_gain_ref[...].reshape(1, -1)
    normed = (centred * lax.rsqrt(variance + EPS) * gain).astype(BF16)
    query_copy.wait()
    queries = nn(normed, query_ref[...]).astype(BF16)

    count = values.shape[0]
    lane = iota((count, LINE), 1)
    padding = jnp.zeros((LINE - 3 * SPAN, 2 * DH), BF16)
    for head in range(HEADS):
        cut = slice(head * DH, (head + 1) * DH)
        query = jnp.concatenate([queries[:, cut], queries[:, cut]], axis=1)
        key = jnp.concatenate([high[:, cut], low[:, cut]], axis=1)
        rows = nt(query, jnp.concatenate([key, key, key, padding], axis=0))
        rows = jnp.where(lane == MASK, -1.0, rows)
        top, rest = split_up(rows)
        rows_ref[head * count : (head + 1) * count, :] = jnp.where((lane >= SPAN) & (lane < 2 * SPAN), rest, top)


def table_rows(feat):
    return LINE + -(-feat // LINE) * 2 * SPAN


def scaled_patches(patches, explicit, feat, rows_ref):
    exact = patches.astype(BF16)
    held = rows_ref.shape[0] - table_rows(feat)
    if explicit:
        total = 0.0
        for part, at in enumerate(range(0, feat, LINE)):
            end = min(at + LINE, feat)
            first = held + LINE + part * 2 * SPAN
            wide = rows_ref[first : first + 2 * SPAN, : end - at]
            features = tn(wide[:SPAN], exact) + tn(wide[SPAN:], exact)
            total = total + jnp.sum(features * features, axis=0, keepdims=True)
        variance = total * (1.0 / feat)
        lost = None
    else:
        gram = rows_ref[held : held + SPAN, : 3 * SPAN]
        form = nn(gram, jnp.concatenate([exact, exact, exact], axis=0))
        variance = jnp.maximum(jnp.sum(form * patches, axis=0, keepdims=True), 0.0)
        diag = jnp.where(iota(gram.shape, 0) == iota(gram.shape, 1), gram.astype(F32), 0.0)
        diag = jnp.sum(diag, axis=-1, keepdims=True)
        scale = jnp.sum(patches * patches * diag, axis=0, keepdims=True)
        lost = jnp.where((variance + EPS) * 128.0 < scale, 1.0, 0.0)
    return patches * lax.rsqrt(variance + EPS), lost


def fill_block(patches, real, explicit, feat, rows_ref, pixel_ref, at):
    width = patches.shape[1]
    scaled, lost = scaled_patches(patches, explicit, feat, rows_ref)
    row = iota((SPAN, width), 0)
    scaled = jnp.where((row == ONE) | (row == ONE_TOO), jnp.where(real, 1.0, 0.0), scaled)
    scaled = jnp.where(row == MASK, jnp.where(real, 0.0, BIG), scaled)
    high, low = split_up(scaled)
    cut = slice(at, at + width)
    pixel_ref[:SPAN, cut] = high
    pixel_ref[SPAN : 2 * SPAN, cut] = high
    pixel_ref[2 * SPAN : 3 * SPAN, cut] = low
    pixel_ref[3 * SPAN :, cut] = jnp.zeros((LINE - 3 * SPAN, width), BF16)
    return lost


def attend(blocks, rows_ref, pixel_ref, score_ref, expo_ref):
    tops, sums = [], []
    count = len(blocks)
    for turn in range(count + 2):
        if turn < count:
            rows, cut = blocks[turn]
            score_ref[turn % 2, rows, : cut.stop - cut.start] = nn(rows_ref[rows], pixel_ref[:, cut])
        if 0 <= turn - 1 < count:
            rows, cut = blocks[turn - 1]
            at = ((turn - 1) % 2, rows, slice(0, cut.stop - cut.start))
            top = jnp.max(score_ref[at], axis=-1, keepdims=True)
            expo_ref[at] = jnp.exp2(score_ref[at] - top).astype(BF16)
            tops.append(top)
        if 0 <= turn - 2 < count:
            rows, cut = blocks[turn - 2]
            at = ((turn - 2) % 2, rows, slice(0, cut.stop - cut.start))
            sums.append(nt(expo_ref[at], pixel_ref[:LANES, cut]))
    return tops, sums


def merged(tops, sums):
    top = functools.reduce(jnp.maximum, tops)
    total = sum(jnp.exp2(t - top) * s for t, s in zip(tops, sums))
    return top, total


def inner_kernel(
    columns, size, feat, strip_ref, rows_ref, sums_ref, tops_ref, pixel_ref, score_ref, expo_ref
):
    width = strip_ref.shape[1]
    inner = width - 2 * LINE
    strip = strip_ref[...]
    shifted = [pltpu.roll(strip, 1, 1), strip, pltpu.roll(strip, width - 1, 1)]
    count = sums_ref.shape[0]
    blocks = [(slice(0, count), slice(at, at + size)) for at in range(0, inner, size)]
    half = count // 2
    halves = [(slice(r, r + half), b) for _, b in blocks for r in (0, half)]

    def run(explicit):
        flags = []

        def fill(turn):
            at, end = blocks[turn][1].start, blocks[turn][1].stop
            cells = [shifted[tap % 3][:, tap // 3 * LINE + at : tap // 3 * LINE + end] for tap in range(TAPS)]
            patches = jnp.concatenate(cells + [jnp.zeros_like(cells[0])], axis=0)
            real = (iota(patches.shape, 1) + at) % LINE < columns
            flags.append(fill_block(patches, real, explicit, feat, rows_ref, pixel_ref, at))

        for turn in range(len(blocks)):
            fill(turn)
        tops, sums = attend(halves, rows_ref, pixel_ref, score_ref, expo_ref)
        tops = [jnp.concatenate(tops[i : i + 2], axis=0) for i in range(0, len(tops), 2)]
        sums = [jnp.concatenate(sums[i : i + 2], axis=0) for i in range(0, len(sums), 2)]
        top, total = merged(tops, sums)
        sums_ref[...] = total
        tops_ref[...] = jnp.broadcast_to(top, tops_ref.shape)
        return [jnp.max(flag) for flag in flags if flag is not None]

    lost = functools.reduce(jnp.maximum, run(False))

    @pl.when(lost > 0.5)
    def _():
        run(True)


def border_kernel(
    columns,
    feat,
    strip_ref,
    before_ref,
    rows_ref,
    inner_sums_ref,
    inner_tops_ref,
    sent_ref,
    pixel_ref,
    score_ref,
    expo_ref,
):
    width = strip_ref.shape[1]
    lines = jnp.concatenate(
        [
            before_ref[...].astype(F32),
            strip_ref[:, : 2 * LINE],
            strip_ref[:, width - 2 * LINE :],
            jnp.zeros((SUB, LINE), F32),
        ],
        axis=1,
    )
    shifted = [pltpu.roll(lines, 1, 1), lines, pltpu.roll(lines, lines.shape[1] - 1, 1)]
    cells = []
    for tap in range(TAPS):
        at = tap // 3 * LINE
        source = shifted[tap % 3]
        cells.append(jnp.concatenate([source[:, at : at + 2 * LINE], source[:, at + 4 * LINE : at + 5 * LINE]], axis=1))
    patches = jnp.concatenate(cells + [jnp.zeros_like(cells[0])], axis=0)
    lane = iota(patches.shape, 1)
    place = lax.axis_index("gx")
    above = (place > 0).astype(jnp.int32)
    final = (place == lax.axis_size("gx") - 1).astype(jnp.int32)
    shown = jnp.where(lane < LINE, above, jnp.where(lane < 2 * LINE, 1, final))
    real = (lane % LINE < columns) & (shown > 0)
    count = sent_ref.shape[0]
    half = score_ref.shape[1] // 2
    blocks = [(slice(at, at + half), slice(0, patches.shape[1])) for at in (0, half)]
    shape = (2 * LANES, LANES)
    row, lane = iota(shape, 0), iota(shape, 1)
    tap = row % LANES
    target = jnp.where((tap < ONE) & (tap % SUB < 6), tap // SUB * 6 + tap % SUB, -1)
    target = jnp.where(tap == ONE, TOTAL, jnp.where(tap == ONE_TOO, TOTAL + 1, target))
    place = jnp.where((target >= 0) & (lane == target + row // LANES * SLOT), 1.0, 0.0).astype(BF16)

    def run(explicit):
        lost = fill_block(patches, real, explicit, feat, rows_ref, pixel_ref, 0)
        tops, sums = attend(blocks, rows_ref, pixel_ref, score_ref, expo_ref)
        tops, sums = jnp.concatenate(tops, axis=0), jnp.concatenate(sums, axis=0)
        top, total = merged([inner_tops_ref[...], tops], [inner_sums_ref[...], sums])
        high = total.astype(BF16)
        low = (total - high.astype(F32)).astype(BF16)
        high = jnp.where(iota(total.shape, 1) == ONE_TOO, low, high)

        def side(values, odd):
            heads = range(odd, HEADS, 2)
            return jnp.concatenate([values[head * count : (head + 1) * count] for head in heads], axis=0)

        placed = nn(jnp.concatenate([side(high, 0), side(high, 1)], axis=1), place)
        lane = iota(placed.shape, 1)
        column = lane % SLOT
        one, two, three = thrice(jnp.where(lane < SLOT, side(top, 0), side(top, 1)))
        placed = jnp.where(column == TOP, one.astype(F32), placed)
        placed = jnp.where(column == TOP + 1, two.astype(F32), placed)
        placed = jnp.where(column == TOP + 2, three.astype(F32), placed).astype(BF16)
        for pair in range(HEADS // 2):
            sent_ref[:, pair * LANES : (pair + 1) * LANES] = placed[pair * count : (pair + 1) * count]
        return lost

    lost = jnp.max(run(False))

    @pl.when(lost > 0.5)
    def _():
        run(True)


def output_kernel(conv_ref, gain_ref, value_ref, out_ref, both_ref):
    weight = conv_ref[...].astype(F32)
    weight = (weight - jnp.mean(weight, axis=-1, keepdims=True)) * gain_ref[...].reshape(1, -1)
    weight = jnp.concatenate([weight, jnp.zeros((SLOT - weight.shape[0], weight.shape[1]), F32)], axis=0)
    both = nn(jnp.concatenate(split_up(weight), axis=0), value_ref[...])
    high, low = split_up(both[:SLOT] + both[SLOT:])
    for head in range(HEADS):
        cut = slice(head * DH, (head + 1) * DH)
        both = nn(jnp.concatenate([high[:, cut], low[:, cut]], axis=0), out_ref[cut])
        both_ref[head * SLOT : (head + 1) * SLOT, :] = (both[:SLOT] + both[SLOT:]).astype(BF16)


def combine_kernel(parts_ref, both_ref, own_ref, result_ref):
    count, share, width = parts_ref.shape
    row, lane = iota((LANES, LANES), 0), iota((LANES, LANES), 1)
    same = row // SLOT == lane // SLOT
    column = row % SLOT
    pick_top = jnp.where(same & (column >= TOP) & (column < TOP + 3), 1.0, 0.0).astype(BF16)
    pick_one = jnp.where(same & (column >= TOTAL) & (column < TOTAL + 2), 1.0, 0.0).astype(BF16)
    means = []
    for at in range(0, width, LANES):
        values = parts_ref[:, :, at : at + LANES].astype(F32)
        parts = values.reshape(count * share, LANES).astype(BF16)
        tops = nn(parts, pick_top).reshape(values.shape)
        ones = nn(parts, pick_one).reshape(values.shape)
        factor = jnp.exp2(tops - jnp.max(tops, axis=0, keepdims=True))
        means.append(jnp.sum(factor * values, axis=0) / jnp.sum(factor * ones, axis=0))
    mean = jnp.concatenate(means, axis=1)
    high = mean.astype(BF16).astype(F32)
    result = nn(jnp.concatenate([high, mean - high], axis=0).astype(BF16), both_ref[...])
    result = own_ref[...].astype(F32) + (result[:share] + result[share:])
    result_ref[...] = result.astype(BF16)


def vmem(count):
    return [pl.BlockSpec(memory_space=pltpu.VMEM)] * count


def kernel(body, name, outs, scratch=(), others=0, count=0, cycles=1000, room=4):
    single = not isinstance(outs, (list, tuple))
    return pl.pallas_call(
        body,
        out_shape=outs,
        in_specs=vmem(count) + [pl.BlockSpec(memory_space=pltpu.HBM)] * others,
        out_specs=vmem(1)[0] if single else tuple(vmem(len(outs))),
        scratch_shapes=list(scratch),
        cost_estimate=pl.CostEstimate(flops=cycles * 4096, bytes_accessed=1 << 20, transcendentals=0),
        compiler_params=pltpu.CompilerParams(vmem_limit_bytes=room << 20),
        name=name,
    )


def on_device(
    pixels,
    conv_weight,
    input_gain,
    key_weight,
    value_weight,
    latents,
    latent_gain,
    query_weight,
    out_weight,
):
    tile_rows, tile_cols, _ = pixels.shape
    across, down = lax.axis_size("gy"), lax.axis_size("gx")
    columns = tile_cols * across
    feat = conv_weight.shape[1]
    lat, width = latents.shape
    share = lat // (across * down)
    held = lat // across

    def shape(dims, dtype=BF16):
        return jax.ShapeDtypeStruct(dims, dtype)

    copies = kernel(
        pack_kernel,
        "pack",
        shape((across, SUB, tile_rows * CELL)),
        [pltpu.VMEM((SUB * 16, LANES), F32)],
        count=1,
    )(pixels.transpose(2, 0, 1))
    tiles = lax.all_to_all(copies, "gy", 0, 0, tiled=True)
    rows = kernel(
        query_kernel,
        "query_rows",
        shape((HEADS * held + table_rows(feat), LINE)),
        [
            pltpu.VMEM((down, share, width), BF16),
            pltpu.VMEM(query_weight.shape, BF16),
            pltpu.VMEM(key_weight.shape, BF16),
            pltpu.SemaphoreType.DMA((3,)),
        ],
        others=3,
        count=3,
        cycles=6000,
        room=60,
    )(conv_weight, input_gain, latent_gain, latents.reshape(down, across, share, width), query_weight, key_weight)
    both = kernel(
        output_kernel, "value_output", shape((HEADS * SLOT, width)), count=4, cycles=6000, room=10
    )(conv_weight, input_gain, value_weight, out_weight)

    tiles, rows = lax.optimization_barrier((tiles, rows))
    strip, last = kernel(
        functools.partial(join_kernel, tile_cols),
        "join",
        [shape((SUB, tile_rows * LINE), F32), shape((SUB, 2 * LINE))],
        count=1,
        cycles=200000,
    )(tiles)
    before = lax.ppermute(last, "gx", [(i, i + 1) for i in range(down - 1)])
    inner = (tile_rows - 2) * LINE
    size = inner // 2
    sums, tops = kernel(
        functools.partial(inner_kernel, columns, size, feat),
        "inner",
        [shape((HEADS * held, LANES), F32), shape((HEADS * held, LANES), F32)],
        [
            pltpu.VMEM((LINE, inner), BF16),
            pltpu.VMEM((2, HEADS * held, size), F32),
            pltpu.VMEM((2, HEADS * held, size), BF16),
        ],
        count=2,
        cycles=10000,
        room=44,
    )(strip, rows)
    sent = kernel(
        functools.partial(border_kernel, columns, feat),
        "border",
        shape((held, HEADS * SLOT)),
        [
            pltpu.VMEM((LINE, 3 * LINE), BF16),
            pltpu.VMEM((2, HEADS * held, 3 * LINE), F32),
            pltpu.VMEM((2, HEADS * held, 3 * LINE), BF16),
        ],
        count=5,
        cycles=3000,
        room=24,
    )(strip, before, rows, sums, tops)
    parts = lax.all_to_all(sent.reshape(down, share, -1), "gx", 0, 0, tiled=True)
    own = lax.dynamic_slice_in_dim(latents, lax.axis_index(GROUP) * share, share, 0)
    return kernel(combine_kernel, "combine", shape((share, width)), count=3, room=6)(parts, both, own)


def solution(mesh):
    return jax.shard_map(
        on_device,
        mesh=mesh,
        in_specs=(P(("ba", "gx"), "gy", None), P(), P(), P(), P(), P(), P(), P(), P()),
        out_specs=P(("ba", "gx", "gy"), None),
        check_vma=False,
    )
```

```python
import functools

import jax
import jax.numpy as jnp
from jax import lax
from jax.experimental import pallas as pl
from jax.experimental.pallas import tpu as pltpu
from jax.sharding import PartitionSpec as P

HEADS = 8
DH = 128
LANES = 128
SUB = 8
TAPS = 9
CELL = 64
LINE = 256
SPAN = 80
ONE, MASK, ONE_TOO = 72, 73, 74
SLOT = 64
TOTAL, TOP = 54, 57
BIG = 1e30
EPS = 1e-05
LOG2E = 1.4426950408889634
GROUP = ("gx", "gy")
F32 = jnp.float32
BF16 = jnp.bfloat16


def product(a, b, left, right):
    return lax.dot_general(a, b, (((left,), (right,)), ((), ())), preferred_element_type=F32)


def nn(a, b):
    return product(a, b, 1, 0)


def nt(a, b):
    return product(a, b, 1, 1)


def tn(a, b):
    return product(a, b, 0, 0)


def iota(shape, dim):
    return lax.broadcasted_iota(jnp.int32, shape, dim)


def split_up(values):
    high = values.astype(BF16)
    return high, (values - high.astype(F32)).astype(BF16)


def thrice(values):
    one = values.astype(BF16)
    rest = values - one.astype(F32)
    two, three = split_up(rest)
    return one, two, three


def pack_kernel(pixel_ref, copies_ref, plane_ref):
    channels, rows, columns = pixel_ref.shape
    pitch = plane_ref.shape[0] // SUB
    plane_ref[...] = jnp.zeros(plane_ref.shape, F32)
    for channel in range(channels):
        plane_ref[channel * pitch : channel * pitch + rows, :columns] = pixel_ref[channel].astype(F32)
    for pair in range(rows // 2):
        even = plane_ref[pl.ds(2 * pair, SUB, stride=pitch), :]
        odd = plane_ref[pl.ds(2 * pair + 1, SUB, stride=pitch), :]
        packed = (even + pltpu.roll(odd, CELL, 1)).astype(BF16)
        for copy in range(copies_ref.shape[0]):
            copies_ref[copy, :, pair * LANES : (pair + 1) * LANES] = packed


def join_kernel(columns, tiles_ref, strip_ref, first_ref):
    tiles, _, width = tiles_ref.shape
    pairs = width // LANES
    lane = iota((pairs * SUB, LANES), 1)
    stacked = [
        jnp.concatenate([tiles_ref[tile, :, pair * LANES : (pair + 1) * LANES].astype(F32) for pair in range(pairs)], axis=0)
        for tile in range(tiles)
    ]
    for parity in range(2):
        halves = []
        for half in range(LINE // LANES):
            line = jnp.zeros((pairs * SUB, LANES), F32)
            for tile in range(tiles):
                start, end = tile * columns - half * LANES, (tile + 1) * columns - half * LANES
                if end <= 0 or start >= LANES:
                    continue
                moved = pltpu.roll(stacked[tile], (start - parity * CELL) % LANES, 1)
                line = jnp.where((lane >= start) & (lane < end), moved, line)
            halves.append(line)
        for pair in range(pairs):
            row = 2 * pair + parity
            for half, line in enumerate(halves):
                at = row * LINE + half * LANES
                strip_ref[:, at : at + LANES] = line[pair * SUB : (pair + 1) * SUB]
    first_ref[...] = strip_ref[:, : 2 * LINE].astype(BF16)


def spread_weight(conv_ref, copies):
    channels = conv_ref.shape[0] // TAPS
    shape = (copies, conv_ref.shape[0])
    row, tap = iota(shape, 0), iota(shape, 1)
    place = row % SPAN
    hit = (place // SUB == tap // channels) & (place % SUB == tap % channels) & (row < 3 * SPAN)
    spread = nn(jnp.where(hit, 1.0, 0.0).astype(BF16), conv_ref[...])
    return spread - jnp.mean(spread, axis=-1, keepdims=True)


def query_kernel(
    key_hbm, conv_hbm, gain_hbm, lat_hbm, lat_gain_hbm, query_hbm, rows_ref,
    key_ref, conv_ref, gain_ref, lat_ref, lat_gain_ref, query_ref, sems,
):
    sources = [key_hbm, conv_hbm, gain_hbm, lat_hbm.at[:, lax.axis_index("gy")], lat_gain_hbm, query_hbm]
    targets = [key_ref, conv_ref, gain_ref, lat_ref, lat_gain_ref, query_ref]
    copies = [pltpu.make_async_copy(*pair, sems.at[i]) for i, pair in enumerate(zip(sources, targets))]
    for copy in copies:
        copy.start()

    copies[1].wait()
    weight = spread_weight(conv_ref, SPAN)
    feat = weight.shape[1]
    high, low = split_up(weight)
    both = jnp.concatenate([high, low], axis=0)
    held = HEADS * lat_ref.shape[0] * lat_ref.shape[1]
    for part, at in enumerate(range(0, feat, LINE)):
        end = min(at + LINE, feat)
        first = held + LINE + part * 2 * SPAN
        rows_ref[first : first + 2 * SPAN, : end - at] = both[:, at:end]
    padding = jnp.zeros((LANES - SPAN, feat), BF16)
    gram = nt(both, jnp.concatenate([high, padding], axis=0)) + nt(both, jnp.concatenate([low, padding], axis=0))
    gram = (gram[:SPAN] + gram[SPAN:]) * (1.0 / feat)
    for part, piece in enumerate(thrice(gram)):
        rows_ref[held : held + SPAN, part * SPAN : (part + 1) * SPAN] = piece[:, :SPAN]

    copies[2].wait()
    copies[0].wait()
    keys = nn(jnp.concatenate(split_up(weight * gain_ref[...].reshape(1, -1)), axis=0), key_ref[...])
    high, low = split_up((keys[:SPAN] + keys[SPAN:]) * (LOG2E / DH**0.5))

    copies[3].wait()
    copies[4].wait()
    values = lat_ref[...].astype(F32)
    values = values.reshape(values.shape[0] * values.shape[1], values.shape[2])
    centred = values - jnp.mean(values, axis=-1, keepdims=True)
    variance = jnp.mean(centred * centred, axis=-1, keepdims=True)
    gain = lat_gain_ref[...].reshape(1, -1)
    normed = (centred * lax.rsqrt(variance + EPS) * gain).astype(BF16)
    copies[5].wait()
    queries = nn(normed, query_ref[...]).astype(BF16)

    count = values.shape[0]
    lane = iota((count, LINE), 1)
    padding = jnp.zeros((LINE - 3 * SPAN, 2 * DH), BF16)
    for head in range(HEADS):
        cut = slice(head * DH, (head + 1) * DH)
        query = jnp.concatenate([queries[:, cut], queries[:, cut]], axis=1)
        key = jnp.concatenate([high[:, cut], low[:, cut]], axis=1)
        rows = nt(query, jnp.concatenate([key, key, key, padding], axis=0))
        rows = jnp.where(lane == MASK, -1.0, rows)
        top, rest = split_up(rows)
        rows_ref[head * count : (head + 1) * count, :] = jnp.where((lane >= SPAN) & (lane < 2 * SPAN), rest, top)


def table_rows(feat):
    return LINE + -(-feat // LINE) * 2 * SPAN


def scaled_patches(patches, explicit, feat, rows_ref):
    exact = patches.astype(BF16)
    held = rows_ref.shape[0] - table_rows(feat)
    if explicit:
        total = 0.0
        for part, at in enumerate(range(0, feat, LINE)):
            end = min(at + LINE, feat)
            first = held + LINE + part * 2 * SPAN
            wide = rows_ref[first : first + 2 * SPAN, : end - at]
            features = tn(wide[:SPAN], exact) + tn(wide[SPAN:], exact)
            total = total + jnp.sum(features * features, axis=0, keepdims=True)
        variance = total * (1.0 / feat)
        lost = None
    else:
        gram = rows_ref[held : held + SPAN, : 3 * SPAN]
        form = nn(gram, jnp.concatenate([exact, exact, exact], axis=0))
        variance = jnp.maximum(jnp.sum(form * patches, axis=0, keepdims=True), 0.0)
        diag = jnp.where(iota(gram.shape, 0) == iota(gram.shape, 1), gram.astype(F32), 0.0)
        diag = jnp.sum(diag, axis=-1, keepdims=True)
        scale = jnp.sum(patches * patches * diag, axis=0, keepdims=True)
        lost = jnp.where((variance + EPS) * 128.0 < scale, 1.0, 0.0)
    return patches * lax.rsqrt(variance + EPS), lost


def fill_block(patches, real, explicit, feat, rows_ref, pixel_ref, at):
    width = patches.shape[1]
    scaled, lost = scaled_patches(patches, explicit, feat, rows_ref)
    row = iota((SPAN, width), 0)
    scaled = jnp.where((row == ONE) | (row == ONE_TOO), jnp.where(real, 1.0, 0.0), scaled)
    scaled = jnp.where(row == MASK, jnp.where(real, 0.0, BIG), scaled)
    high, low = split_up(scaled)
    cut = slice(at, at + width)
    pixel_ref[:SPAN, cut] = high
    pixel_ref[SPAN : 2 * SPAN, cut] = high
    pixel_ref[2 * SPAN : 3 * SPAN, cut] = low
    pixel_ref[3 * SPAN :, cut] = jnp.zeros((LINE - 3 * SPAN, width), BF16)
    return lost


def attend(blocks, rows_ref, pixel_ref, score_ref, expo_ref):
    tops, sums = [], []
    count = len(blocks)
    for turn in range(count + 2):
        if turn < count:
            rows, cut = blocks[turn]
            score_ref[turn % 2, rows, : cut.stop - cut.start] = nn(rows_ref[rows], pixel_ref[:, cut])
        if 0 <= turn - 1 < count:
            rows, cut = blocks[turn - 1]
            at = ((turn - 1) % 2, rows, slice(0, cut.stop - cut.start))
            top = jnp.max(score_ref[at], axis=-1, keepdims=True)
            expo_ref[at] = jnp.exp2(score_ref[at] - top).astype(BF16)
            tops.append(top)
        if 0 <= turn - 2 < count:
            rows, cut = blocks[turn - 2]
            at = ((turn - 2) % 2, rows, slice(0, cut.stop - cut.start))
            sums.append(nt(expo_ref[at], pixel_ref[:LANES, cut]))
    return tops, sums


def merged(tops, sums):
    top = functools.reduce(jnp.maximum, tops)
    total = sum(jnp.exp2(t - top) * s for t, s in zip(tops, sums))
    return top, total


def inner_kernel(
    columns, size, feat, strip_ref, rows_ref, sums_ref, tops_ref, pixel_ref, score_ref, expo_ref
):
    width = strip_ref.shape[1]
    inner = width - 2 * LINE
    strip = strip_ref[...]
    shifted = [pltpu.roll(strip, 1, 1), strip, pltpu.roll(strip, width - 1, 1)]
    count = sums_ref.shape[0]
    blocks = [(slice(0, count), slice(at, at + size)) for at in range(0, inner, size)]
    half = count // 2
    halves = [(slice(r, r + half), b) for _, b in blocks for r in (0, half)]

    def run(explicit):
        flags = []

        def fill(turn):
            at, end = blocks[turn][1].start, blocks[turn][1].stop
            cells = [shifted[tap % 3][:, tap // 3 * LINE + at : tap // 3 * LINE + end] for tap in range(TAPS)]
            patches = jnp.concatenate(cells + [jnp.zeros_like(cells[0])], axis=0)
            real = (iota(patches.shape, 1) + at) % LINE < columns
            flags.append(fill_block(patches, real, explicit, feat, rows_ref, pixel_ref, at))

        for turn in range(len(blocks)):
            fill(turn)
        tops, sums = attend(halves, rows_ref, pixel_ref, score_ref, expo_ref)
        tops = [jnp.concatenate(tops[i : i + 2], axis=0) for i in range(0, len(tops), 2)]
        sums = [jnp.concatenate(sums[i : i + 2], axis=0) for i in range(0, len(sums), 2)]
        top, total = merged(tops, sums)
        sums_ref[...] = total
        tops_ref[...] = jnp.broadcast_to(top, tops_ref.shape)
        return [jnp.max(flag) for flag in flags if flag is not None]

    lost = functools.reduce(jnp.maximum, run(False))

    @pl.when(lost > 0.5)
    def _():
        run(True)


def border_kernel(
    columns,
    feat,
    strip_ref,
    after_ref,
    rows_ref,
    inner_sums_ref,
    inner_tops_ref,
    sent_ref,
    pixel_ref,
    score_ref,
    expo_ref,
):
    width = strip_ref.shape[1]
    lines = jnp.concatenate(
        [
            strip_ref[:, width - 2 * LINE :],
            after_ref[...].astype(F32),
            jnp.zeros((SUB, LINE), F32),
            strip_ref[:, : 2 * LINE],
        ],
        axis=1,
    )
    shifted = [pltpu.roll(lines, 1, 1), lines, pltpu.roll(lines, lines.shape[1] - 1, 1)]
    place_x = lax.axis_index("gx")
    below = (place_x < lax.axis_size("gx") - 1).astype(jnp.int32)
    count = sent_ref.shape[0]
    half = score_ref.shape[1] // 2
    shape = (2 * LANES, LANES)
    row, lane = iota(shape, 0), iota(shape, 1)
    tap = row % LANES
    target = jnp.where((tap < ONE) & (tap % SUB < 6), tap // SUB * 6 + tap % SUB, -1)
    target = jnp.where(tap == ONE, TOTAL, jnp.where(tap == ONE_TOO, TOTAL + 1, target))
    place = jnp.where((target >= 0) & (lane == target + row // LANES * SLOT), 1.0, 0.0).astype(BF16)

    def run(explicit, starts):
        cells = []
        for tap in range(TAPS):
            at = tap // 3 * LINE
            source = shifted[tap % 3]
            cells.append(jnp.concatenate([source[:, start + at : start + at + LINE] for start in starts], axis=1))
        patches = jnp.concatenate(cells + [jnp.zeros_like(cells[0])], axis=0)
        lane = iota(patches.shape, 1)
        real = (lane % LINE < columns) & (jnp.where(lane // LINE == 1, below, 1) > 0)
        lost = fill_block(patches, real, explicit, feat, rows_ref, pixel_ref, 0)
        blocks = [(slice(at, at + half), slice(0, patches.shape[1])) for at in (0, half)]
        tops, sums = attend(blocks, rows_ref, pixel_ref, score_ref, expo_ref)
        tops, sums = jnp.concatenate(tops, axis=0), jnp.concatenate(sums, axis=0)
        top, total = merged([inner_tops_ref[...], tops], [inner_sums_ref[...], sums])
        high = total.astype(BF16)
        low = (total - high.astype(F32)).astype(BF16)
        high = jnp.where(iota(total.shape, 1) == ONE_TOO, low, high)

        def side(values, odd):
            heads = range(odd, HEADS, 2)
            return jnp.concatenate([values[head * count : (head + 1) * count] for head in heads], axis=0)

        placed = nn(jnp.concatenate([side(high, 0), side(high, 1)], axis=1), place)
        lane = iota(placed.shape, 1)
        column = lane % SLOT
        one, two, three = thrice(jnp.where(lane < SLOT, side(top, 0), side(top, 1)))
        placed = jnp.where(column == TOP, one.astype(F32), placed)
        placed = jnp.where(column == TOP + 1, two.astype(F32), placed)
        placed = jnp.where(column == TOP + 2, three.astype(F32), placed).astype(BF16)
        for pair in range(HEADS // 2):
            sent_ref[:, pair * LANES : (pair + 1) * LANES] = placed[pair * count : (pair + 1) * count]
        return lost

    def checked(starts):
        lost = jnp.max(run(False, starts))

        @pl.when(lost > 0.5)
        def _():
            run(True, starts)

    @pl.when(place_x > 0)
    def _():
        checked([0, LINE])

    @pl.when(place_x == 0)
    def _():
        checked([0, LINE, 4 * LINE])


def output_kernel(conv_ref, gain_ref, value_ref, out_ref, both_ref):
    weight = conv_ref[...].astype(F32)
    weight = (weight - jnp.mean(weight, axis=-1, keepdims=True)) * gain_ref[...].reshape(1, -1)
    weight = jnp.concatenate([weight, jnp.zeros((SLOT - weight.shape[0], weight.shape[1]), F32)], axis=0)
    both = nn(jnp.concatenate(split_up(weight), axis=0), value_ref[...])
    high, low = split_up(both[:SLOT] + both[SLOT:])
    for head in range(HEADS):
        cut = slice(head * DH, (head + 1) * DH)
        both = nn(jnp.concatenate([high[:, cut], low[:, cut]], axis=0), out_ref[cut])
        both_ref[head * SLOT : (head + 1) * SLOT, :] = (both[:SLOT] + both[SLOT:]).astype(BF16)


def combine_kernel(parts_ref, both_ref, own_ref, result_ref):
    count, share, width = parts_ref.shape
    row, lane = iota((LANES, LANES), 0), iota((LANES, LANES), 1)
    same = row // SLOT == lane // SLOT
    column = row % SLOT
    pick_top = jnp.where(same & (column >= TOP) & (column < TOP + 3), 1.0, 0.0).astype(BF16)
    pick_one = jnp.where(same & (column >= TOTAL) & (column < TOTAL + 2), 1.0, 0.0).astype(BF16)
    means = []
    for at in range(0, width, LANES):
        values = parts_ref[:, :, at : at + LANES].astype(F32)
        parts = values.reshape(count * share, LANES).astype(BF16)
        tops = nn(parts, pick_top).reshape(values.shape)
        ones = nn(parts, pick_one).reshape(values.shape)
        factor = jnp.exp2(tops - jnp.max(tops, axis=0, keepdims=True))
        means.append(jnp.sum(factor * values, axis=0) / jnp.sum(factor * ones, axis=0))
    mean = jnp.concatenate(means, axis=1)
    high = mean.astype(BF16).astype(F32)
    result = nn(jnp.concatenate([high, mean - high], axis=0).astype(BF16), both_ref[...])
    result = own_ref[...].astype(F32) + (result[:share] + result[share:])
    result_ref[...] = result.astype(BF16)


def vmem(count):
    return [pl.BlockSpec(memory_space=pltpu.VMEM)] * count


def kernel(body, name, outs, scratch=(), others=0, count=0, cycles=1000, room=4):
    single = not isinstance(outs, (list, tuple))
    return pl.pallas_call(
        body,
        out_shape=outs,
        in_specs=vmem(count) + [pl.BlockSpec(memory_space=pltpu.HBM)] * others,
        out_specs=vmem(1)[0] if single else tuple(vmem(len(outs))),
        scratch_shapes=list(scratch),
        cost_estimate=pl.CostEstimate(flops=cycles * 4096, bytes_accessed=1 << 20, transcendentals=0),
        compiler_params=pltpu.CompilerParams(vmem_limit_bytes=room << 20),
        name=name,
    )


def on_device(
    pixels,
    conv_weight,
    input_gain,
    key_weight,
    value_weight,
    latents,
    latent_gain,
    query_weight,
    out_weight,
):
    tile_rows, tile_cols, _ = pixels.shape
    across, down = lax.axis_size("gy"), lax.axis_size("gx")
    columns = tile_cols * across
    feat = conv_weight.shape[1]
    lat, width = latents.shape
    share = lat // (across * down)
    held = lat // across

    def shape(dims, dtype=BF16):
        return jax.ShapeDtypeStruct(dims, dtype)

    copies = kernel(
        pack_kernel,
        "pack",
        shape((across, SUB, tile_rows * CELL)),
        [pltpu.VMEM((SUB * 16, LANES), F32)],
        count=1,
    )(pixels.transpose(2, 0, 1))
    tiles = lax.all_to_all(copies, "gy", 0, 0, tiled=True)
    rows = kernel(
        query_kernel,
        "query_rows",
        shape((HEADS * held + table_rows(feat), LINE)),
        [
            pltpu.VMEM(key_weight.shape, BF16),
            pltpu.VMEM(conv_weight.shape, BF16),
            pltpu.VMEM(input_gain.shape, F32),
            pltpu.VMEM((down, share, width), BF16),
            pltpu.VMEM(latent_gain.shape, F32),
            pltpu.VMEM(query_weight.shape, BF16),
            pltpu.SemaphoreType.DMA((6,)),
        ],
        others=6,
        cycles=6000,
        room=60,
    )(key_weight, conv_weight, input_gain, latents.reshape(down, across, share, width), latent_gain, query_weight)
    both = kernel(
        output_kernel, "value_output", shape((HEADS * SLOT, width)), count=4, cycles=6000, room=10
    )(conv_weight, input_gain, value_weight, out_weight)

    tiles, rows = lax.optimization_barrier((tiles, rows))
    strip, first = kernel(
        functools.partial(join_kernel, tile_cols),
        "join",
        [shape((SUB, tile_rows * LINE), F32), shape((SUB, 2 * LINE))],
        count=1,
        cycles=200000,
    )(tiles)
    after = lax.ppermute(first, "gx", [(i + 1, i) for i in range(down - 1)])
    inner = (tile_rows - 2) * LINE
    size = inner // 2
    sums, tops = kernel(
        functools.partial(inner_kernel, columns, size, feat),
        "inner",
        [shape((HEADS * held, LANES), F32), shape((HEADS * held, LANES), F32)],
        [
            pltpu.VMEM((LINE, inner), BF16),
            pltpu.VMEM((2, HEADS * held, size), F32),
            pltpu.VMEM((2, HEADS * held, size), BF16),
        ],
        count=2,
        cycles=10000,
        room=44,
    )(strip, rows)
    sent = kernel(
        functools.partial(border_kernel, columns, feat),
        "border",
        shape((held, HEADS * SLOT)),
        [
            pltpu.VMEM((LINE, 3 * LINE), BF16),
            pltpu.VMEM((2, HEADS * held, 3 * LINE), F32),
            pltpu.VMEM((2, HEADS * held, 3 * LINE), BF16),
        ],
        count=5,
        cycles=3000,
        room=24,
    )(strip, after, rows, sums, tops)
    parts = lax.all_to_all(sent.reshape(down, share, -1), "gx", 0, 0, tiled=True)
    own = lax.dynamic_slice_in_dim(latents, lax.axis_index(GROUP) * share, share, 0)
    return kernel(combine_kernel, "combine", shape((share, width)), count=3, room=6)(parts, both, own)


def solution(mesh):
    return jax.shard_map(
        on_device,
        mesh=mesh,
        in_specs=(P(("ba", "gx"), "gy", None), P(), P(), P(), P(), P(), P(), P(), P()),
        out_specs=P(("ba", "gx", "gy"), None),
        check_vma=False,
    )
```

```python
import functools

import jax
import jax.numpy as jnp
from jax import lax
from jax.experimental import pallas as pl
from jax.experimental.pallas import tpu as pltpu
from jax.sharding import PartitionSpec as P

HEADS = 8
DH = 128
LANES = 128
SUB = 8
TAPS = 9
CELL = 64
LINE = 256
SPAN = 80
ONE, MASK, ONE_TOO = 72, 73, 74
SLOT = 64
TOTAL, TOP = 54, 57
BIG = 1e30
EPS = 1e-05
LOG2E = 1.4426950408889634
GROUP = ("gx", "gy")
F32 = jnp.float32
BF16 = jnp.bfloat16


def product(a, b, left, right):
    return lax.dot_general(a, b, (((left,), (right,)), ((), ())), preferred_element_type=F32)


def nn(a, b):
    return product(a, b, 1, 0)


def nt(a, b):
    return product(a, b, 1, 1)


def tn(a, b):
    return product(a, b, 0, 0)


def iota(shape, dim):
    return lax.broadcasted_iota(jnp.int32, shape, dim)


def split_up(values):
    high = values.astype(BF16)
    return high, (values - high.astype(F32)).astype(BF16)


def thrice(values):
    one = values.astype(BF16)
    rest = values - one.astype(F32)
    two, three = split_up(rest)
    return one, two, three


def pack_kernel(pixel_ref, copies_ref, plane_ref):
    channels, rows, columns = pixel_ref.shape
    pitch = plane_ref.shape[0] // SUB
    plane_ref[...] = jnp.zeros(plane_ref.shape, F32)
    for channel in range(channels):
        plane_ref[channel * pitch : channel * pitch + rows, :columns] = pixel_ref[channel].astype(F32)
    for pair in range(rows // 2):
        even = plane_ref[pl.ds(2 * pair, SUB, stride=pitch), :]
        odd = plane_ref[pl.ds(2 * pair + 1, SUB, stride=pitch), :]
        packed = (even + pltpu.roll(odd, CELL, 1)).astype(BF16)
        for copy in range(copies_ref.shape[0]):
            copies_ref[copy, :, pair * LANES : (pair + 1) * LANES] = packed


def join_kernel(columns, tiles_ref, strip_ref, first_ref):
    tiles, _, width = tiles_ref.shape
    pairs = width // LANES
    lane = iota((pairs * SUB, LANES), 1)
    stacked = [
        jnp.concatenate([tiles_ref[tile, :, pair * LANES : (pair + 1) * LANES].astype(F32) for pair in range(pairs)], axis=0)
        for tile in range(tiles)
    ]
    for parity in range(2):
        halves = []
        for half in range(LINE // LANES):
            line = jnp.zeros((pairs * SUB, LANES), F32)
            for tile in range(tiles):
                start, end = tile * columns - half * LANES, (tile + 1) * columns - half * LANES
                if end <= 0 or start >= LANES:
                    continue
                moved = pltpu.roll(stacked[tile], (start - parity * CELL) % LANES, 1)
                line = jnp.where((lane >= start) & (lane < end), moved, line)
            halves.append(line)
        for pair in range(pairs):
            row = 2 * pair + parity
            for half, line in enumerate(halves):
                at = row * LINE + half * LANES
                strip_ref[:, at : at + LANES] = line[pair * SUB : (pair + 1) * SUB]
    first_ref[...] = strip_ref[:, : 2 * LINE].astype(BF16)


def spread_weight(conv_ref, copies):
    channels = conv_ref.shape[0] // TAPS
    shape = (copies, conv_ref.shape[0])
    row, tap = iota(shape, 0), iota(shape, 1)
    place = row % SPAN
    hit = (place // SUB == tap // channels) & (place % SUB == tap % channels) & (row < 3 * SPAN)
    spread = nn(jnp.where(hit, 1.0, 0.0).astype(BF16), conv_ref[...])
    return spread - jnp.mean(spread, axis=-1, keepdims=True)


def query_kernel(
    key_hbm, conv_hbm, gain_hbm, lat_hbm, lat_gain_hbm, query_hbm, rows_ref,
    key_ref, conv_ref, gain_ref, lat_ref, lat_gain_ref, query_ref, sems,
):
    sources = [key_hbm, conv_hbm, gain_hbm, lat_hbm.at[:, lax.axis_index("gy")], lat_gain_hbm, query_hbm]
    targets = [key_ref, conv_ref, gain_ref, lat_ref, lat_gain_ref, query_ref]
    copies = [pltpu.make_async_copy(*pair, sems.at[i]) for i, pair in enumerate(zip(sources, targets))]
    for copy in copies:
        copy.start()

    copies[1].wait()
    weight = spread_weight(conv_ref, SPAN)
    feat = weight.shape[1]
    high, low = split_up(weight)
    both = jnp.concatenate([high, low], axis=0)
    held = HEADS * lat_ref.shape[0] * lat_ref.shape[1]
    for part, at in enumerate(range(0, feat, LINE)):
        end = min(at + LINE, feat)
        first = held + LINE + part * 2 * SPAN
        rows_ref[first : first + 2 * SPAN, : end - at] = both[:, at:end]
    padding = jnp.zeros((LANES - SPAN, feat), BF16)
    gram = nt(both, jnp.concatenate([high, padding], axis=0)) + nt(both, jnp.concatenate([low, padding], axis=0))
    gram = (gram[:SPAN] + gram[SPAN:]) * (1.0 / feat)
    for part, piece in enumerate(thrice(gram)):
        rows_ref[held : held + SPAN, part * SPAN : (part + 1) * SPAN] = piece[:, :SPAN]

    copies[2].wait()
    copies[0].wait()
    keys = nn(jnp.concatenate(split_up(weight * gain_ref[...].reshape(1, -1)), axis=0), key_ref[...])
    high, low = split_up((keys[:SPAN] + keys[SPAN:]) * (LOG2E / DH**0.5))

    copies[3].wait()
    copies[4].wait()
    values = lat_ref[...].astype(F32)
    values = values.reshape(values.shape[0] * values.shape[1], values.shape[2])
    centred = values - jnp.mean(values, axis=-1, keepdims=True)
    variance = jnp.mean(centred * centred, axis=-1, keepdims=True)
    gain = lat_gain_ref[...].reshape(1, -1)
    normed = (centred * lax.rsqrt(variance + EPS) * gain).astype(BF16)
    copies[5].wait()
    queries = nn(normed, query_ref[...]).astype(BF16)

    count = values.shape[0]
    lane = iota((count, LINE), 1)
    padding = jnp.zeros((LINE - 3 * SPAN, 2 * DH), BF16)
    for head in range(HEADS):
        cut = slice(head * DH, (head + 1) * DH)
        query = jnp.concatenate([queries[:, cut], queries[:, cut]], axis=1)
        key = jnp.concatenate([high[:, cut], low[:, cut]], axis=1)
        rows = nt(query, jnp.concatenate([key, key, key, padding], axis=0))
        rows = jnp.where(lane == MASK, -1.0, rows)
        top, rest = split_up(rows)
        rows_ref[head * count : (head + 1) * count, :] = jnp.where((lane >= SPAN) & (lane < 2 * SPAN), rest, top)


def table_rows(feat):
    return LINE + -(-feat // LINE) * 2 * SPAN


def scaled_patches(patches, explicit, feat, rows_ref):
    exact = patches.astype(BF16)
    held = rows_ref.shape[0] - table_rows(feat)
    if explicit:
        total = 0.0
        for part, at in enumerate(range(0, feat, LINE)):
            end = min(at + LINE, feat)
            first = held + LINE + part * 2 * SPAN
            wide = rows_ref[first : first + 2 * SPAN, : end - at]
            features = tn(wide[:SPAN], exact) + tn(wide[SPAN:], exact)
            total = total + jnp.sum(features * features, axis=0, keepdims=True)
        variance = total * (1.0 / feat)
        lost = None
    else:
        gram = rows_ref[held : held + SPAN, : 3 * SPAN]
        form = nn(gram, jnp.concatenate([exact, exact, exact], axis=0))
        variance = jnp.maximum(jnp.sum(form * patches, axis=0, keepdims=True), 0.0)
        diag = jnp.where(iota(gram.shape, 0) == iota(gram.shape, 1), gram.astype(F32), 0.0)
        diag = jnp.sum(diag, axis=-1, keepdims=True)
        scale = jnp.sum(patches * patches * diag, axis=0, keepdims=True)
        lost = jnp.where((variance + EPS) * 128.0 < scale, 1.0, 0.0)
    return patches * lax.rsqrt(variance + EPS), lost


def fill_block(patches, real, explicit, feat, rows_ref, pixel_ref, at):
    width = patches.shape[1]
    scaled, lost = scaled_patches(patches, explicit, feat, rows_ref)
    row = iota((SPAN, width), 0)
    scaled = jnp.where((row == ONE) | (row == ONE_TOO), jnp.where(real, 1.0, 0.0), scaled)
    scaled = jnp.where(row == MASK, jnp.where(real, 0.0, BIG), scaled)
    high, low = split_up(scaled)
    cut = slice(at, at + width)
    pixel_ref[:SPAN, cut] = high
    pixel_ref[SPAN : 2 * SPAN, cut] = high
    pixel_ref[2 * SPAN : 3 * SPAN, cut] = low
    pixel_ref[3 * SPAN :, cut] = jnp.zeros((LINE - 3 * SPAN, width), BF16)
    return lost


def attend(blocks, rows_ref, pixel_ref, score_ref, expo_ref):
    tops, sums = [], []
    count = len(blocks)
    for turn in range(count + 2):
        if turn < count:
            rows, cut = blocks[turn]
            score_ref[turn % 2, rows, : cut.stop - cut.start] = nn(rows_ref[rows], pixel_ref[:, cut])
        if 0 <= turn - 1 < count:
            rows, cut = blocks[turn - 1]
            at = ((turn - 1) % 2, rows, slice(0, cut.stop - cut.start))
            top = jnp.max(score_ref[at], axis=-1, keepdims=True)
            expo_ref[at] = jnp.exp2(score_ref[at] - top).astype(BF16)
            tops.append(top)
        if 0 <= turn - 2 < count:
            rows, cut = blocks[turn - 2]
            at = ((turn - 2) % 2, rows, slice(0, cut.stop - cut.start))
            sums.append(nt(expo_ref[at], pixel_ref[:LANES, cut]))
    return tops, sums


def merged(tops, sums):
    top = functools.reduce(jnp.maximum, tops)
    total = sum(jnp.exp2(t - top) * s for t, s in zip(tops, sums))
    return top, total


def inner_kernel(
    columns, size, feat, strip_ref, rows_ref, sums_ref, tops_ref, pixel_ref, score_ref, expo_ref
):
    width = strip_ref.shape[1]
    inner = width - 2 * LINE
    strip = strip_ref[...]
    shifted = [pltpu.roll(strip, 1, 1), strip, pltpu.roll(strip, width - 1, 1)]
    count = sums_ref.shape[0]
    blocks = [(slice(0, count), slice(at, at + size)) for at in range(0, inner, size)]
    half = count // 2
    halves = [(slice(r, r + half), b) for _, b in blocks for r in (0, half)]

    def run(explicit):
        flags = []

        def fill(turn):
            at, end = blocks[turn][1].start, blocks[turn][1].stop
            cells = [shifted[tap % 3][:, tap // 3 * LINE + at : tap // 3 * LINE + end] for tap in range(TAPS)]
            patches = jnp.concatenate(cells + [jnp.zeros_like(cells[0])], axis=0)
            real = (iota(patches.shape, 1) + at) % LINE < columns
            flags.append(fill_block(patches, real, explicit, feat, rows_ref, pixel_ref, at))

        for turn in range(len(blocks)):
            fill(turn)
        tops, sums = attend(halves, rows_ref, pixel_ref, score_ref, expo_ref)
        tops = [jnp.concatenate(tops[i : i + 2], axis=0) for i in range(0, len(tops), 2)]
        sums = [jnp.concatenate(sums[i : i + 2], axis=0) for i in range(0, len(sums), 2)]
        top, total = merged(tops, sums)
        sums_ref[...] = total
        tops_ref[...] = jnp.broadcast_to(top, tops_ref.shape)
        return [jnp.max(flag) for flag in flags if flag is not None]

    lost = functools.reduce(jnp.maximum, run(False))

    @pl.when(lost > 0.5)
    def _():
        run(True)


def border_kernel(
    columns,
    feat,
    strip_ref,
    after_ref,
    rows_ref,
    inner_sums_ref,
    inner_tops_ref,
    sent_ref,
    pixel_ref,
    score_ref,
    expo_ref,
):
    width = strip_ref.shape[1]
    lines = jnp.concatenate(
        [
            strip_ref[:, width - 2 * LINE :],
            after_ref[...].astype(F32),
            jnp.zeros((SUB, LINE), F32),
            strip_ref[:, : 2 * LINE],
        ],
        axis=1,
    )
    shifted = [pltpu.roll(lines, 1, 1), lines, pltpu.roll(lines, lines.shape[1] - 1, 1)]
    place_x = lax.axis_index("gx")
    below = (place_x < lax.axis_size("gx") - 1).astype(jnp.int32)
    count = sent_ref.shape[0]
    half = score_ref.shape[1] // 2
    shape = (2 * LANES, LANES)
    row, lane = iota(shape, 0), iota(shape, 1)
    tap = row % LANES
    target = jnp.where((tap < ONE) & (tap % SUB < 6), tap // SUB * 6 + tap % SUB, -1)
    target = jnp.where(tap == ONE, TOTAL, jnp.where(tap == ONE_TOO, TOTAL + 1, target))
    place = jnp.where((target >= 0) & (lane == target + row // LANES * SLOT), 1.0, 0.0).astype(BF16)

    def run(explicit, starts):
        cells = []
        for tap in range(TAPS):
            at = tap // 3 * LINE
            source = shifted[tap % 3]
            cells.append(jnp.concatenate([source[:, start + at : start + at + LINE] for start in starts], axis=1))
        patches = jnp.concatenate(cells + [jnp.zeros_like(cells[0])], axis=0)
        lane = iota(patches.shape, 1)
        real = (lane % LINE < columns) & (jnp.where(lane // LINE == 1, below, 1) > 0)
        lost = fill_block(patches, real, explicit, feat, rows_ref, pixel_ref, 0)
        blocks = [(slice(at, at + half), slice(0, patches.shape[1])) for at in (0, half)]
        tops, sums = attend(blocks, rows_ref, pixel_ref, score_ref, expo_ref)
        tops, sums = jnp.concatenate(tops, axis=0), jnp.concatenate(sums, axis=0)
        top, total = merged([inner_tops_ref[...], tops], [inner_sums_ref[...], sums])
        high = total.astype(BF16)
        low = (total - high.astype(F32)).astype(BF16)
        high = jnp.where(iota(total.shape, 1) == ONE_TOO, low, high)

        def side(values, odd):
            heads = range(odd, HEADS, 2)
            return jnp.concatenate([values[head * count : (head + 1) * count] for head in heads], axis=0)

        placed = nn(jnp.concatenate([side(high, 0), side(high, 1)], axis=1), place)
        lane = iota(placed.shape, 1)
        column = lane % SLOT
        one, two, three = thrice(jnp.where(lane < SLOT, side(top, 0), side(top, 1)))
        placed = jnp.where(column == TOP, one.astype(F32), placed)
        placed = jnp.where(column == TOP + 1, two.astype(F32), placed)
        placed = jnp.where(column == TOP + 2, three.astype(F32), placed).astype(BF16)
        for pair in range(HEADS // 2):
            sent_ref[:, pair * LANES : (pair + 1) * LANES] = placed[pair * count : (pair + 1) * count]
        return lost

    def checked(starts):
        lost = jnp.max(run(False, starts))

        @pl.when(lost > 0.5)
        def _():
            run(True, starts)

    @pl.when(place_x > 0)
    def _():
        checked([0, LINE])

    @pl.when(place_x == 0)
    def _():
        checked([0, LINE, 4 * LINE])


def output_kernel(conv_ref, gain_ref, value_ref, out_ref, both_ref):
    weight = conv_ref[...].astype(F32)
    weight = (weight - jnp.mean(weight, axis=-1, keepdims=True)) * gain_ref[...].reshape(1, -1)
    weight = jnp.concatenate([weight, jnp.zeros((SLOT - weight.shape[0], weight.shape[1]), F32)], axis=0)
    both = nn(jnp.concatenate(split_up(weight), axis=0), value_ref[...])
    high, low = split_up(both[:SLOT] + both[SLOT:])
    for head in range(HEADS):
        cut = slice(head * DH, (head + 1) * DH)
        both = nn(jnp.concatenate([high[:, cut], low[:, cut]], axis=0), out_ref[cut])
        both_ref[head * SLOT : (head + 1) * SLOT, :] = (both[:SLOT] + both[SLOT:]).astype(BF16)


def combine_kernel(parts_ref, both_ref, own_ref, result_ref):
    count, share, width = parts_ref.shape
    row, lane = iota((LANES, LANES), 0), iota((LANES, LANES), 1)
    same = row // SLOT == lane // SLOT
    column = row % SLOT
    pick_top = jnp.where(same & (column >= TOP) & (column < TOP + 3), 1.0, 0.0).astype(BF16)
    pick_one = jnp.where(same & (column >= TOTAL) & (column < TOTAL + 2), 1.0, 0.0).astype(BF16)
    means = []
    for at in range(0, width, LANES):
        values = parts_ref[:, :, at : at + LANES].astype(F32)
        parts = values.reshape(count * share, LANES).astype(BF16)
        tops = nn(parts, pick_top).reshape(values.shape)
        ones = nn(parts, pick_one).reshape(values.shape)
        factor = jnp.exp2(tops - jnp.max(tops, axis=0, keepdims=True))
        means.append(jnp.sum(factor * values, axis=0) / jnp.sum(factor * ones, axis=0))
    mean = jnp.concatenate(means, axis=1)
    high = mean.astype(BF16).astype(F32)
    result = nn(jnp.concatenate([high, mean - high], axis=0).astype(BF16), both_ref[...])
    result = own_ref[...].astype(F32) + (result[:share] + result[share:])
    result_ref[...] = result.astype(BF16)


def vmem(count):
    return [pl.BlockSpec(memory_space=pltpu.VMEM)] * count


def kernel(body, name, outs, scratch=(), others=0, count=0, cycles=1000, room=4):
    single = not isinstance(outs, (list, tuple))
    return pl.pallas_call(
        body,
        out_shape=outs,
        in_specs=vmem(count) + [pl.BlockSpec(memory_space=pltpu.HBM)] * others,
        out_specs=vmem(1)[0] if single else tuple(vmem(len(outs))),
        scratch_shapes=list(scratch),
        cost_estimate=pl.CostEstimate(flops=cycles * 4096, bytes_accessed=1 << 20, transcendentals=0),
        compiler_params=pltpu.CompilerParams(vmem_limit_bytes=int(room * 1024) << 10),
        name=name,
    )


def on_device(
    pixels,
    conv_weight,
    input_gain,
    key_weight,
    value_weight,
    latents,
    latent_gain,
    query_weight,
    out_weight,
):
    tile_rows, tile_cols, _ = pixels.shape
    across, down = lax.axis_size("gy"), lax.axis_size("gx")
    columns = tile_cols * across
    feat = conv_weight.shape[1]
    lat, width = latents.shape
    share = lat // (across * down)
    held = lat // across

    def shape(dims, dtype=BF16):
        return jax.ShapeDtypeStruct(dims, dtype)

    copies = kernel(
        pack_kernel,
        "pack",
        shape((across, SUB, tile_rows * CELL)),
        [pltpu.VMEM((SUB * 16, LANES), F32)],
        count=1,
        cycles=1000000,
    )(pixels.transpose(2, 0, 1))
    tiles = lax.all_to_all(copies, "gy", 0, 0, tiled=True)
    rows = kernel(
        query_kernel,
        "query_rows",
        shape((HEADS * held + table_rows(feat), LINE)),
        [
            pltpu.VMEM(key_weight.shape, BF16),
            pltpu.VMEM(conv_weight.shape, BF16),
            pltpu.VMEM(input_gain.shape, F32),
            pltpu.VMEM((down, share, width), BF16),
            pltpu.VMEM(latent_gain.shape, F32),
            pltpu.VMEM(query_weight.shape, BF16),
            pltpu.SemaphoreType.DMA((6,)),
        ],
        others=6,
        cycles=6000,
        room=52.7,
    )(key_weight, conv_weight, input_gain, latents.reshape(down, across, share, width), latent_gain, query_weight)
    both = kernel(
        output_kernel, "value_output", shape((HEADS * SLOT, width)), count=4, cycles=6000, room=10
    )(conv_weight, input_gain, value_weight, out_weight)

    tiles, rows = lax.optimization_barrier((tiles, rows))
    strip, first = kernel(
        functools.partial(join_kernel, tile_cols),
        "join",
        [shape((SUB, tile_rows * LINE), F32), shape((SUB, 2 * LINE))],
        count=1,
        cycles=200000,
    )(tiles)
    after = lax.ppermute(first, "gx", [(i + 1, i) for i in range(down - 1)])
    inner = (tile_rows - 2) * LINE
    size = inner // 2
    sums, tops = kernel(
        functools.partial(inner_kernel, columns, size, feat),
        "inner",
        [shape((HEADS * held, LANES), F32), shape((HEADS * held, LANES), F32)],
        [
            pltpu.VMEM((LINE, inner), BF16),
            pltpu.VMEM((2, HEADS * held, size), F32),
            pltpu.VMEM((2, HEADS * held, size), BF16),
        ],
        count=2,
        cycles=10000,
        room=44,
    )(strip, rows)
    sent = kernel(
        functools.partial(border_kernel, columns, feat),
        "border",
        shape((held, HEADS * SLOT)),
        [
            pltpu.VMEM((LINE, 3 * LINE), BF16),
            pltpu.VMEM((2, HEADS * held, 3 * LINE), F32),
            pltpu.VMEM((2, HEADS * held, 3 * LINE), BF16),
        ],
        count=5,
        cycles=3000,
        room=24,
    )(strip, after, rows, sums, tops)
    parts = lax.all_to_all(sent.reshape(down, share, -1), "gx", 0, 0, tiled=True)
    own = lax.dynamic_slice_in_dim(latents, lax.axis_index(GROUP) * share, share, 0)
    return kernel(combine_kernel, "combine", shape((share, width)), count=3, room=6)(parts, both, own)


def solution(mesh):
    return jax.shard_map(
        on_device,
        mesh=mesh,
        in_specs=(P(("ba", "gx"), "gy", None), P(), P(), P(), P(), P(), P(), P(), P()),
        out_specs=P(("ba", "gx", "gy"), None),
        check_vma=False,
    )
```

```python
import functools

import jax
import jax.numpy as jnp
from jax import lax
from jax.experimental import pallas as pl
from jax.experimental.pallas import tpu as pltpu
from jax.sharding import PartitionSpec as P

HEADS = 8
DH = 128
LANES = 128
SUB = 8
TAPS = 9
CELL = 64
LINE = 256
SPAN = 80
ONE, MASK, ONE_TOO = 72, 73, 74
SLOT = 64
TOTAL, TOP = 54, 57
BIG = 1e30
EPS = 1e-05
LOG2E = 1.4426950408889634
GROUP = ("gx", "gy")
F32 = jnp.float32
BF16 = jnp.bfloat16


def product(a, b, left, right):
    return lax.dot_general(a, b, (((left,), (right,)), ((), ())), preferred_element_type=F32)


def nn(a, b):
    return product(a, b, 1, 0)


def nt(a, b):
    return product(a, b, 1, 1)


def tn(a, b):
    return product(a, b, 0, 0)


def iota(shape, dim):
    return lax.broadcasted_iota(jnp.int32, shape, dim)


def split_up(values):
    high = values.astype(BF16)
    return high, (values - high.astype(F32)).astype(BF16)


def thrice(values):
    one = values.astype(BF16)
    rest = values - one.astype(F32)
    two, three = split_up(rest)
    return one, two, three


def pack_kernel(pixel_ref, copies_ref, plane_ref):
    channels, rows, columns = pixel_ref.shape
    pitch = plane_ref.shape[0] // SUB
    plane_ref[...] = jnp.zeros(plane_ref.shape, F32)
    for channel in range(channels):
        plane_ref[channel * pitch : channel * pitch + rows, :columns] = pixel_ref[channel].astype(F32)
    for pair in range(rows // 2):
        even = plane_ref[pl.ds(2 * pair, SUB, stride=pitch), :]
        odd = plane_ref[pl.ds(2 * pair + 1, SUB, stride=pitch), :]
        packed = (even + pltpu.roll(odd, CELL, 1)).astype(BF16)
        for copy in range(copies_ref.shape[0]):
            copies_ref[copy, :, pair * LANES : (pair + 1) * LANES] = packed


def join_kernel(columns, tiles_ref, strip_ref, first_ref):
    tiles, _, width = tiles_ref.shape
    pairs = width // LANES
    lane = iota((pairs * SUB, LANES), 1)
    stacked = [
        jnp.concatenate([tiles_ref[tile, :, pair * LANES : (pair + 1) * LANES].astype(F32) for pair in range(pairs)], axis=0)
        for tile in range(tiles)
    ]
    for parity in range(2):
        halves = []
        for half in range(LINE // LANES):
            line = jnp.zeros((pairs * SUB, LANES), F32)
            for tile in range(tiles):
                start, end = tile * columns - half * LANES, (tile + 1) * columns - half * LANES
                if end <= 0 or start >= LANES:
                    continue
                moved = pltpu.roll(stacked[tile], (start - parity * CELL) % LANES, 1)
                line = jnp.where((lane >= start) & (lane < end), moved, line)
            halves.append(line)
        for pair in range(pairs):
            row = 2 * pair + parity
            for half, line in enumerate(halves):
                at = row * LINE + half * LANES
                strip_ref[:, at : at + LANES] = line[pair * SUB : (pair + 1) * SUB]
    first_ref[...] = strip_ref[:, : 2 * LINE].astype(BF16)


def spread_weight(conv_ref, copies):
    channels = conv_ref.shape[0] // TAPS
    shape = (copies, conv_ref.shape[0])
    row, tap = iota(shape, 0), iota(shape, 1)
    place = row % SPAN
    hit = (place // SUB == tap // channels) & (place % SUB == tap % channels) & (row < 3 * SPAN)
    spread = nn(jnp.where(hit, 1.0, 0.0).astype(BF16), conv_ref[...])
    return spread - jnp.mean(spread, axis=-1, keepdims=True)


def query_kernel(
    key_hbm, conv_hbm, gain_hbm, lat_hbm, lat_gain_hbm, query_hbm, rows_ref,
    key_ref, conv_ref, gain_ref, lat_ref, lat_gain_ref, query_ref, sems,
):
    sources = [key_hbm, conv_hbm, gain_hbm, lat_hbm.at[:, lax.axis_index("gy")], lat_gain_hbm, query_hbm]
    targets = [key_ref, conv_ref, gain_ref, lat_ref, lat_gain_ref, query_ref]
    copies = [pltpu.make_async_copy(*pair, sems.at[i]) for i, pair in enumerate(zip(sources, targets))]
    for copy in copies:
        copy.start()

    copies[1].wait()
    weight = spread_weight(conv_ref, SPAN)
    feat = weight.shape[1]
    high, low = split_up(weight)
    both = jnp.concatenate([high, low], axis=0)
    held = HEADS * lat_ref.shape[0] * lat_ref.shape[1]
    for part, at in enumerate(range(0, feat, LINE)):
        end = min(at + LINE, feat)
        first = held + LINE + part * 2 * SPAN
        rows_ref[first : first + 2 * SPAN, : end - at] = both[:, at:end]
    padding = jnp.zeros((LANES - SPAN, feat), BF16)
    gram = nt(both, jnp.concatenate([high, padding], axis=0)) + nt(both, jnp.concatenate([low, padding], axis=0))
    gram = (gram[:SPAN] + gram[SPAN:]) * (1.0 / feat)
    for part, piece in enumerate(thrice(gram)):
        rows_ref[held : held + SPAN, part * SPAN : (part + 1) * SPAN] = piece[:, :SPAN]

    copies[2].wait()
    copies[0].wait()
    keys = nn(jnp.concatenate(split_up(weight * gain_ref[...].reshape(1, -1)), axis=0), key_ref[...])
    high, low = split_up((keys[:SPAN] + keys[SPAN:]) * (LOG2E / DH**0.5))

    copies[3].wait()
    copies[4].wait()
    values = lat_ref[...].astype(F32)
    values = values.reshape(values.shape[0] * values.shape[1], values.shape[2])
    centred = values - jnp.mean(values, axis=-1, keepdims=True)
    variance = jnp.mean(centred * centred, axis=-1, keepdims=True)
    gain = lat_gain_ref[...].reshape(1, -1)
    normed = (centred * lax.rsqrt(variance + EPS) * gain).astype(BF16)
    copies[5].wait()
    queries = nn(normed, query_ref[...]).astype(BF16)

    count = values.shape[0]
    lane = iota((count, LINE), 1)
    padding = jnp.zeros((LINE - 3 * SPAN, 2 * DH), BF16)
    for head in range(HEADS):
        cut = slice(head * DH, (head + 1) * DH)
        query = jnp.concatenate([queries[:, cut], queries[:, cut]], axis=1)
        key = jnp.concatenate([high[:, cut], low[:, cut]], axis=1)
        rows = nt(query, jnp.concatenate([key, key, key, padding], axis=0))
        rows = jnp.where(lane == MASK, -1.0, rows)
        top, rest = split_up(rows)
        rows_ref[head * count : (head + 1) * count, :] = jnp.where((lane >= SPAN) & (lane < 2 * SPAN), rest, top)


def table_rows(feat):
    return LINE + -(-feat // LINE) * 2 * SPAN


def scaled_patches(patches, explicit, feat, rows_ref):
    exact = patches.astype(BF16)
    held = rows_ref.shape[0] - table_rows(feat)
    if explicit:
        total = 0.0
        for part, at in enumerate(range(0, feat, LINE)):
            end = min(at + LINE, feat)
            first = held + LINE + part * 2 * SPAN
            wide = rows_ref[first : first + 2 * SPAN, : end - at]
            features = tn(wide[:SPAN], exact) + tn(wide[SPAN:], exact)
            total = total + jnp.sum(features * features, axis=0, keepdims=True)
        variance = total * (1.0 / feat)
        lost = None
    else:
        gram = rows_ref[held : held + SPAN, : 3 * SPAN]
        form = nn(gram, jnp.concatenate([exact, exact, exact], axis=0))
        variance = jnp.maximum(jnp.sum(form * patches, axis=0, keepdims=True), 0.0)
        diag = jnp.where(iota(gram.shape, 0) == iota(gram.shape, 1), gram.astype(F32), 0.0)
        diag = jnp.sum(diag, axis=-1, keepdims=True)
        scale = jnp.sum(patches * patches * diag, axis=0, keepdims=True)
        lost = jnp.where((variance + EPS) * 128.0 < scale, 1.0, 0.0)
    return patches * lax.rsqrt(variance + EPS), lost


def fill_block(patches, real, explicit, feat, rows_ref, pixel_ref, at):
    width = patches.shape[1]
    scaled, lost = scaled_patches(patches, explicit, feat, rows_ref)
    row = iota((SPAN, width), 0)
    scaled = jnp.where((row == ONE) | (row == ONE_TOO), jnp.where(real, 1.0, 0.0), scaled)
    scaled = jnp.where(row == MASK, jnp.where(real, 0.0, BIG), scaled)
    high, low = split_up(scaled)
    cut = slice(at, at + width)
    pixel_ref[:SPAN, cut] = high
    pixel_ref[SPAN : 2 * SPAN, cut] = high
    pixel_ref[2 * SPAN : 3 * SPAN, cut] = low
    pixel_ref[3 * SPAN :, cut] = jnp.zeros((LINE - 3 * SPAN, width), BF16)
    return lost


def attend(blocks, rows_ref, pixel_ref, score_ref, expo_ref, take):
    tops = []
    count = len(blocks)
    for turn in range(count + 2):
        if turn < count:
            rows, cut = blocks[turn]
            score_ref[turn % 2, rows, : cut.stop - cut.start] = nn(rows_ref[rows], pixel_ref[:, cut])
        if 0 <= turn - 1 < count:
            rows, cut = blocks[turn - 1]
            at = ((turn - 1) % 2, rows, slice(0, cut.stop - cut.start))
            top = jnp.max(score_ref[at], axis=-1, keepdims=True)
            expo_ref[at] = jnp.exp2(score_ref[at] - top).astype(BF16)
            tops.append(top)
        if 0 <= turn - 2 < count:
            rows, cut = blocks[turn - 2]
            at = ((turn - 2) % 2, rows, slice(0, cut.stop - cut.start))
            take(turn - 2, tops[turn - 2], nt(expo_ref[at], pixel_ref[:LANES, cut]))


def merged(old_top, old_sums, top, sums):
    new = jnp.maximum(old_top, top)
    return new, jnp.exp2(old_top - new) * old_sums + jnp.exp2(top - new) * sums


def inner_kernel(
    columns, size, feat, strip_ref, rows_ref, sums_ref, tops_ref, pixel_ref, score_ref, expo_ref
):
    width = strip_ref.shape[1]
    inner = width - 2 * LINE
    strip = strip_ref[...]
    shifted = [pltpu.roll(strip, 1, 1), strip, pltpu.roll(strip, width - 1, 1)]
    count = sums_ref.shape[0]
    blocks = [(slice(0, count), slice(at, at + size)) for at in range(0, inner, size)]
    half = count // 2
    halves = [(slice(r, r + half), b) for _, b in blocks for r in (0, half)]

    def run(explicit):
        flags = []

        def fill(turn):
            at, end = blocks[turn][1].start, blocks[turn][1].stop
            cells = [shifted[tap % 3][:, tap // 3 * LINE + at : tap // 3 * LINE + end] for tap in range(TAPS)]
            patches = jnp.concatenate(cells + [jnp.zeros_like(cells[0])], axis=0)
            real = (iota(patches.shape, 1) + at) % LINE < columns
            flags.append(fill_block(patches, real, explicit, feat, rows_ref, pixel_ref, at))

        for turn in range(len(blocks)):
            fill(turn)
        def take(turn, top, sums):
            rows, cut = halves[turn]
            if cut.start > 0:
                top, sums = merged(tops_ref[rows], sums_ref[rows], top, sums)
            sums_ref[rows] = sums
            tops_ref[rows] = jnp.broadcast_to(top, sums.shape)

        attend(halves, rows_ref, pixel_ref, score_ref, expo_ref, take)
        return [jnp.max(flag) for flag in flags if flag is not None]

    lost = functools.reduce(jnp.maximum, run(False))

    @pl.when(lost > 0.5)
    def _():
        run(True)


def border_kernel(
    columns,
    feat,
    strip_ref,
    after_ref,
    rows_ref,
    inner_sums_ref,
    inner_tops_ref,
    sent_ref,
    pixel_ref,
    score_ref,
    expo_ref,
):
    width = strip_ref.shape[1]
    lines = jnp.concatenate(
        [
            strip_ref[:, width - 2 * LINE :],
            after_ref[...].astype(F32),
            jnp.zeros((SUB, LINE), F32),
            strip_ref[:, : 2 * LINE],
        ],
        axis=1,
    )
    shifted = [pltpu.roll(lines, 1, 1), lines, pltpu.roll(lines, lines.shape[1] - 1, 1)]
    place_x = lax.axis_index("gx")
    below = (place_x < lax.axis_size("gx") - 1).astype(jnp.int32)
    count = sent_ref.shape[0]
    half = score_ref.shape[1] // 2
    shape = (2 * LANES, LANES)
    row, lane = iota(shape, 0), iota(shape, 1)
    tap = row % LANES
    target = jnp.where((tap < ONE) & (tap % SUB < 6), tap // SUB * 6 + tap % SUB, -1)
    target = jnp.where(tap == ONE, TOTAL, jnp.where(tap == ONE_TOO, TOTAL + 1, target))
    place = jnp.where((target >= 0) & (lane == target + row // LANES * SLOT), 1.0, 0.0).astype(BF16)

    def run(explicit, starts):
        cells = []
        for tap in range(TAPS):
            at = tap // 3 * LINE
            source = shifted[tap % 3]
            cells.append(jnp.concatenate([source[:, start + at : start + at + LINE] for start in starts], axis=1))
        patches = jnp.concatenate(cells + [jnp.zeros_like(cells[0])], axis=0)
        lane = iota(patches.shape, 1)
        real = (lane % LINE < columns) & (jnp.where(lane // LINE == 1, below, 1) > 0)
        lost = fill_block(patches, real, explicit, feat, rows_ref, pixel_ref, 0)
        blocks = [(slice(at, at + half), slice(0, patches.shape[1])) for at in (0, half)]

        def take(turn, top, sums):
            rows = blocks[turn][0]
            top, total = merged(inner_tops_ref[rows], inner_sums_ref[rows], top, sums)
            high = total.astype(BF16)
            low = (total - high.astype(F32)).astype(BF16)
            high = jnp.where(iota(total.shape, 1) == ONE_TOO, low, high)

            def side(values, odd):
                heads = range(odd, half // count, 2)
                return jnp.concatenate([values[head * count : (head + 1) * count] for head in heads], axis=0)

            placed = nn(jnp.concatenate([side(high, 0), side(high, 1)], axis=1), place)
            lane = iota(placed.shape, 1)
            column = lane % SLOT
            one, two, three = thrice(jnp.where(lane < SLOT, side(top, 0), side(top, 1)))
            placed = jnp.where(column == TOP, one.astype(F32), placed)
            placed = jnp.where(column == TOP + 1, two.astype(F32), placed)
            placed = jnp.where(column == TOP + 2, three.astype(F32), placed).astype(BF16)
            first = rows.start // count // 2
            for pair in range(half // count // 2):
                at = (first + pair) * LANES
                sent_ref[:, at : at + LANES] = placed[pair * count : (pair + 1) * count]

        attend(blocks, rows_ref, pixel_ref, score_ref, expo_ref, take)
        return lost

    def checked(starts):
        lost = jnp.max(run(False, starts))

        @pl.when(lost > 0.5)
        def _():
            run(True, starts)

    @pl.when(place_x > 0)
    def _():
        checked([0, LINE])

    @pl.when(place_x == 0)
    def _():
        checked([0, LINE, 4 * LINE])


def output_kernel(conv_ref, gain_ref, value_ref, out_ref, both_ref):
    weight = conv_ref[...].astype(F32)
    weight = (weight - jnp.mean(weight, axis=-1, keepdims=True)) * gain_ref[...].reshape(1, -1)
    weight = jnp.concatenate([weight, jnp.zeros((SLOT - weight.shape[0], weight.shape[1]), F32)], axis=0)
    both = nn(jnp.concatenate(split_up(weight), axis=0), value_ref[...])
    high, low = split_up(both[:SLOT] + both[SLOT:])
    for head in range(HEADS):
        cut = slice(head * DH, (head + 1) * DH)
        both = nn(jnp.concatenate([high[:, cut], low[:, cut]], axis=0), out_ref[cut])
        both_ref[head * SLOT : (head + 1) * SLOT, :] = (both[:SLOT] + both[SLOT:]).astype(BF16)


def combine_kernel(parts_ref, both_ref, own_ref, result_ref):
    count, share, width = parts_ref.shape
    row, lane = iota((LANES, LANES), 0), iota((LANES, LANES), 1)
    same = row // SLOT == lane // SLOT
    column = row % SLOT
    pick_top = jnp.where(same & (column >= TOP) & (column < TOP + 3), 1.0, 0.0).astype(BF16)
    pick_one = jnp.where(same & (column >= TOTAL) & (column < TOTAL + 2), 1.0, 0.0).astype(BF16)
    means = []
    for at in range(0, width, LANES):
        values = parts_ref[:, :, at : at + LANES].astype(F32)
        parts = values.reshape(count * share, LANES).astype(BF16)
        tops = nn(parts, pick_top).reshape(values.shape)
        ones = nn(parts, pick_one).reshape(values.shape)
        factor = jnp.exp2(tops - jnp.max(tops, axis=0, keepdims=True))
        means.append(jnp.sum(factor * values, axis=0) / jnp.sum(factor * ones, axis=0))
    mean = jnp.concatenate(means, axis=1)
    high = mean.astype(BF16).astype(F32)
    result = nn(jnp.concatenate([high, mean - high], axis=0).astype(BF16), both_ref[...])
    result = own_ref[...].astype(F32) + (result[:share] + result[share:])
    result_ref[...] = result.astype(BF16)


def vmem(count):
    return [pl.BlockSpec(memory_space=pltpu.VMEM)] * count


def kernel(body, name, outs, scratch=(), others=0, count=0, cycles=1000, room=4):
    single = not isinstance(outs, (list, tuple))
    return pl.pallas_call(
        body,
        out_shape=outs,
        in_specs=vmem(count) + [pl.BlockSpec(memory_space=pltpu.HBM)] * others,
        out_specs=vmem(1)[0] if single else tuple(vmem(len(outs))),
        scratch_shapes=list(scratch),
        cost_estimate=pl.CostEstimate(flops=cycles * 4096, bytes_accessed=1 << 20, transcendentals=0),
        compiler_params=pltpu.CompilerParams(vmem_limit_bytes=int(room * 1024) << 10),
        name=name,
    )


def on_device(
    pixels,
    conv_weight,
    input_gain,
    key_weight,
    value_weight,
    latents,
    latent_gain,
    query_weight,
    out_weight,
):
    tile_rows, tile_cols, _ = pixels.shape
    across, down = lax.axis_size("gy"), lax.axis_size("gx")
    columns = tile_cols * across
    feat = conv_weight.shape[1]
    lat, width = latents.shape
    share = lat // (across * down)
    held = lat // across

    def shape(dims, dtype=BF16):
        return jax.ShapeDtypeStruct(dims, dtype)

    copies = kernel(
        pack_kernel,
        "pack",
        shape((across, SUB, tile_rows * CELL)),
        [pltpu.VMEM((SUB * 16, LANES), F32)],
        count=1,
        cycles=1000000,
    )(pixels.transpose(2, 0, 1))
    tiles = lax.all_to_all(copies, "gy", 0, 0, tiled=True)
    rows = kernel(
        query_kernel,
        "query_rows",
        shape((HEADS * held + table_rows(feat), LINE)),
        [
            pltpu.VMEM(key_weight.shape, BF16),
            pltpu.VMEM(conv_weight.shape, BF16),
            pltpu.VMEM(input_gain.shape, F32),
            pltpu.VMEM((down, share, width), BF16),
            pltpu.VMEM(latent_gain.shape, F32),
            pltpu.VMEM(query_weight.shape, BF16),
            pltpu.SemaphoreType.DMA((6,)),
        ],
        others=6,
        cycles=6000,
        room=52.7,
    )(key_weight, conv_weight, input_gain, latents.reshape(down, across, share, width), latent_gain, query_weight)
    both = kernel(
        output_kernel, "value_output", shape((HEADS * SLOT, width)), count=4, cycles=6000, room=10
    )(conv_weight, input_gain, value_weight, out_weight)

    tiles, rows = lax.optimization_barrier((tiles, rows))
    strip, first = kernel(
        functools.partial(join_kernel, tile_cols),
        "join",
        [shape((SUB, tile_rows * LINE), F32), shape((SUB, 2 * LINE))],
        count=1,
        cycles=200000,
    )(tiles)
    after = lax.ppermute(first, "gx", [(i + 1, i) for i in range(down - 1)])
    inner = (tile_rows - 2) * LINE
    size = inner // 4
    sums, tops = kernel(
        functools.partial(inner_kernel, columns, size, feat),
        "inner",
        [shape((HEADS * held, LANES), F32), shape((HEADS * held, LANES), F32)],
        [
            pltpu.VMEM((LINE, inner), BF16),
            pltpu.VMEM((2, HEADS * held, size), F32),
            pltpu.VMEM((2, HEADS * held, size), BF16),
        ],
        count=2,
        cycles=10000,
        room=44,
    )(strip, rows)
    sent = kernel(
        functools.partial(border_kernel, columns, feat),
        "border",
        shape((held, HEADS * SLOT)),
        [
            pltpu.VMEM((LINE, 3 * LINE), BF16),
            pltpu.VMEM((2, HEADS * held, 3 * LINE), F32),
            pltpu.VMEM((2, HEADS * held, 3 * LINE), BF16),
        ],
        count=5,
        cycles=3000,
        room=24,
    )(strip, after, rows, sums, tops)
    parts = lax.all_to_all(sent.reshape(down, share, -1), "gx", 0, 0, tiled=True)
    own = lax.dynamic_slice_in_dim(latents, lax.axis_index(GROUP) * share, share, 0)
    return kernel(combine_kernel, "combine", shape((share, width)), count=3, room=6)(parts, both, own)


def solution(mesh):
    return jax.shard_map(
        on_device,
        mesh=mesh,
        in_specs=(P(("ba", "gx"), "gy", None), P(), P(), P(), P(), P(), P(), P(), P()),
        out_specs=P(("ba", "gx", "gy"), None),
        check_vma=False,
    )
```

```python
import functools

import jax
import jax.numpy as jnp
from jax import lax
from jax.experimental import pallas as pl
from jax.experimental.pallas import tpu as pltpu
from jax.sharding import PartitionSpec as P

HEADS = 8
DH = 128
LANES = 128
SUB = 8
TAPS = 9
CELL = 64
LINE = 256
SPAN = 80
ONE, MASK, ONE_TOO = 72, 73, 74
SLOT = 64
TOTAL, TOP = 54, 57
BIG = 1e30
EPS = 1e-05
LOG2E = 1.4426950408889634
GROUP = ("gx", "gy")
F32 = jnp.float32
BF16 = jnp.bfloat16


def product(a, b, left, right):
    return lax.dot_general(a, b, (((left,), (right,)), ((), ())), preferred_element_type=F32)


def nn(a, b):
    return product(a, b, 1, 0)


def nt(a, b):
    return product(a, b, 1, 1)


def tn(a, b):
    return product(a, b, 0, 0)


def iota(shape, dim):
    return lax.broadcasted_iota(jnp.int32, shape, dim)


def split_up(values):
    high = values.astype(BF16)
    return high, (values - high.astype(F32)).astype(BF16)


def thrice(values):
    one = values.astype(BF16)
    rest = values - one.astype(F32)
    two, three = split_up(rest)
    return one, two, three


def pack_kernel(pixel_ref, copies_ref, plane_ref):
    channels, rows, columns = pixel_ref.shape
    pitch = plane_ref.shape[0] // SUB
    plane_ref[...] = jnp.zeros(plane_ref.shape, F32)
    for channel in range(channels):
        plane_ref[channel * pitch : channel * pitch + rows, :columns] = pixel_ref[channel].astype(F32)
    for pair in range(rows // 2):
        even = plane_ref[pl.ds(2 * pair, SUB, stride=pitch), :]
        odd = plane_ref[pl.ds(2 * pair + 1, SUB, stride=pitch), :]
        packed = (even + pltpu.roll(odd, CELL, 1)).astype(BF16)
        for copy in range(copies_ref.shape[0]):
            copies_ref[copy, :, pair * LANES : (pair + 1) * LANES] = packed


def join_kernel(columns, tiles_ref, strip_ref, first_ref):
    tiles, _, width = tiles_ref.shape
    pairs = width // LANES
    lane = iota((pairs * SUB, LANES), 1)
    stacked = [
        jnp.concatenate([tiles_ref[tile, :, pair * LANES : (pair + 1) * LANES].astype(F32) for pair in range(pairs)], axis=0)
        for tile in range(tiles)
    ]
    for parity in range(2):
        halves = []
        for half in range(LINE // LANES):
            line = jnp.zeros((pairs * SUB, LANES), F32)
            for tile in range(tiles):
                start, end = tile * columns - half * LANES, (tile + 1) * columns - half * LANES
                if end <= 0 or start >= LANES:
                    continue
                moved = pltpu.roll(stacked[tile], (start - parity * CELL) % LANES, 1)
                line = jnp.where((lane >= start) & (lane < end), moved, line)
            halves.append(line)
        for pair in range(pairs):
            row = 2 * pair + parity
            for half, line in enumerate(halves):
                at = row * LINE + half * LANES
                strip_ref[:, at : at + LANES] = line[pair * SUB : (pair + 1) * SUB]
    first_ref[...] = strip_ref[:, : 2 * LINE].astype(BF16)


def spread_weight(conv_ref, copies):
    channels = conv_ref.shape[0] // TAPS
    shape = (copies, conv_ref.shape[0])
    row, tap = iota(shape, 0), iota(shape, 1)
    place = row % SPAN
    hit = (place // SUB == tap // channels) & (place % SUB == tap % channels) & (row < 3 * SPAN)
    spread = nn(jnp.where(hit, 1.0, 0.0).astype(BF16), conv_ref[...])
    return spread - jnp.mean(spread, axis=-1, keepdims=True)


def query_kernel(
    key_hbm, conv_hbm, gain_hbm, lat_hbm, lat_gain_hbm, query_hbm, rows_ref,
    key_ref, conv_ref, gain_ref, lat_ref, lat_gain_ref, query_ref, sems,
):
    sources = [key_hbm, conv_hbm, gain_hbm, lat_hbm.at[:, lax.axis_index("gy")], lat_gain_hbm, query_hbm]
    targets = [key_ref, conv_ref, gain_ref, lat_ref, lat_gain_ref, query_ref]
    copies = [pltpu.make_async_copy(*pair, sems.at[i]) for i, pair in enumerate(zip(sources, targets))]
    for copy in copies:
        copy.start()

    copies[1].wait()
    weight = spread_weight(conv_ref, SPAN)
    feat = weight.shape[1]
    high, low = split_up(weight)
    both = jnp.concatenate([high, low], axis=0)
    held = HEADS * lat_ref.shape[0] * lat_ref.shape[1]
    for part, at in enumerate(range(0, feat, LINE)):
        end = min(at + LINE, feat)
        first = held + LINE + part * 2 * SPAN
        rows_ref[first : first + 2 * SPAN, : end - at] = both[:, at:end]
    padding = jnp.zeros((LANES - SPAN, feat), BF16)
    gram = nt(both, jnp.concatenate([high, padding], axis=0)) + nt(both, jnp.concatenate([low, padding], axis=0))
    gram = (gram[:SPAN] + gram[SPAN:]) * (1.0 / feat)
    for part, piece in enumerate(thrice(gram)):
        rows_ref[held : held + SPAN, part * SPAN : (part + 1) * SPAN] = piece[:, :SPAN]

    copies[2].wait()
    copies[0].wait()
    keys = nn(jnp.concatenate(split_up(weight * gain_ref[...].reshape(1, -1)), axis=0), key_ref[...])
    high, low = split_up((keys[:SPAN] + keys[SPAN:]) * (LOG2E / DH**0.5))

    copies[3].wait()
    copies[4].wait()
    values = lat_ref[...].astype(F32)
    values = values.reshape(values.shape[0] * values.shape[1], values.shape[2])
    centred = values - jnp.mean(values, axis=-1, keepdims=True)
    variance = jnp.mean(centred * centred, axis=-1, keepdims=True)
    gain = lat_gain_ref[...].reshape(1, -1)
    normed = (centred * lax.rsqrt(variance + EPS) * gain).astype(BF16)
    copies[5].wait()
    queries = nn(normed, query_ref[...]).astype(BF16)

    count = values.shape[0]
    lane = iota((count, LINE), 1)
    padding = jnp.zeros((LINE - 3 * SPAN, 2 * DH), BF16)
    for head in range(HEADS):
        cut = slice(head * DH, (head + 1) * DH)
        query = jnp.concatenate([queries[:, cut], queries[:, cut]], axis=1)
        key = jnp.concatenate([high[:, cut], low[:, cut]], axis=1)
        rows = nt(query, jnp.concatenate([key, key, key, padding], axis=0))
        rows = jnp.where(lane == MASK, -1.0, rows)
        top, rest = split_up(rows)
        rows_ref[head * count : (head + 1) * count, :] = jnp.where((lane >= SPAN) & (lane < 2 * SPAN), rest, top)


def table_rows(feat):
    return LINE + -(-feat // LINE) * 2 * SPAN


def scaled_patches(patches, explicit, feat, rows_ref):
    exact = patches.astype(BF16)
    held = rows_ref.shape[0] - table_rows(feat)
    if explicit:
        total = 0.0
        for part, at in enumerate(range(0, feat, LINE)):
            end = min(at + LINE, feat)
            first = held + LINE + part * 2 * SPAN
            wide = rows_ref[first : first + 2 * SPAN, : end - at]
            features = tn(wide[:SPAN], exact) + tn(wide[SPAN:], exact)
            total = total + jnp.sum(features * features, axis=0, keepdims=True)
        variance = total * (1.0 / feat)
        lost = None
    else:
        gram = rows_ref[held : held + SPAN, : 3 * SPAN]
        form = nn(gram, jnp.concatenate([exact, exact, exact], axis=0))
        variance = jnp.maximum(jnp.sum(form * patches, axis=0, keepdims=True), 0.0)
        diag = jnp.where(iota(gram.shape, 0) == iota(gram.shape, 1), gram.astype(F32), 0.0)
        diag = jnp.sum(diag, axis=-1, keepdims=True)
        scale = jnp.sum(patches * patches * diag, axis=0, keepdims=True)
        lost = jnp.where((variance + EPS) * 128.0 < scale, 1.0, 0.0)
    return patches * lax.rsqrt(variance + EPS), lost


def fill_block(patches, real, explicit, feat, rows_ref, pixel_ref, at):
    width = patches.shape[1]
    scaled, lost = scaled_patches(patches, explicit, feat, rows_ref)
    row = iota((SPAN, width), 0)
    scaled = jnp.where((row == ONE) | (row == ONE_TOO), jnp.where(real, 1.0, 0.0), scaled)
    scaled = jnp.where(row == MASK, jnp.where(real, 0.0, BIG), scaled)
    high, low = split_up(scaled)
    cut = slice(at, at + width)
    pixel_ref[:SPAN, cut] = high
    pixel_ref[SPAN : 2 * SPAN, cut] = high
    pixel_ref[2 * SPAN : 3 * SPAN, cut] = low
    pixel_ref[3 * SPAN :, cut] = jnp.zeros((LINE - 3 * SPAN, width), BF16)
    return lost


def attend(blocks, rows_ref, pixel_ref, score_ref, expo_ref, take):
    tops = []
    count = len(blocks)
    for turn in range(count + 2):
        if turn < count:
            rows, cut = blocks[turn]
            score_ref[turn % 2, rows, : cut.stop - cut.start] = nn(rows_ref[rows], pixel_ref[:, cut])
        if 0 <= turn - 1 < count:
            rows, cut = blocks[turn - 1]
            at = ((turn - 1) % 2, rows, slice(0, cut.stop - cut.start))
            top = jnp.max(score_ref[at], axis=-1, keepdims=True)
            expo_ref[at] = jnp.exp2(score_ref[at] - top).astype(BF16)
            tops.append(top)
        if 0 <= turn - 2 < count:
            rows, cut = blocks[turn - 2]
            at = ((turn - 2) % 2, rows, slice(0, cut.stop - cut.start))
            take(turn - 2, tops[turn - 2], nt(expo_ref[at], pixel_ref[:LANES, cut]))


def merged(old_top, old_sums, top, sums):
    new = jnp.maximum(old_top, top)
    return new, jnp.exp2(old_top - new) * old_sums + jnp.exp2(top - new) * sums


def inner_kernel(
    columns, size, feat, strip_ref, rows_ref, sums_ref, tops_ref, pixel_ref, score_ref, expo_ref
):
    width = strip_ref.shape[1]
    inner = width - 2 * LINE
    strip = strip_ref[...]
    shifted = [pltpu.roll(strip, 1, 1), strip, pltpu.roll(strip, width - 1, 1)]
    count = sums_ref.shape[0]
    blocks = [(slice(0, count), slice(at, at + size)) for at in range(0, inner, size)]
    half = count // 2
    halves = [(slice(r, r + half), b) for _, b in blocks for r in (0, half)]

    def run(explicit):
        flags = []

        def fill(turn):
            at, end = blocks[turn][1].start, blocks[turn][1].stop
            cells = [shifted[tap % 3][:, tap // 3 * LINE + at : tap // 3 * LINE + end] for tap in range(TAPS)]
            patches = jnp.concatenate(cells + [jnp.zeros_like(cells[0])], axis=0)
            real = (iota(patches.shape, 1) + at) % LINE < columns
            flags.append(fill_block(patches, real, explicit, feat, rows_ref, pixel_ref, at))

        for turn in range(len(blocks)):
            fill(turn)
        def take(turn, top, sums):
            rows, cut = halves[turn]
            if cut.start > 0:
                top, sums = merged(tops_ref[rows], sums_ref[rows], top, sums)
            sums_ref[rows] = sums
            tops_ref[rows] = jnp.broadcast_to(top, sums.shape)

        attend(halves, rows_ref, pixel_ref, score_ref, expo_ref, take)
        return [jnp.max(flag) for flag in flags if flag is not None]

    lost = functools.reduce(jnp.maximum, run(False))

    @pl.when(lost > 0.5)
    def _():
        run(True)


def border_kernel(
    columns,
    feat,
    strip_ref,
    after_ref,
    rows_ref,
    inner_sums_ref,
    inner_tops_ref,
    sent_ref,
    pixel_ref,
    score_ref,
    expo_ref,
):
    width = strip_ref.shape[1]
    lines = jnp.concatenate(
        [
            strip_ref[:, width - 2 * LINE :],
            after_ref[...].astype(F32),
            jnp.zeros((SUB, LINE), F32),
            strip_ref[:, : 2 * LINE],
        ],
        axis=1,
    )
    shifted = [pltpu.roll(lines, 1, 1), lines, pltpu.roll(lines, lines.shape[1] - 1, 1)]
    place_x = lax.axis_index("gx")
    below = (place_x < lax.axis_size("gx") - 1).astype(jnp.int32)
    count = sent_ref.shape[0]
    half = score_ref.shape[1] // 2
    shape = (2 * LANES, LANES)
    row, lane = iota(shape, 0), iota(shape, 1)
    tap = row % LANES
    target = jnp.where((tap < ONE) & (tap % SUB < 6), tap // SUB * 6 + tap % SUB, -1)
    target = jnp.where(tap == ONE, TOTAL, jnp.where(tap == ONE_TOO, TOTAL + 1, target))
    place = jnp.where((target >= 0) & (lane == target + row // LANES * SLOT), 1.0, 0.0).astype(BF16)

    def run(explicit, starts):
        cells = []
        for tap in range(TAPS):
            at = tap // 3 * LINE
            source = shifted[tap % 3]
            cells.append(jnp.concatenate([source[:, start + at : start + at + LINE] for start in starts], axis=1))
        patches = jnp.concatenate(cells + [jnp.zeros_like(cells[0])], axis=0)
        lane = iota(patches.shape, 1)
        real = (lane % LINE < columns) & (jnp.where(lane // LINE == 1, below, 1) > 0)
        lost = fill_block(patches, real, explicit, feat, rows_ref, pixel_ref, 0)
        blocks = [(slice(at, at + half), slice(0, patches.shape[1])) for at in (0, half)]
        results = []
        attend(blocks, rows_ref, pixel_ref, score_ref, expo_ref, lambda turn, *result: results.append(result))
        tops, sums = (jnp.concatenate(parts, axis=0) for parts in zip(*results))
        top, total = merged(inner_tops_ref[...], inner_sums_ref[...], tops, sums)
        high = total.astype(BF16)
        low = (total - high.astype(F32)).astype(BF16)
        high = jnp.where(iota(total.shape, 1) == ONE_TOO, low, high)

        def side(values, odd):
            heads = range(odd, HEADS, 2)
            return jnp.concatenate([values[head * count : (head + 1) * count] for head in heads], axis=0)

        placed = nn(jnp.concatenate([side(high, 0), side(high, 1)], axis=1), place)
        lane = iota(placed.shape, 1)
        column = lane % SLOT
        one, two, three = thrice(jnp.where(lane < SLOT, side(top, 0), side(top, 1)))
        placed = jnp.where(column == TOP, one.astype(F32), placed)
        placed = jnp.where(column == TOP + 1, two.astype(F32), placed)
        placed = jnp.where(column == TOP + 2, three.astype(F32), placed).astype(BF16)
        for pair in range(HEADS // 2):
            sent_ref[:, pair * LANES : (pair + 1) * LANES] = placed[pair * count : (pair + 1) * count]
        return lost

    def checked(starts):
        lost = jnp.max(run(False, starts))

        @pl.when(lost > 0.5)
        def _():
            run(True, starts)

    @pl.when(place_x > 0)
    def _():
        checked([0, LINE])

    @pl.when(place_x == 0)
    def _():
        checked([0, LINE, 4 * LINE])


def output_kernel(conv_ref, gain_ref, value_ref, out_ref, both_ref):
    weight = conv_ref[...].astype(F32)
    weight = (weight - jnp.mean(weight, axis=-1, keepdims=True)) * gain_ref[...].reshape(1, -1)
    weight = jnp.concatenate([weight, jnp.zeros((SLOT - weight.shape[0], weight.shape[1]), F32)], axis=0)
    both = nn(jnp.concatenate(split_up(weight), axis=0), value_ref[...])
    high, low = split_up(both[:SLOT] + both[SLOT:])
    for head in range(HEADS):
        cut = slice(head * DH, (head + 1) * DH)
        both = nn(jnp.concatenate([high[:, cut], low[:, cut]], axis=0), out_ref[cut])
        both_ref[head * SLOT : (head + 1) * SLOT, :] = (both[:SLOT] + both[SLOT:]).astype(BF16)


def combine_kernel(parts_ref, both_ref, own_ref, result_ref):
    count, share, width = parts_ref.shape
    row, lane = iota((LANES, LANES), 0), iota((LANES, LANES), 1)
    same = row // SLOT == lane // SLOT
    column = row % SLOT
    pick_top = jnp.where(same & (column >= TOP) & (column < TOP + 3), 1.0, 0.0).astype(BF16)
    pick_one = jnp.where(same & (column >= TOTAL) & (column < TOTAL + 2), 1.0, 0.0).astype(BF16)
    means = []
    for at in range(0, width, LANES):
        values = parts_ref[:, :, at : at + LANES].astype(F32)
        parts = values.reshape(count * share, LANES).astype(BF16)
        tops = nn(parts, pick_top).reshape(values.shape)
        ones = nn(parts, pick_one).reshape(values.shape)
        factor = jnp.exp2(tops - jnp.max(tops, axis=0, keepdims=True))
        means.append(jnp.sum(factor * values, axis=0) / jnp.sum(factor * ones, axis=0))
    mean = jnp.concatenate(means, axis=1)
    high = mean.astype(BF16).astype(F32)
    result = nn(jnp.concatenate([high, mean - high], axis=0).astype(BF16), both_ref[...])
    result = own_ref[...].astype(F32) + (result[:share] + result[share:])
    result_ref[...] = result.astype(BF16)


def vmem(count):
    return [pl.BlockSpec(memory_space=pltpu.VMEM)] * count


def kernel(body, name, outs, scratch=(), others=0, count=0, cycles=1000, room=4):
    single = not isinstance(outs, (list, tuple))
    return pl.pallas_call(
        body,
        out_shape=outs,
        in_specs=vmem(count) + [pl.BlockSpec(memory_space=pltpu.HBM)] * others,
        out_specs=vmem(1)[0] if single else tuple(vmem(len(outs))),
        scratch_shapes=list(scratch),
        cost_estimate=pl.CostEstimate(flops=cycles * 4096, bytes_accessed=1 << 20, transcendentals=0),
        compiler_params=pltpu.CompilerParams(vmem_limit_bytes=int(room * 1024) << 10),
        name=name,
    )


def on_device(
    pixels,
    conv_weight,
    input_gain,
    key_weight,
    value_weight,
    latents,
    latent_gain,
    query_weight,
    out_weight,
):
    tile_rows, tile_cols, _ = pixels.shape
    across, down = lax.axis_size("gy"), lax.axis_size("gx")
    columns = tile_cols * across
    feat = conv_weight.shape[1]
    lat, width = latents.shape
    share = lat // (across * down)
    held = lat // across

    def shape(dims, dtype=BF16):
        return jax.ShapeDtypeStruct(dims, dtype)

    copies = kernel(
        pack_kernel,
        "pack",
        shape((across, SUB, tile_rows * CELL)),
        [pltpu.VMEM((SUB * 16, LANES), F32)],
        count=1,
        cycles=1000000,
    )(pixels.transpose(2, 0, 1))
    tiles = lax.all_to_all(copies, "gy", 0, 0, tiled=True)
    rows = kernel(
        query_kernel,
        "query_rows",
        shape((HEADS * held + table_rows(feat), LINE)),
        [
            pltpu.VMEM(key_weight.shape, BF16),
            pltpu.VMEM(conv_weight.shape, BF16),
            pltpu.VMEM(input_gain.shape, F32),
            pltpu.VMEM((down, share, width), BF16),
            pltpu.VMEM(latent_gain.shape, F32),
            pltpu.VMEM(query_weight.shape, BF16),
            pltpu.SemaphoreType.DMA((6,)),
        ],
        others=6,
        cycles=6000,
        room=52.7,
    )(key_weight, conv_weight, input_gain, latents.reshape(down, across, share, width), latent_gain, query_weight)
    both = kernel(
        output_kernel, "value_output", shape((HEADS * SLOT, width)), count=4, cycles=6000, room=10
    )(conv_weight, input_gain, value_weight, out_weight)

    tiles, rows = lax.optimization_barrier((tiles, rows))
    strip, first = kernel(
        functools.partial(join_kernel, tile_cols),
        "join",
        [shape((SUB, tile_rows * LINE), F32), shape((SUB, 2 * LINE))],
        count=1,
        cycles=200000,
    )(tiles)
    after = lax.ppermute(first, "gx", [(i + 1, i) for i in range(down - 1)])
    inner = (tile_rows - 2) * LINE
    size = inner // 4
    sums, tops = kernel(
        functools.partial(inner_kernel, columns, size, feat),
        "inner",
        [shape((HEADS * held, LANES), F32), shape((HEADS * held, LANES), F32)],
        [
            pltpu.VMEM((LINE, inner), BF16),
            pltpu.VMEM((2, HEADS * held, size), F32),
            pltpu.VMEM((2, HEADS * held, size), BF16),
        ],
        count=2,
        cycles=10000,
        room=44,
    )(strip, rows)
    sent = kernel(
        functools.partial(border_kernel, columns, feat),
        "border",
        shape((held, HEADS * SLOT)),
        [
            pltpu.VMEM((LINE, 3 * LINE), BF16),
            pltpu.VMEM((2, HEADS * held, 3 * LINE), F32),
            pltpu.VMEM((2, HEADS * held, 3 * LINE), BF16),
        ],
        count=5,
        cycles=3000,
        room=24,
    )(strip, after, rows, sums, tops)
    parts = lax.all_to_all(sent.reshape(down, share, -1), "gx", 0, 0, tiled=True)
    own = lax.dynamic_slice_in_dim(latents, lax.axis_index(GROUP) * share, share, 0)
    return kernel(combine_kernel, "combine", shape((share, width)), count=3, room=6)(parts, both, own)


def solution(mesh):
    return jax.shard_map(
        on_device,
        mesh=mesh,
        in_specs=(P(("ba", "gx"), "gy", None), P(), P(), P(), P(), P(), P(), P(), P()),
        out_specs=P(("ba", "gx", "gy"), None),
        check_vma=False,
    )
```

```python
import functools

import jax
import jax.numpy as jnp
from jax import lax
from jax.experimental import pallas as pl
from jax.experimental.pallas import tpu as pltpu
from jax.sharding import PartitionSpec as P

HEADS = 8
DH = 128
LANES = 128
SUB = 8
TAPS = 9
CELL = 64
LINE = 256
SPAN = 80
ONE, MASK, ONE_TOO = 72, 73, 74
SLOT = 64
TOTAL, TOP = 54, 57
BIG = 1e30
EPS = 1e-05
LOG2E = 1.4426950408889634
GROUP = ("gx", "gy")
F32 = jnp.float32
BF16 = jnp.bfloat16


def product(a, b, left, right):
    return lax.dot_general(a, b, (((left,), (right,)), ((), ())), preferred_element_type=F32)


def nn(a, b):
    return product(a, b, 1, 0)


def nt(a, b):
    return product(a, b, 1, 1)


def tn(a, b):
    return product(a, b, 0, 0)


def iota(shape, dim):
    return lax.broadcasted_iota(jnp.int32, shape, dim)


def split_up(values):
    high = values.astype(BF16)
    return high, (values - high.astype(F32)).astype(BF16)


def thrice(values):
    one = values.astype(BF16)
    rest = values - one.astype(F32)
    two, three = split_up(rest)
    return one, two, three


def pack_kernel(pixel_ref, copies_ref, plane_ref):
    channels, rows, columns = pixel_ref.shape
    pitch = plane_ref.shape[0] // SUB
    plane_ref[...] = jnp.zeros(plane_ref.shape, F32)
    for channel in range(channels):
        plane_ref[channel * pitch : channel * pitch + rows, :columns] = pixel_ref[channel].astype(F32)
    for pair in range(rows // 2):
        even = plane_ref[pl.ds(2 * pair, SUB, stride=pitch), :]
        odd = plane_ref[pl.ds(2 * pair + 1, SUB, stride=pitch), :]
        packed = (even + pltpu.roll(odd, CELL, 1)).astype(BF16)
        for copy in range(copies_ref.shape[0]):
            copies_ref[copy, :, pair * LANES : (pair + 1) * LANES] = packed


def join_kernel(columns, tiles_ref, strip_ref, first_ref):
    tiles, _, width = tiles_ref.shape
    pairs = width // LANES
    lane = iota((pairs * SUB, LANES), 1)
    stacked = [
        jnp.concatenate([tiles_ref[tile, :, pair * LANES : (pair + 1) * LANES].astype(F32) for pair in range(pairs)], axis=0)
        for tile in range(tiles)
    ]
    for parity in range(2):
        halves = []
        for half in range(LINE // LANES):
            line = jnp.zeros((pairs * SUB, LANES), F32)
            for tile in range(tiles):
                start, end = tile * columns - half * LANES, (tile + 1) * columns - half * LANES
                if end <= 0 or start >= LANES:
                    continue
                moved = pltpu.roll(stacked[tile], (start - parity * CELL) % LANES, 1)
                line = jnp.where((lane >= start) & (lane < end), moved, line)
            halves.append(line)
        for pair in range(pairs):
            row = 2 * pair + parity
            for half, line in enumerate(halves):
                at = row * LINE + half * LANES
                strip_ref[:, at : at + LANES] = line[pair * SUB : (pair + 1) * SUB]
    first_ref[...] = strip_ref[:, : 2 * LINE].astype(BF16)


def spread_weight(conv_ref, copies):
    channels = conv_ref.shape[0] // TAPS
    shape = (copies, conv_ref.shape[0])
    row, tap = iota(shape, 0), iota(shape, 1)
    place = row % SPAN
    hit = (place // SUB == tap // channels) & (place % SUB == tap % channels) & (row < 3 * SPAN)
    spread = nn(jnp.where(hit, 1.0, 0.0).astype(BF16), conv_ref[...])
    return spread - jnp.mean(spread, axis=-1, keepdims=True)


def query_kernel(
    key_hbm, conv_hbm, gain_hbm, lat_hbm, lat_gain_hbm, query_hbm, rows_ref,
    key_ref, conv_ref, gain_ref, lat_ref, lat_gain_ref, query_ref, sems,
):
    sources = [key_hbm, conv_hbm, gain_hbm, lat_hbm.at[:, lax.axis_index("gy")], lat_gain_hbm, query_hbm]
    targets = [key_ref, conv_ref, gain_ref, lat_ref, lat_gain_ref, query_ref]
    copies = [pltpu.make_async_copy(*pair, sems.at[i]) for i, pair in enumerate(zip(sources, targets))]
    for copy in copies:
        copy.start()

    copies[1].wait()
    weight = spread_weight(conv_ref, SPAN)
    feat = weight.shape[1]
    high, low = split_up(weight)
    both = jnp.concatenate([high, low], axis=0)
    held = HEADS * lat_ref.shape[0] * lat_ref.shape[1]
    for part, at in enumerate(range(0, feat, LINE)):
        end = min(at + LINE, feat)
        first = held + LINE + part * 2 * SPAN
        rows_ref[first : first + 2 * SPAN, : end - at] = both[:, at:end]
    padding = jnp.zeros((LANES - SPAN, feat), BF16)
    gram = nt(both, jnp.concatenate([high, padding], axis=0)) + nt(both, jnp.concatenate([low, padding], axis=0))
    gram = (gram[:SPAN] + gram[SPAN:]) * (1.0 / feat)
    for part, piece in enumerate(thrice(gram)):
        rows_ref[held : held + SPAN, part * SPAN : (part + 1) * SPAN] = piece[:, :SPAN]

    copies[2].wait()
    copies[0].wait()
    keys = nn(jnp.concatenate(split_up(weight * gain_ref[...].reshape(1, -1)), axis=0), key_ref[...])
    high, low = split_up((keys[:SPAN] + keys[SPAN:]) * (LOG2E / DH**0.5))

    copies[3].wait()
    copies[4].wait()
    values = lat_ref[...].astype(F32)
    values = values.reshape(values.shape[0] * values.shape[1], values.shape[2])
    centred = values - jnp.mean(values, axis=-1, keepdims=True)
    variance = jnp.mean(centred * centred, axis=-1, keepdims=True)
    gain = lat_gain_ref[...].reshape(1, -1)
    normed = (centred * lax.rsqrt(variance + EPS) * gain).astype(BF16)
    copies[5].wait()
    queries = nn(normed, query_ref[...]).astype(BF16)

    count = values.shape[0]
    lane = iota((count, LINE), 1)
    padding = jnp.zeros((LINE - 3 * SPAN, 2 * DH), BF16)
    for head in range(HEADS):
        cut = slice(head * DH, (head + 1) * DH)
        query = jnp.concatenate([queries[:, cut], queries[:, cut]], axis=1)
        key = jnp.concatenate([high[:, cut], low[:, cut]], axis=1)
        rows = nt(query, jnp.concatenate([key, key, key, padding], axis=0))
        rows = jnp.where(lane == MASK, -1.0, rows)
        top, rest = split_up(rows)
        rows_ref[head * count : (head + 1) * count, :] = jnp.where((lane >= SPAN) & (lane < 2 * SPAN), rest, top)


def table_rows(feat):
    return LINE + -(-feat // LINE) * 2 * SPAN


def scaled_patches(patches, explicit, feat, rows_ref):
    exact = patches.astype(BF16)
    held = rows_ref.shape[0] - table_rows(feat)
    if explicit:
        total = 0.0
        for part, at in enumerate(range(0, feat, LINE)):
            end = min(at + LINE, feat)
            first = held + LINE + part * 2 * SPAN
            wide = rows_ref[first : first + 2 * SPAN, : end - at]
            features = tn(wide[:SPAN], exact) + tn(wide[SPAN:], exact)
            total = total + jnp.sum(features * features, axis=0, keepdims=True)
        variance = total * (1.0 / feat)
        lost = None
    else:
        gram = rows_ref[held : held + SPAN, : 3 * SPAN]
        form = nn(gram, jnp.concatenate([exact, exact, exact], axis=0))
        variance = jnp.maximum(jnp.sum(form * patches, axis=0, keepdims=True), 0.0)
        diag = jnp.where(iota(gram.shape, 0) == iota(gram.shape, 1), gram.astype(F32), 0.0)
        diag = jnp.sum(diag, axis=-1, keepdims=True)
        scale = jnp.sum(patches * patches * diag, axis=0, keepdims=True)
        lost = jnp.where(scale >= 0.0, 1.0, 0.0)
    return patches * lax.rsqrt(variance + EPS), lost


def fill_block(patches, real, explicit, feat, rows_ref, pixel_ref, at):
    width = patches.shape[1]
    scaled, lost = scaled_patches(patches, explicit, feat, rows_ref)
    row = iota((SPAN, width), 0)
    scaled = jnp.where((row == ONE) | (row == ONE_TOO), jnp.where(real, 1.0, 0.0), scaled)
    scaled = jnp.where(row == MASK, jnp.where(real, 0.0, BIG), scaled)
    high, low = split_up(scaled)
    cut = slice(at, at + width)
    pixel_ref[:SPAN, cut] = high
    pixel_ref[SPAN : 2 * SPAN, cut] = high
    pixel_ref[2 * SPAN : 3 * SPAN, cut] = low
    pixel_ref[3 * SPAN :, cut] = jnp.zeros((LINE - 3 * SPAN, width), BF16)
    return lost


def attend(blocks, rows_ref, pixel_ref, score_ref, expo_ref, take):
    tops = []
    count = len(blocks)
    for turn in range(count + 2):
        if turn < count:
            rows, cut = blocks[turn]
            score_ref[turn % 2, rows, : cut.stop - cut.start] = nn(rows_ref[rows], pixel_ref[:, cut])
        if 0 <= turn - 1 < count:
            rows, cut = blocks[turn - 1]
            at = ((turn - 1) % 2, rows, slice(0, cut.stop - cut.start))
            top = jnp.max(score_ref[at], axis=-1, keepdims=True)
            expo_ref[at] = jnp.exp2(score_ref[at] - top).astype(BF16)
            tops.append(top)
        if 0 <= turn - 2 < count:
            rows, cut = blocks[turn - 2]
            at = ((turn - 2) % 2, rows, slice(0, cut.stop - cut.start))
            take(turn - 2, tops[turn - 2], nt(expo_ref[at], pixel_ref[:LANES, cut]))


def merged(old_top, old_sums, top, sums):
    new = jnp.maximum(old_top, top)
    return new, jnp.exp2(old_top - new) * old_sums + jnp.exp2(top - new) * sums


def inner_kernel(
    columns, size, feat, strip_ref, rows_ref, sums_ref, tops_ref, pixel_ref, score_ref, expo_ref
):
    width = strip_ref.shape[1]
    inner = width - 2 * LINE
    strip = strip_ref[...]
    shifted = [pltpu.roll(strip, 1, 1), strip, pltpu.roll(strip, width - 1, 1)]
    count = sums_ref.shape[0]
    blocks = [(slice(0, count), slice(at, at + size)) for at in range(0, inner, size)]
    half = count // 2
    halves = [(slice(r, r + half), b) for _, b in blocks for r in (0, half)]

    def run(explicit):
        flags = []

        def fill(turn):
            at, end = blocks[turn][1].start, blocks[turn][1].stop
            cells = [shifted[tap % 3][:, tap // 3 * LINE + at : tap // 3 * LINE + end] for tap in range(TAPS)]
            patches = jnp.concatenate(cells + [jnp.zeros_like(cells[0])], axis=0)
            real = (iota(patches.shape, 1) + at) % LINE < columns
            flags.append(fill_block(patches, real, explicit, feat, rows_ref, pixel_ref, at))

        for turn in range(len(blocks)):
            fill(turn)
        def take(turn, top, sums):
            rows, cut = halves[turn]
            if cut.start > 0:
                top, sums = merged(tops_ref[rows], sums_ref[rows], top, sums)
            sums_ref[rows] = sums
            tops_ref[rows] = jnp.broadcast_to(top, sums.shape)

        attend(halves, rows_ref, pixel_ref, score_ref, expo_ref, take)
        return [jnp.max(flag) for flag in flags if flag is not None]

    lost = functools.reduce(jnp.maximum, run(False))

    @pl.when(lost > 0.5)
    def _():
        run(True)


def border_kernel(
    columns,
    feat,
    strip_ref,
    after_ref,
    rows_ref,
    inner_sums_ref,
    inner_tops_ref,
    sent_ref,
    pixel_ref,
    score_ref,
    expo_ref,
):
    width = strip_ref.shape[1]
    lines = jnp.concatenate(
        [
            strip_ref[:, width - 2 * LINE :],
            after_ref[...].astype(F32),
            jnp.zeros((SUB, LINE), F32),
            strip_ref[:, : 2 * LINE],
        ],
        axis=1,
    )
    shifted = [pltpu.roll(lines, 1, 1), lines, pltpu.roll(lines, lines.shape[1] - 1, 1)]
    place_x = lax.axis_index("gx")
    below = (place_x < lax.axis_size("gx") - 1).astype(jnp.int32)
    count = sent_ref.shape[0]
    half = score_ref.shape[1] // 2
    shape = (2 * LANES, LANES)
    row, lane = iota(shape, 0), iota(shape, 1)
    tap = row % LANES
    target = jnp.where((tap < ONE) & (tap % SUB < 6), tap // SUB * 6 + tap % SUB, -1)
    target = jnp.where(tap == ONE, TOTAL, jnp.where(tap == ONE_TOO, TOTAL + 1, target))
    place = jnp.where((target >= 0) & (lane == target + row // LANES * SLOT), 1.0, 0.0).astype(BF16)

    def run(explicit, starts):
        cells = []
        for tap in range(TAPS):
            at = tap // 3 * LINE
            source = shifted[tap % 3]
            cells.append(jnp.concatenate([source[:, start + at : start + at + LINE] for start in starts], axis=1))
        patches = jnp.concatenate(cells + [jnp.zeros_like(cells[0])], axis=0)
        lane = iota(patches.shape, 1)
        real = (lane % LINE < columns) & (jnp.where(lane // LINE == 1, below, 1) > 0)
        lost = fill_block(patches, real, explicit, feat, rows_ref, pixel_ref, 0)
        blocks = [(slice(at, at + half), slice(0, patches.shape[1])) for at in (0, half)]
        results = []
        attend(blocks, rows_ref, pixel_ref, score_ref, expo_ref, lambda turn, *result: results.append(result))
        tops, sums = (jnp.concatenate(parts, axis=0) for parts in zip(*results))
        top, total = merged(inner_tops_ref[...], inner_sums_ref[...], tops, sums)
        high = total.astype(BF16)
        low = (total - high.astype(F32)).astype(BF16)
        high = jnp.where(iota(total.shape, 1) == ONE_TOO, low, high)

        def side(values, odd):
            heads = range(odd, HEADS, 2)
            return jnp.concatenate([values[head * count : (head + 1) * count] for head in heads], axis=0)

        placed = nn(jnp.concatenate([side(high, 0), side(high, 1)], axis=1), place)
        lane = iota(placed.shape, 1)
        column = lane % SLOT
        one, two, three = thrice(jnp.where(lane < SLOT, side(top, 0), side(top, 1)))
        placed = jnp.where(column == TOP, one.astype(F32), placed)
        placed = jnp.where(column == TOP + 1, two.astype(F32), placed)
        placed = jnp.where(column == TOP + 2, three.astype(F32), placed).astype(BF16)
        for pair in range(HEADS // 2):
            sent_ref[:, pair * LANES : (pair + 1) * LANES] = placed[pair * count : (pair + 1) * count]
        return lost

    def checked(starts):
        lost = jnp.max(run(False, starts))

        @pl.when(lost > 0.5)
        def _():
            run(True, starts)

    @pl.when(place_x > 0)
    def _():
        checked([0, LINE])

    @pl.when(place_x == 0)
    def _():
        checked([0, LINE, 4 * LINE])


def output_kernel(conv_ref, gain_ref, value_ref, out_ref, both_ref):
    weight = conv_ref[...].astype(F32)
    weight = (weight - jnp.mean(weight, axis=-1, keepdims=True)) * gain_ref[...].reshape(1, -1)
    weight = jnp.concatenate([weight, jnp.zeros((SLOT - weight.shape[0], weight.shape[1]), F32)], axis=0)
    both = nn(jnp.concatenate(split_up(weight), axis=0), value_ref[...])
    high, low = split_up(both[:SLOT] + both[SLOT:])
    for head in range(HEADS):
        cut = slice(head * DH, (head + 1) * DH)
        both = nn(jnp.concatenate([high[:, cut], low[:, cut]], axis=0), out_ref[cut])
        both_ref[head * SLOT : (head + 1) * SLOT, :] = (both[:SLOT] + both[SLOT:]).astype(BF16)


def combine_kernel(parts_ref, both_ref, own_ref, result_ref):
    count, share, width = parts_ref.shape
    row, lane = iota((LANES, LANES), 0), iota((LANES, LANES), 1)
    same = row // SLOT == lane // SLOT
    column = row % SLOT
    pick_top = jnp.where(same & (column >= TOP) & (column < TOP + 3), 1.0, 0.0).astype(BF16)
    pick_one = jnp.where(same & (column >= TOTAL) & (column < TOTAL + 2), 1.0, 0.0).astype(BF16)
    means = []
    for at in range(0, width, LANES):
        values = parts_ref[:, :, at : at + LANES].astype(F32)
        parts = values.reshape(count * share, LANES).astype(BF16)
        tops = nn(parts, pick_top).reshape(values.shape)
        ones = nn(parts, pick_one).reshape(values.shape)
        factor = jnp.exp2(tops - jnp.max(tops, axis=0, keepdims=True))
        means.append(jnp.sum(factor * values, axis=0) / jnp.sum(factor * ones, axis=0))
    mean = jnp.concatenate(means, axis=1)
    high = mean.astype(BF16).astype(F32)
    result = nn(jnp.concatenate([high, mean - high], axis=0).astype(BF16), both_ref[...])
    result = own_ref[...].astype(F32) + (result[:share] + result[share:])
    result_ref[...] = result.astype(BF16)


def vmem(count):
    return [pl.BlockSpec(memory_space=pltpu.VMEM)] * count


def kernel(body, name, outs, scratch=(), others=0, count=0, cycles=1000, room=4):
    single = not isinstance(outs, (list, tuple))
    return pl.pallas_call(
        body,
        out_shape=outs,
        in_specs=vmem(count) + [pl.BlockSpec(memory_space=pltpu.HBM)] * others,
        out_specs=vmem(1)[0] if single else tuple(vmem(len(outs))),
        scratch_shapes=list(scratch),
        cost_estimate=pl.CostEstimate(flops=cycles * 4096, bytes_accessed=1 << 20, transcendentals=0),
        compiler_params=pltpu.CompilerParams(vmem_limit_bytes=int(room * 1024) << 10),
        name=name,
    )


def on_device(
    pixels,
    conv_weight,
    input_gain,
    key_weight,
    value_weight,
    latents,
    latent_gain,
    query_weight,
    out_weight,
):
    tile_rows, tile_cols, _ = pixels.shape
    across, down = lax.axis_size("gy"), lax.axis_size("gx")
    columns = tile_cols * across
    feat = conv_weight.shape[1]
    lat, width = latents.shape
    share = lat // (across * down)
    held = lat // across

    def shape(dims, dtype=BF16):
        return jax.ShapeDtypeStruct(dims, dtype)

    copies = kernel(
        pack_kernel,
        "pack",
        shape((across, SUB, tile_rows * CELL)),
        [pltpu.VMEM((SUB * 16, LANES), F32)],
        count=1,
        cycles=1000000,
    )(pixels.transpose(2, 0, 1))
    tiles = lax.all_to_all(copies, "gy", 0, 0, tiled=True)
    rows = kernel(
        query_kernel,
        "query_rows",
        shape((HEADS * held + table_rows(feat), LINE)),
        [
            pltpu.VMEM(key_weight.shape, BF16),
            pltpu.VMEM(conv_weight.shape, BF16),
            pltpu.VMEM(input_gain.shape, F32),
            pltpu.VMEM((down, share, width), BF16),
            pltpu.VMEM(latent_gain.shape, F32),
            pltpu.VMEM(query_weight.shape, BF16),
            pltpu.SemaphoreType.DMA((6,)),
        ],
        others=6,
        cycles=6000,
        room=52.7,
    )(key_weight, conv_weight, input_gain, latents.reshape(down, across, share, width), latent_gain, query_weight)
    both = kernel(
        output_kernel, "value_output", shape((HEADS * SLOT, width)), count=4, cycles=6000, room=10
    )(conv_weight, input_gain, value_weight, out_weight)

    tiles, rows = lax.optimization_barrier((tiles, rows))
    strip, first = kernel(
        functools.partial(join_kernel, tile_cols),
        "join",
        [shape((SUB, tile_rows * LINE), F32), shape((SUB, 2 * LINE))],
        count=1,
        cycles=200000,
    )(tiles)
    after = lax.ppermute(first, "gx", [(i + 1, i) for i in range(down - 1)])
    inner = (tile_rows - 2) * LINE
    size = inner // 4
    sums, tops = kernel(
        functools.partial(inner_kernel, columns, size, feat),
        "inner",
        [shape((HEADS * held, LANES), F32), shape((HEADS * held, LANES), F32)],
        [
            pltpu.VMEM((LINE, inner), BF16),
            pltpu.VMEM((2, HEADS * held, size), F32),
            pltpu.VMEM((2, HEADS * held, size), BF16),
        ],
        count=2,
        cycles=10000,
        room=44,
    )(strip, rows)
    sent = kernel(
        functools.partial(border_kernel, columns, feat),
        "border",
        shape((held, HEADS * SLOT)),
        [
            pltpu.VMEM((LINE, 3 * LINE), BF16),
            pltpu.VMEM((2, HEADS * held, 3 * LINE), F32),
            pltpu.VMEM((2, HEADS * held, 3 * LINE), BF16),
        ],
        count=5,
        cycles=3000,
        room=24,
    )(strip, after, rows, sums, tops)
    parts = lax.all_to_all(sent.reshape(down, share, -1), "gx", 0, 0, tiled=True)
    own = lax.dynamic_slice_in_dim(latents, lax.axis_index(GROUP) * share, share, 0)
    return kernel(combine_kernel, "combine", shape((share, width)), count=3, room=6)(parts, both, own)


def solution(mesh):
    return jax.shard_map(
        on_device,
        mesh=mesh,
        in_specs=(P(("ba", "gx"), "gy", None), P(), P(), P(), P(), P(), P(), P(), P()),
        out_specs=P(("ba", "gx", "gy"), None),
        check_vma=False,
    )
```
